32 devices in a mesh: gx: 8 (over y, x, core), gy: 4 (over z).
Axes of the slice: x: 2, y: 2, z: 4, core: 2. Of those that a mesh axis runs over, the one named last changes fastest.
Arguments:
- right_side: float32 [3, 128, 32, 256], P(None, 'gx', 'gy'), may hold values from -12 to 12
- labels: int32 [128, 32, 256], P('gx', 'gy'), may hold values 0 or 1
Outputs:
- solution: float32 [3, 128, 32, 256], P(None, 'gx', 'gy')
- residual: float32 [3, 128, 32, 256], P(None, 'gx', 'gy')
The draws below stay inside these ranges and needn't reach their ends.
All inputs are finite; a program needn't handle non-finite values. No bound on the sum of `labels` on one device may be relied on, other than what follows from the above.
Results may differ from the reference program's by a relative error of at most 0.0003.
Values sent between devices are 32-bit elements; how exact they have to be, the bound alone decides.
No kernel may reach another device: no remote copies, remote signals or barrier semaphores. Data moves between devices by JAX's collectives and lax.ppermute only.
A program may use at most 64 MiB of HBM per device.

```python
import math
import jax
import jax.numpy as jnp
import numpy as np
from jax import lax

NZ = 256
ITERS = 4
NX = 128
NY = 32


def draw_right_side(key, part):
    key_base = jax.random.fold_in(jax.random.fold_in(key, 11), 0)
    position_x = jnp.arange(NX, dtype=jnp.float32) / NX
    position_y = jnp.arange(NY, dtype=jnp.float32) / NY
    base_values = jnp.clip(jax.random.normal(key_base, (3, NX, NY, NZ), jnp.float32), -4.0, 4.0)
    amplitude = jnp.exp(math.log(3.0) * (0.5 * position_x[:, None] + 0.5 * position_y[None, :]))
    values = base_values * amplitude[None, :, :, None]
    return values.astype(jnp.float32)


def place_ends(entries, own_key, smallest, largest):
    dims = entries.shape
    spot = [jax.random.randint(jax.random.fold_in(own_key, axis), (), 0, dims[axis]) for axis in range(len(dims))]
    entries = entries.at[tuple(spot)].set(smallest)
    longest = dims.index(max(dims))
    spot[longest] = (spot[longest] + 1) % dims[longest]
    return entries.at[tuple(spot)].set(largest)


def setup_inputs(seed: int = 0) -> dict:
    key_list = jax.random.split(jax.random.key(seed), 3)
    return {
        "right_side": draw_right_side(jax.random.fold_in(key_list[2], 71), 0),
        "labels": place_ends((jax.random.randint(key_list[1], (NX, NY, NZ), 0, 3) < 1).astype(jnp.int32), jax.random.fold_in(key_list[1], 1), 0, 1),
    }


LAMBDA_SOFT = 0.5769231
LAMBDA_RISE = 1.6452991
SHEAR_SOFT = 0.3846154
SHEAR_RISE = 2.9487179
KAPPA = 0.05

def corner_bits(corner):
    return (corner >> 2 & 1, corner >> 1 & 1, corner & 1)

def element_tables():
    gauss_offset = 0.5 / math.sqrt(3.0)
    gauss_points = [0.5 - gauss_offset, 0.5 + gauss_offset]
    lame_table = np.zeros((24, 24))
    shear_table = np.zeros((24, 24))
    normal_block = np.zeros((6, 6))
    normal_block[:3, :3] = 1.0
    shear_block = np.zeros((6, 6))
    for entry in range(6):
        shear_block[entry, entry] = 2.0 if entry < 3 else 1.0
    for point_x in gauss_points:
        for point_y in gauss_points:
            for point_z in gauss_points:
                strain = np.zeros((6, 24))
                for corner in range(8):
                    cx_bit, cy_bit, cz_bit = corner_bits(corner)
                    shape_x = point_x if cx_bit else 1.0 - point_x
                    shape_y = point_y if cy_bit else 1.0 - point_y
                    shape_z = point_z if cz_bit else 1.0 - point_z
                    slope_x = 1.0 if cx_bit else -1.0
                    slope_y = 1.0 if cy_bit else -1.0
                    slope_z = 1.0 if cz_bit else -1.0
                    grad_x = slope_x * shape_y * shape_z
                    grad_y = shape_x * slope_y * shape_z
                    grad_z = shape_x * shape_y * slope_z
                    column = 3 * corner
                    strain[0, column] = grad_x
                    strain[1, column + 1] = grad_y
                    strain[2, column + 2] = grad_z
                    strain[3, column + 1] = grad_z
                    strain[3, column + 2] = grad_y
                    strain[4, column] = grad_z
                    strain[4, column + 2] = grad_x
                    strain[5, column] = grad_y
                    strain[5, column + 1] = grad_x
                lame_table += 0.125 * strain.T @ normal_block @ strain
                shear_table += 0.125 * strain.T @ shear_block @ strain
    return np.concatenate([lame_table, shear_table], 0).astype(np.float32)

def table_diagonal(table):
    return np.array([table[entry, entry] for entry in range(24)], dtype=np.float32)

def moduli(labels):
    stiff = labels.astype(jnp.float32)
    return (LAMBDA_SOFT + LAMBDA_RISE * stiff, SHEAR_SOFT + SHEAR_RISE * stiff)

def reference(right_side, labels):
    tables = element_tables()
    stiffness = jnp.asarray(tables, dtype=jnp.float32)
    diag_lame = jnp.asarray(table_diagonal(tables[:24]), dtype=jnp.float32)
    diag_shear = jnp.asarray(table_diagonal(tables[24:]), dtype=jnp.float32)
    lame_first, shear_modulus = moduli(labels)
    row_block = math.gcd(NX, 8)
    block_count = NX // row_block

    def operate(vector_in):
        wrapped = jnp.concatenate([vector_in, vector_in[:, :1]], 1)

        def one_block(number):
            offset = number * row_block
            node_values = lax.dynamic_slice_in_dim(wrapped, offset, row_block + 1, 1)
            lame_block = lax.dynamic_slice_in_dim(lame_first, offset, row_block, 0)
            shear_part = lax.dynamic_slice_in_dim(shear_modulus, offset, row_block, 0)
            rolled_z = jnp.roll(node_values, -1, 3)
            corner_views = []
            for corner in range(8):
                cx_bit, cy_bit, cz_bit = corner_bits(corner)
                source_nodes = rolled_z if cz_bit else node_values
                corner_view = source_nodes[:, cx_bit:cx_bit + row_block]
                if cy_bit:
                    corner_view = jnp.roll(corner_view, -1, 2)
                corner_views.append(corner_view)
            stacked = jnp.concatenate(corner_views, 0).reshape(24, -1)
            products = jnp.dot(stiffness, stacked, precision=lax.Precision.HIGHEST, preferred_element_type=jnp.float32)
            forces = (lame_block.reshape(1, -1) * products[:24] + shear_part.reshape(1, -1) * products[24:]).reshape(8, 3, row_block, NY, NZ)
            lower_sum = jnp.zeros((3, row_block, NY, NZ), jnp.float32)
            upper_sum = jnp.zeros((3, row_block, NY, NZ), jnp.float32)
            for corner in range(8):
                cx_bit, cy_bit, cz_bit = corner_bits(corner)
                portion = forces[corner]
                if cy_bit:
                    portion = jnp.roll(portion, 1, 2)
                if cz_bit:
                    portion = jnp.roll(portion, 1, 3)
                if cx_bit:
                    upper_sum = upper_sum + portion
                else:
                    lower_sum = lower_sum + portion
            return (lower_sum, upper_sum)
        lower_sum, upper_sum = lax.map(one_block, jnp.arange(block_count, dtype=jnp.int32))
        lower_sum = jnp.moveaxis(lower_sum, 0, 1).reshape(3, NX, NY, NZ)
        upper_sum = jnp.moveaxis(upper_sum, 0, 1).reshape(3, NX, NY, NZ)
        return lower_sum + jnp.roll(upper_sum, 1, 1) + KAPPA * vector_in
    diagonal = jnp.zeros((3, NX, NY, NZ), jnp.float32) + KAPPA
    for corner in range(8):
        cx_bit, cy_bit, cz_bit = corner_bits(corner)
        portion = lame_first[None] * diag_lame[3 * corner:3 * corner + 3, None, None, None] + shear_modulus[None] * diag_shear[3 * corner:3 * corner + 3, None, None, None]
        portion = jnp.roll(portion, (cx_bit, cy_bit, cz_bit), (1, 2, 3))
        diagonal = diagonal + portion
    solution = jnp.zeros_like(right_side)
    residual = right_side
    scaled = residual / diagonal
    direction = scaled
    descent = jnp.sum(residual * scaled)
    for iteration in range(ITERS):
        image_vector = operate(direction)
        step_length = descent / jnp.sum(direction * image_vector)
        solution = solution + step_length * direction
        residual = residual - step_length * image_vector
        scaled = residual / diagonal
        descent_new = jnp.sum(residual * scaled)
        direction = scaled + descent_new / descent * direction
        descent = descent_new
    return (solution, residual)
```

```python
import jax
import jax.numpy as jnp
from jax import lax
from jax.experimental import pallas as pl
from jax.experimental.pallas import tpu as pltpu
from jax.sharding import PartitionSpec as P

ITERS = 4
HALO = ITERS
LAMBDA_SOFT = 0.5769231
LAMBDA_RISE = 1.6452991
SHEAR_SOFT = 0.3846154
SHEAR_RISE = 2.9487179
KAPPA = 0.05
CENTRE = 0.5 * (0.5 + 2.6)
HALF = 0.5 * (2.6 - 0.5)
SUMS = 14


def shifted(shard, axis, by):
    size = lax.axis_size(axis)
    return lax.ppermute(shard, axis, [(i, (i + by) % size) for i in range(size)])


def roll(v, by, axis):
    return pltpu.roll(v, by % v.shape[axis], axis)


def gather_modes(v):
    ahead = roll(v, -1, 1)
    out = {}
    for bz, a in ((0, v + ahead), (1, ahead - v)):
        up = roll(a, -1, 0)
        out[0, bz] = a + up
        out[1, bz] = up - a
    return out


def scatter_modes(r):
    part = []
    for bz in (0, 1):
        part.append((r[0, bz] - r[1, bz]) + roll(r[0, bz] + r[1, bz], 1, 0))
    return (part[0] - part[1]) + roll(part[0] + part[1], 1, 1)


def voxel_forces(c, stiff):
    lam = (LAMBDA_SOFT / 16) + (LAMBDA_RISE / 16) * stiff
    mu = (SHEAR_SOFT / 16) + (SHEAR_RISE / 16) * stiff
    mu2 = mu + mu
    lam3 = lam * (1.0 / 3)
    mu3 = mu * (1.0 / 3)
    top = ((LAMBDA_SOFT + 4 * SHEAR_SOFT) / 144) + ((LAMBDA_RISE + 4 * SHEAR_RISE) / 144) * stiff
    f = {}
    normal = ((0, 1, 0, 0), (1, 0, 1, 0), (2, 0, 0, 1))
    t = lam * (c[normal[0]] + c[normal[1]] + c[normal[2]])
    for p in normal:
        f[p] = t + mu2 * c[p]
    for p, q in (
        ((0, 1, 1, 0), (2, 0, 1, 1)),
        ((0, 1, 0, 1), (1, 0, 1, 1)),
        ((1, 1, 1, 0), (2, 1, 0, 1)),
    ):
        t = lam3 * (c[p] + c[q])
        f[p] = t + mu * c[p]
        f[q] = t + mu * c[q]
    for comp in range(3):
        p = (comp, 1, 1, 1)
        f[p] = top * c[p]
    for p, q in (
        ((0, 0, 1, 0), (1, 1, 0, 0)),
        ((0, 0, 0, 1), (2, 1, 0, 0)),
        ((1, 0, 0, 1), (2, 0, 1, 0)),
    ):
        f[p] = f[q] = mu * (c[p] + c[q])
    bend = ((0, 0, 1, 1), (1, 1, 0, 1), (2, 1, 1, 0))
    t = c[bend[0]] + c[bend[1]] + c[bend[2]]
    for p in bend:
        f[p] = mu3 * (t + c[p])
    return f


MODES = [(comp, by, bz) for comp in range(3) for by in (0, 1) for bz in (0, 1)]


def basis_kernel(r_ref, lab_ref, edge_ref, t_out, d_out, sums_out, t_ref, inv_ref, q_ref, f_ref):
    planes, rows, depth = r_ref.shape[1:]
    own_x = planes - 2 * HALO
    own_y = rows - 2 * HALO
    lo, hi = HALO, HALO + own_x
    first_row = own_y + HALO

    base = 8 * (LAMBDA_SOFT + 4 * SHEAR_SOFT) / 9 + KAPPA
    rise = (LAMBDA_RISE + 4 * SHEAR_RISE) / 9
    row_id = lax.broadcasted_iota(jnp.int32, (rows, depth), 0)

    def layer(m):
        l = lab_ref[m]
        lz = l + roll(l, 1, 1)
        e = edge_ref[pl.ds(m, 1), :]
        ez = jnp.broadcast_to(e + roll(e, 1, 1), (rows, depth))
        return lz + jnp.where(row_id == first_row, ez, roll(lz, 1, 0))

    def start(n, before):
        here = layer(n + 1)
        diag = base + rise * (before + here)
        inv = 1.0 / diag
        inv_ref[n] = inv
        for comp in range(3):
            t_ref[0, comp, n] = r_ref[comp, n] * inv

        @pl.when((n >= lo) & (n < hi))
        def _():
            d_out[n - lo] = diag[:own_y]
            for comp in range(3):
                t_out[0, comp, n - lo] = t_ref[0, comp, n][:own_y]

        return here

    lax.fori_loop(0, planes, start, layer(0))

    tiles = [
        (slice(a, a + 8), slice(b, b + 128)) for a in range(0, rows, 8) for b in range(0, depth, 128)
    ]
    totals = []
    for k in range(ITERS):
        first, last = k, planes - k

        def forward(n, _):
            for comp in range(3):
                out = gather_modes(t_ref[k, comp, n])
                for i, (cc, by, bz) in enumerate(MODES):
                    if cc == comp:
                        q_ref[i, n] = out[by, bz]
            return _

        lax.fori_loop(first, last, forward, 0)

        for tile in tiles:

            def voxels(n, carry):
                near, behind = carry
                far = [q_ref[i, n + 1, tile[0], tile[1]] for i in range(len(MODES))]
                c = {}
                for i, (comp, by, bz) in enumerate(MODES):
                    if (by, bz) != (0, 0):
                        c[comp, 0, by, bz] = near[i] + far[i]
                    c[comp, 1, by, bz] = far[i] - near[i]
                f = voxel_forces(c, lab_ref[n + 1, tile[0], tile[1]])
                ahead = []
                for i, (comp, by, bz) in enumerate(MODES):
                    up = f[comp, 1, by, bz]
                    if (by, bz) != (0, 0):
                        flat = f[comp, 0, by, bz]
                        f_ref[i, n, tile[0], tile[1]] = behind[i] + (flat - up)
                        ahead.append(flat + up)
                    else:
                        f_ref[i, n, tile[0], tile[1]] = behind[i] - up
                        ahead.append(up)
                return far, ahead

            near = [q_ref[i, first, tile[0], tile[1]] for i in range(len(MODES))]
            lax.fori_loop(first, last - 1, voxels, (near, [jnp.zeros_like(v) for v in near]))

        def advance(n, own, acc):
            acc = list(acc)
            inv = inv_ref[n]
            for comp in range(3):
                modes = {
                    (by, bz): f_ref[i, n]
                    for i, (cc, by, bz) in enumerate(MODES)
                    if cc == comp
                }
                t = t_ref[k, comp, n]
                image = scatter_modes(modes) + KAPPA * t
                if own:
                    for j in range(k + 1):
                        acc[j] += t_ref[j, comp, n, :own_y] * image[:own_y]
                    acc[k + 1] += t[:own_y] * r_ref[comp, n, :own_y]
                new = image * inv
                if k == 1:
                    new = (new - CENTRE * t) * (1 / HALF)
                elif k > 1:
                    new = (new - CENTRE * t) * (2 / HALF) - t_ref[k - 1, comp, n]
                if k + 1 < ITERS:
                    t_ref[k + 1, comp, n] = new
                if own:
                    t_out[k + 1, comp, n - lo] = new[:own_y]
            return tuple(acc)

        if k + 1 < ITERS:
            lax.fori_loop(first + 1, lo, lambda n, c: advance(n, False, c), ())
            lax.fori_loop(hi, last - 1, lambda n, c: advance(n, False, c), ())
        zero = jnp.zeros((own_y, depth), jnp.float32)
        acc = lax.fori_loop(lo, hi, lambda n, c: advance(n, True, c), (zero,) * (k + 2))
        totals.extend(acc)

    lane = lax.broadcasted_iota(jnp.int32, (1, 128), 1)
    packed = jnp.zeros((1, 128), jnp.float32)
    for i, v in enumerate(totals):
        s = jnp.sum(jnp.sum(v, axis=0, keepdims=True), axis=1, keepdims=True)
        packed = jnp.where(lane == i, s, packed)
    sums_out[...] = packed


def combine_kernel(sums_ref, t_ref, d_ref, x_out, r_out):
    total = jnp.sum(sums_ref[...], axis=0, keepdims=True)
    lane = lax.broadcasted_iota(jnp.int32, total.shape, 1)
    entry = [
        jnp.sum(jnp.where(lane == i, total, 0.0), axis=1, keepdims=True) for i in range(SUMS)
    ]
    gram, right = {}, []
    place = 0
    for k in range(ITERS):
        for j in range(k + 1):
            gram[j, k] = gram[k, j] = entry[place]
            place += 1
        right.append(entry[place])
        place += 1
    scale = [gram[k, k] for k in range(ITERS)]
    inv, low = [], {}
    for k in range(ITERS):
        pivot = gram[k, k]
        good = pivot > 1e-7 * scale[k]
        inv.append(jnp.where(good, 1.0 / jnp.where(good, pivot, 1.0), 0.0))
        for i in range(k + 1, ITERS):
            low[i, k] = gram[i, k] * inv[k]
        for i in range(k + 1, ITERS):
            for j in range(k + 1, i + 1):
                gram[i, j] = gram[j, i] = gram[i, j] - low[i, k] * gram[j, k]
            right[i] = right[i] - low[i, k] * right[k]
    y = [None] * ITERS
    for k in reversed(range(ITERS)):
        y[k] = right[k] * inv[k]
        for i in range(k + 1, ITERS):
            y[k] = y[k] - low[i, k] * y[i]
    e = [jnp.ones_like(y[0])] + [jnp.zeros_like(y[0]) for _ in range(ITERS)]
    for k in range(ITERS):
        if k == 0:
            e[1] = e[1] - y[0]
        elif k == 1:
            e[2] = e[2] - HALF * y[1]
            e[1] = e[1] - CENTRE * y[1]
        else:
            e[k + 1] = e[k + 1] - (HALF / 2) * y[k]
            e[k - 1] = e[k - 1] - (HALF / 2) * y[k]
            e[k] = e[k] - CENTRE * y[k]
    shape = d_ref.shape[1:]
    y = [jnp.broadcast_to(v, shape) for v in y]
    e = [jnp.broadcast_to(v, shape) for v in e]

    def body(n, _):
        diag = d_ref[n]
        for comp in range(3):
            t = [t_ref[k, comp, n] for k in range(ITERS + 1)]
            x, r = y[0] * t[0], e[0] * t[0]
            for k in range(1, ITERS):
                x = x + y[k] * t[k]
                r = r + e[k] * t[k]
            r = r + e[ITERS] * t[ITERS]
            x_out[comp, n] = x
            r_out[comp, n] = r * diag
        return _

    lax.fori_loop(0, d_ref.shape[0], body, 0)


def local(right_side, labels):
    own_x, own_y, depth = labels.shape
    h = HALO
    devices = lax.axis_size("gx") * lax.axis_size("gy")
    lab = labels.astype(jnp.float32)
    both = jnp.concatenate([right_side, lab[None]], 0)

    to_plus = both[:, :, own_y - h :].reshape(4 * own_x, h, depth)
    edge_rows = lab[:, own_y - h - 1].reshape(own_x // h, h, depth)
    from_minus = shifted(jnp.concatenate([to_plus, edge_rows], 0), "gy", 1)
    from_plus = shifted(both[:, :, :h].reshape(4 * own_x, h, depth), "gy", -1)

    def to_next(block, voxels, extra):
        parts = [block[:, own_x - h :].reshape(3 * h, -1, depth), voxels[own_x - h - 1 :]]
        return shifted(jnp.concatenate(parts + extra, 0), "gx", 1)

    def to_previous(block, voxels, extra):
        parts = [block[:, :h].reshape(3 * h, -1, depth), voxels[:h]]
        return shifted(jnp.concatenate(parts + extra, 0), "gx", -1)

    below = to_next(right_side, lab, [])
    above = to_previous(right_side, lab, [])

    side = jnp.concatenate(
        [
            from_plus.reshape(4, own_x, h, depth),
            from_minus[: 4 * own_x].reshape(4, own_x, h, depth),
        ],
        2,
    )
    edge = from_minus[4 * own_x :].reshape(own_x, depth)
    side_r, side_l = side[:3], side[3]

    def padded(rows):
        return jnp.pad(rows, ((0, 2 * h - rows.shape[0]), (0, 0)))[None]

    below_side = to_next(side_r, side_l, [padded(edge[own_x - h - 1 :])])
    above_side = to_previous(side_r, side_l, [padded(edge[:h])])

    def extended(block, voxels, low, high):
        nodes = jnp.concatenate(
            [
                low[: 3 * h].reshape(3, h, -1, depth),
                block,
                high[: 3 * h].reshape(3, h, -1, depth),
            ],
            1,
        )
        cells = jnp.concatenate([low[3 * h : 4 * h + 1], voxels, high[3 * h : 4 * h]], 0)
        return nodes, cells

    nodes_a, cells_a = extended(right_side, lab, below, above)
    nodes_b, cells_b = extended(side_r, side_l, below_side, above_side)
    nodes = jnp.concatenate([nodes_a, nodes_b], 2)
    cells = jnp.concatenate([cells_a, cells_b], 1)
    edges = jnp.concatenate([below_side[4 * h + 1, : h + 1], edge, above_side[4 * h, :h]], 0)

    planes, rows = nodes.shape[1:3]
    f32 = jnp.float32
    basis, diagonal, sums = pl.pallas_call(
        basis_kernel,
        out_shape=(
            jax.ShapeDtypeStruct((ITERS + 1, 3, own_x, own_y, depth), f32),
            jax.ShapeDtypeStruct((own_x, own_y, depth), f32),
            jax.ShapeDtypeStruct((1, 128), f32),
        ),
        scratch_shapes=[
            pltpu.VMEM((ITERS, 3, planes, rows, depth), f32),
            pltpu.VMEM((planes, rows, depth), f32),
            pltpu.VMEM((len(MODES), planes, rows, depth), f32),
            pltpu.VMEM((len(MODES), planes, rows, depth), f32),
        ],
        name="basis",
    )(nodes, cells, edges)

    everyone = lax.all_to_all(
        jnp.broadcast_to(sums[None], (devices,) + sums.shape), ("gx", "gy"), 0, 0
    )
    out = jax.ShapeDtypeStruct(right_side.shape, f32)
    return pl.pallas_call(combine_kernel, out_shape=(out, out), name="combine")(
        everyone.reshape(devices, 128), basis, diagonal
    )


def solution(mesh):
    in_specs = (P(None, "gx", "gy", None), P("gx", "gy", None))
    out_specs = (P(None, "gx", "gy", None), P(None, "gx", "gy", None))
    return jax.shard_map(local, mesh=mesh, in_specs=in_specs, out_specs=out_specs, check_vma=False)
```

```python
import functools

import jax
import jax.numpy as jnp
from jax import lax
from jax.experimental import pallas as pl
from jax.experimental.pallas import tpu as pltpu
from jax.sharding import PartitionSpec as P


ITERS = 4
HALO = ITERS
LAMBDA_SOFT = 0.5769231
LAMBDA_RISE = 1.6452991
SHEAR_SOFT = 0.3846154
SHEAR_RISE = 2.9487179
KAPPA = 0.05
CENTRE = 0.5 * (0.5 + 2.6)
HALF = 0.5 * (2.6 - 0.5)
SUMS = 14


def shifted(shard, axis, by):
    size = lax.axis_size(axis)
    return lax.ppermute(shard, axis, [(i, (i + by) % size) for i in range(size)])


def roll(v, by, axis):
    return pltpu.roll(v, by % v.shape[axis], axis)


def gather_modes(v):
    ahead = roll(v, -1, 1)
    out = {}
    for bz, a in ((0, v + ahead), (1, ahead - v)):
        up = roll(a, -1, 0)
        out[0, bz] = a + up
        out[1, bz] = up - a
    return out


def scatter_modes(r):
    part = []
    for bz in (0, 1):
        part.append((r[0, bz] - r[1, bz]) + roll(r[0, bz] + r[1, bz], 1, 0))
    return (part[0] - part[1]) + roll(part[0] + part[1], 1, 1)


def voxel_forces(c, stiff):
    lam = (LAMBDA_SOFT / 16) + (LAMBDA_RISE / 16) * stiff
    mu = (SHEAR_SOFT / 16) + (SHEAR_RISE / 16) * stiff
    mu2 = mu + mu
    lam3 = lam * (1.0 / 3)
    mu3 = mu * (1.0 / 3)
    top = ((LAMBDA_SOFT + 4 * SHEAR_SOFT) / 144) + ((LAMBDA_RISE + 4 * SHEAR_RISE) / 144) * stiff
    f = {}
    normal = ((0, 1, 0, 0), (1, 0, 1, 0), (2, 0, 0, 1))
    t = lam * (c[normal[0]] + c[normal[1]] + c[normal[2]])
    for p in normal:
        f[p] = t + mu2 * c[p]
    for p, q in (
        ((0, 1, 1, 0), (2, 0, 1, 1)),
        ((0, 1, 0, 1), (1, 0, 1, 1)),
        ((1, 1, 1, 0), (2, 1, 0, 1)),
    ):
        t = lam3 * (c[p] + c[q])
        f[p] = t + mu * c[p]
        f[q] = t + mu * c[q]
    for comp in range(3):
        p = (comp, 1, 1, 1)
        f[p] = top * c[p]
    for p, q in (
        ((0, 0, 1, 0), (1, 1, 0, 0)),
        ((0, 0, 0, 1), (2, 1, 0, 0)),
        ((1, 0, 0, 1), (2, 0, 1, 0)),
    ):
        f[p] = f[q] = mu * (c[p] + c[q])
    bend = ((0, 0, 1, 1), (1, 1, 0, 1), (2, 1, 1, 0))
    t = c[bend[0]] + c[bend[1]] + c[bend[2]]
    for p in bend:
        f[p] = mu3 * (t + c[p])
    return f


MODES = [(comp, by, bz) for comp in range(3) for by in (0, 1) for bz in (0, 1)]


def pairs(start, stop, body, carry):
    def two(i, carry):
        n = start + 2 * i
        return body(n + 1, body(n, carry))

    return lax.fori_loop(0, (stop - start + 1) // 2, two, carry)


def assemble(block, voxels, low, high, row, node_ref, cell_ref):
    h = HALO
    count = block.shape[1]
    tile = slice(row, row + block.shape[2])
    for i in range(h):
        for comp in range(3):
            node_ref[comp, i, tile] = low[comp * h + i]
            node_ref[comp, h + count + i, tile] = high[comp * h + i]
        cell_ref[h + 1 + count + i, tile] = high[3 * h + i]
    for i in range(h + 1):
        cell_ref[i, tile] = low[3 * h + i]

    def own(n, _):
        for comp in range(3):
            node_ref[comp, h + n, tile] = block[comp, n]
        cell_ref[h + 1 + n, tile] = voxels[n]
        return _

    pairs(0, count, own, 0)


def basis_kernel(
    r_own, lab_own, side_ref, edge_own, below, above, below_side, above_side,
    t_out, d_out, sums_out, r_ref, lab_ref, edge_ref, t_ref, inv_ref, q_ref, f_ref,
):
    planes, rows, depth = r_ref.shape[1:]
    own_x = planes - 2 * HALO
    own_y = rows - 2 * HALO
    lo, hi = HALO, HALO + own_x
    first_row = own_y + HALO

    assemble(r_own, lab_own, below, above, 0, r_ref, lab_ref)
    assemble(side_ref, side_ref.at[3], below_side, above_side, own_y, r_ref, lab_ref)
    edge_ref[0 : HALO + 1] = below_side[4 * HALO + 1, 0 : HALO + 1]
    edge_ref[lo + 1 : hi + 1] = edge_own[...]
    edge_ref[hi + 1 : hi + 1 + HALO] = above_side[4 * HALO, 0:HALO]

    base = 8 * (LAMBDA_SOFT + 4 * SHEAR_SOFT) / 9 + KAPPA
    rise = (LAMBDA_RISE + 4 * SHEAR_RISE) / 9
    row_id = lax.broadcasted_iota(jnp.int32, (rows, depth), 0)

    def layer(m):
        l = lab_ref[m]
        lz = l + roll(l, 1, 1)
        e = edge_ref[pl.ds(m, 1), :]
        ez = jnp.broadcast_to(e + roll(e, 1, 1), (rows, depth))
        return lz + jnp.where(row_id == first_row, ez, roll(lz, 1, 0))

    def start(own, n, before):
        here = layer(n + 1)
        diag = base + rise * (before + here)
        inv = 1.0 / diag
        inv_ref[n] = inv
        if own:
            d_out[n - lo] = diag[:own_y]
        for comp in range(3):
            t = r_ref[comp, n] * inv
            t_ref[0, comp, n] = t
            if own:
                t_out[0, comp, n - lo] = t[:own_y]
        return here

    before = pairs(0, lo, functools.partial(start, False), layer(0))
    before = pairs(lo, hi, functools.partial(start, True), before)
    pairs(hi, planes, functools.partial(start, False), before)

    tiles = [
        (slice(a, a + 8), slice(b, b + 128)) for a in range(0, rows, 8) for b in range(0, depth, 128)
    ]
    totals = []
    for k in range(ITERS):
        first, last = k, planes - k

        def forward(n, _):
            for comp in range(3):
                out = gather_modes(t_ref[k, comp, n])
                for i, (cc, by, bz) in enumerate(MODES):
                    if cc == comp:
                        for j, tile in enumerate(tiles):
                            q_ref[n, j, i] = out[by, bz][tile]
            return _

        pairs(first, last, forward, 0)

        for j, tile in enumerate(tiles):

            def voxels(n, carry):
                near, behind = carry
                far = [q_ref[n + 1, j, i] for i in range(len(MODES))]
                c = {}
                for i, (comp, by, bz) in enumerate(MODES):
                    if (by, bz) != (0, 0):
                        c[comp, 0, by, bz] = near[i] + far[i]
                    c[comp, 1, by, bz] = far[i] - near[i]
                f = voxel_forces(c, lab_ref[n + 1, tile[0], tile[1]])
                ahead = []
                for i, (comp, by, bz) in enumerate(MODES):
                    up = f[comp, 1, by, bz]
                    if (by, bz) != (0, 0):
                        flat = f[comp, 0, by, bz]
                        f_ref[n, j, i] = behind[i] + (flat - up)
                        ahead.append(flat + up)
                    else:
                        f_ref[n, j, i] = behind[i] - up
                        ahead.append(up)
                return far, ahead

            near = [q_ref[first, j, i] for i in range(len(MODES))]
            pairs(first, last - 1, voxels, (near, [jnp.zeros_like(v) for v in near]))

        def modes_at(n, comp):
            out = {}
            for i, (cc, by, bz) in enumerate(MODES):
                if cc == comp:
                    v = [f_ref[n, j, i] for j in range(len(tiles))]
                    across = depth // 128
                    out[by, bz] = jnp.concatenate(
                        [
                            jnp.concatenate(v[a * across : (a + 1) * across], 1)
                            for a in range(rows // 8)
                        ],
                        0,
                    )
            return out

        def advance(n, own, acc):
            acc = list(acc)
            inv = inv_ref[n]
            for comp in range(3):
                t = t_ref[k, comp, n]
                image = scatter_modes(modes_at(n, comp)) + KAPPA * t
                if own:
                    for j in range(k + 1):
                        acc[j] += t_ref[j, comp, n, :own_y] * image[:own_y]
                    acc[k + 1] += t[:own_y] * r_ref[comp, n, :own_y]
                new = image * inv
                if k == 1:
                    new = (new - CENTRE * t) * (1 / HALF)
                elif k > 1:
                    new = (new - CENTRE * t) * (2 / HALF) - t_ref[k - 1, comp, n]
                if k + 1 < ITERS:
                    t_ref[k + 1, comp, n] = new
                if own:
                    t_out[k + 1, comp, n - lo] = new[:own_y]
            return tuple(acc)

        def beside(i, _):
            advance(first + 1 + i, False, ())
            advance(hi + i, False, ())
            return _

        if k + 1 < ITERS:
            lax.fori_loop(0, lo - first - 1, beside, 0)
        zero = jnp.zeros((own_y, depth), jnp.float32)
        totals.extend(pairs(lo, hi, lambda n, c: advance(n, True, c), (zero,) * (k + 2)))

    lane = lax.broadcasted_iota(jnp.int32, (1, 128), 1)
    packed = jnp.zeros((1, 128), jnp.float32)
    for i, v in enumerate(totals):
        s = jnp.sum(jnp.sum(v, axis=0, keepdims=True), axis=1, keepdims=True)
        packed = jnp.where(lane == i, s, packed)
    sums_out[...] = jnp.broadcast_to(packed[None], sums_out.shape)


def pack_kernel(r_in, lab_in, r_out, lab_out, up_out, down_out, next_out, previous_out):
    h = HALO
    own_x, own_y = lab_in.shape[:2]

    def body(n, _):
        l = lab_in[n].astype(jnp.float32)
        lab_out[n] = l
        up_out[3 * own_x + n] = l[own_y - h :]
        up_out[4 * own_x + n // h, pl.ds(n % h, 1)] = l[own_y - h - 1 : own_y - h]
        down_out[3 * own_x + n] = l[:h]
        for comp in range(3):
            r = r_in[comp, n]
            r_out[comp, n] = r
            up_out[comp * own_x + n] = r[own_y - h :]
            down_out[comp * own_x + n] = r[:h]
        return _

    pairs(0, own_x, body, 0)
    for i in range(h):
        for comp in range(3):
            next_out[comp * h + i] = r_in[comp, own_x - h + i]
            previous_out[comp * h + i] = r_in[comp, i]
        previous_out[3 * h + i] = lab_in[i].astype(jnp.float32)
    for i in range(h + 1):
        next_out[3 * h + i] = lab_in[own_x - h - 1 + i].astype(jnp.float32)


def combine_kernel(sums_ref, t_ref, d_ref, x_out, r_out):
    total = jnp.sum(sums_ref[...], axis=0, keepdims=True)
    lane = lax.broadcasted_iota(jnp.int32, total.shape, 1)
    entry = [
        jnp.sum(jnp.where(lane == i, total, 0.0), axis=1, keepdims=True) for i in range(SUMS)
    ]
    gram, right = {}, []
    place = 0
    for k in range(ITERS):
        for j in range(k + 1):
            gram[j, k] = gram[k, j] = entry[place]
            place += 1
        right.append(entry[place])
        place += 1
    scale = [gram[k, k] for k in range(ITERS)]
    inv, low = [], {}
    for k in range(ITERS):
        pivot = gram[k, k]
        good = pivot > 1e-7 * scale[k]
        inv.append(jnp.where(good, 1.0 / jnp.where(good, pivot, 1.0), 0.0))
        for i in range(k + 1, ITERS):
            low[i, k] = gram[i, k] * inv[k]
        for i in range(k + 1, ITERS):
            for j in range(k + 1, i + 1):
                gram[i, j] = gram[j, i] = gram[i, j] - low[i, k] * gram[j, k]
            right[i] = right[i] - low[i, k] * right[k]
    y = [None] * ITERS
    for k in reversed(range(ITERS)):
        y[k] = right[k] * inv[k]
        for i in range(k + 1, ITERS):
            y[k] = y[k] - low[i, k] * y[i]
    e = [jnp.ones_like(y[0])] + [jnp.zeros_like(y[0]) for _ in range(ITERS)]
    for k in range(ITERS):
        if k == 0:
            e[1] = e[1] - y[0]
        elif k == 1:
            e[2] = e[2] - HALF * y[1]
            e[1] = e[1] - CENTRE * y[1]
        else:
            e[k + 1] = e[k + 1] - (HALF / 2) * y[k]
            e[k - 1] = e[k - 1] - (HALF / 2) * y[k]
            e[k] = e[k] - CENTRE * y[k]
    shape = d_ref.shape[1:]
    y = [jnp.broadcast_to(v, shape) for v in y]
    e = [jnp.broadcast_to(v, shape) for v in e]

    def body(n, _):
        diag = d_ref[n]
        for comp in range(3):
            t = [t_ref[k, comp, n] for k in range(ITERS + 1)]
            x, r = y[0] * t[0], e[0] * t[0]
            for k in range(1, ITERS):
                x = x + y[k] * t[k]
                r = r + e[k] * t[k]
            r = r + e[ITERS] * t[ITERS]
            x_out[comp, n] = x
            r_out[comp, n] = r * diag
        return _

    lax.fori_loop(0, d_ref.shape[0], body, 0)


def local(right_side, labels):
    own_x, own_y, depth = labels.shape
    h = HALO
    f32 = jnp.float32
    devices = lax.axis_size("gx") * lax.axis_size("gy")
    small = pltpu.CompilerParams(vmem_limit_bytes=16 * 2**20)
    right_side, lab, up, down, to_next, to_previous = pl.pallas_call(
        pack_kernel,
        out_shape=(
            jax.ShapeDtypeStruct(right_side.shape, f32),
            jax.ShapeDtypeStruct(labels.shape, f32),
            jax.ShapeDtypeStruct((4 * own_x + own_x // h, h, depth), f32),
            jax.ShapeDtypeStruct((4 * own_x, h, depth), f32),
            jax.ShapeDtypeStruct((4 * h + 1, own_y, depth), f32),
            jax.ShapeDtypeStruct((4 * h, own_y, depth), f32),
        ),
        compiler_params=small,
        name="pack",
    )(right_side, labels)

    from_minus = shifted(up, "gy", 1)
    from_plus = shifted(down, "gy", -1)
    below = shifted(to_next, "gx", 1)
    above = shifted(to_previous, "gx", -1)

    side = jnp.concatenate(
        [
            from_plus.reshape(4, own_x, h, depth),
            from_minus[: 4 * own_x].reshape(4, own_x, h, depth),
        ],
        2,
    )
    edge = from_minus[4 * own_x :].reshape(own_x, depth)

    def block(start, voxel_start, stop):
        rows = edge[voxel_start:stop]
        return jnp.concatenate(
            [
                side[:3, start:stop].reshape(3 * h, 2 * h, depth),
                side[3, voxel_start:stop],
                jnp.pad(rows, ((0, 2 * h - rows.shape[0]), (0, 0)))[None],
            ],
            0,
        )

    below_side = shifted(block(own_x - h, own_x - h - 1, own_x), "gx", 1)
    above_side = shifted(block(0, 0, h), "gx", -1)

    planes, rows = own_x + 2 * h, own_y + 2 * h
    tiles = (rows // 8) * (depth // 128)
    basis, diagonal, sums = pl.pallas_call(
        basis_kernel,
        out_shape=(
            jax.ShapeDtypeStruct((ITERS + 1, 3, own_x, own_y, depth), f32),
            jax.ShapeDtypeStruct((own_x, own_y, depth), f32),
            jax.ShapeDtypeStruct((devices, 1, 128), f32),
        ),
        scratch_shapes=[
            pltpu.VMEM((3, planes, rows, depth), f32),
            pltpu.VMEM((planes + 1, rows, depth), f32),
            pltpu.VMEM((planes + 8, depth), f32),
            pltpu.VMEM((ITERS, 3, planes, rows, depth), f32),
            pltpu.VMEM((planes, rows, depth), f32),
            pltpu.VMEM((planes + 1, tiles, len(MODES), 8, 128), f32),
            pltpu.VMEM((planes + 1, tiles, len(MODES), 8, 128), f32),
        ],
        compiler_params=pltpu.CompilerParams(vmem_limit_bytes=32 * 2**20),
        name="basis",
    )(right_side, lab, side, edge, below, above, below_side, above_side)

    everyone = lax.all_to_all(sums, ("gx", "gy"), 0, 0)
    out = jax.ShapeDtypeStruct(right_side.shape, f32)
    return pl.pallas_call(combine_kernel, out_shape=(out, out), compiler_params=small, name="combine")(
        everyone.reshape(devices, 128), basis, diagonal
    )


def solution(mesh):
    in_specs = (P(None, "gx", "gy", None), P("gx", "gy", None))
    out_specs = (P(None, "gx", "gy", None), P(None, "gx", "gy", None))
    return jax.shard_map(local, mesh=mesh, in_specs=in_specs, out_specs=out_specs, check_vma=False)
```

```python
import functools

import jax
import jax.numpy as jnp
from jax import lax
from jax.experimental import pallas as pl
from jax.experimental.pallas import tpu as pltpu
from jax.sharding import PartitionSpec as P


ITERS = 4
HALO = ITERS
LAMBDA_SOFT = 0.5769231
LAMBDA_RISE = 1.6452991
SHEAR_SOFT = 0.3846154
SHEAR_RISE = 2.9487179
KAPPA = 0.05
CENTRE = 0.5 * (0.5 + 2.6)
HALF = 0.5 * (2.6 - 0.5)
SUMS = 14
WIDTH = 4


def shifted(shard, axis, by):
    size = lax.axis_size(axis)
    return lax.ppermute(shard, axis, [(i, (i + by) % size) for i in range(size)])


def roll(v, by, axis):
    return pltpu.roll(v, by % v.shape[axis], axis)


def gather_modes(v, ahead):
    out = {}
    for bz, a in ((0, v + ahead), (1, ahead - v)):
        up = roll(a, -1, 0)
        out[0, bz] = a + up
        out[1, bz] = up - a
    return out


def scatter_modes(r):
    part = []
    for bz in (0, 1):
        part.append((r[0, bz] - r[1, bz]) + roll(r[0, bz] + r[1, bz], 1, 0))
    return part[0] - part[1], part[0] + part[1]


def voxel_forces(c, stiff):
    lam = (LAMBDA_SOFT / 16) + (LAMBDA_RISE / 16) * stiff
    mu = (SHEAR_SOFT / 16) + (SHEAR_RISE / 16) * stiff
    mu2 = mu + mu
    lam3 = lam * (1.0 / 3)
    mu3 = mu * (1.0 / 3)
    top = ((LAMBDA_SOFT + 4 * SHEAR_SOFT) / 144) + ((LAMBDA_RISE + 4 * SHEAR_RISE) / 144) * stiff
    f = {}
    normal = ((0, 1, 0, 0), (1, 0, 1, 0), (2, 0, 0, 1))
    t = lam * (c[normal[0]] + c[normal[1]] + c[normal[2]])
    for p in normal:
        f[p] = t + mu2 * c[p]
    for p, q in (
        ((0, 1, 1, 0), (2, 0, 1, 1)),
        ((0, 1, 0, 1), (1, 0, 1, 1)),
        ((1, 1, 1, 0), (2, 1, 0, 1)),
    ):
        t = lam3 * (c[p] + c[q])
        f[p] = t + mu * c[p]
        f[q] = t + mu * c[q]
    for comp in range(3):
        p = (comp, 1, 1, 1)
        f[p] = top * c[p]
    for p, q in (
        ((0, 0, 1, 0), (1, 1, 0, 0)),
        ((0, 0, 0, 1), (2, 1, 0, 0)),
        ((1, 0, 0, 1), (2, 0, 1, 0)),
    ):
        f[p] = f[q] = mu * (c[p] + c[q])
    bend = ((0, 0, 1, 1), (1, 1, 0, 1), (2, 1, 1, 0))
    t = c[bend[0]] + c[bend[1]] + c[bend[2]]
    for p in bend:
        f[p] = mu3 * (t + c[p])
    return f


MODES = [(comp, by, bz) for comp in range(3) for by in (0, 1) for bz in (0, 1)]


def strides(start, stop, width, body, carry):
    def several(i, carry):
        return body(start + width * i, carry)

    return lax.fori_loop(0, -((start - stop) // width), several, carry)


def pairs(start, stop, body, carry):
    return strides(start, stop, 2, lambda n, c: body(n + 1, body(n, c)), carry)


def assemble(block, voxels, low, high, row, node_ref, cell_ref):
    h = HALO
    count = block.shape[1]
    tile = slice(row, row + block.shape[2])
    for i in range(h):
        for comp in range(3):
            node_ref[comp, i, tile] = low[comp * h + i]
            node_ref[comp, h + count + i, tile] = high[comp * h + i]
        cell_ref[h + 1 + count + i, tile] = high[3 * h + i]
    for i in range(h + 1):
        cell_ref[i, tile] = low[3 * h + i]

    def own(n, _):
        for comp in range(3):
            node_ref[comp, h + n, tile] = block[comp, n]
        cell_ref[h + 1 + n, tile] = voxels[n]
        return _

    pairs(0, count, own, 0)


def basis_kernel(
    r_own, lab_own, side_ref, edge_own, below, above, below_side, above_side,
    t_out, d_out, sums_out, r_ref, lab_ref, edge_ref, t_ref, inv_ref, turn_ref, image_ref, q_ref, f_ref,
):
    planes, rows, depth = r_ref.shape[1:]
    own_x = planes - 2 * HALO
    own_y = rows - 2 * HALO
    lo, hi = HALO, HALO + own_x
    first_row = own_y + HALO

    assemble(r_own, lab_own, below, above, 0, r_ref, lab_ref)
    assemble(side_ref, side_ref.at[3], below_side, above_side, own_y, r_ref, lab_ref)
    edge_ref[0 : HALO + 1] = below_side[4 * HALO + 1, 0 : HALO + 1]
    edge_ref[lo + 1 : hi + 1] = edge_own[...]
    edge_ref[hi + 1 : hi + 1 + HALO] = above_side[4 * HALO, 0:HALO]

    base = 8 * (LAMBDA_SOFT + 4 * SHEAR_SOFT) / 9 + KAPPA
    rise = (LAMBDA_RISE + 4 * SHEAR_RISE) / 9
    row_id = lax.broadcasted_iota(jnp.int32, (rows, depth), 0)

    edges = edge_ref[...]
    edge_ref[...] = edges + roll(edges, 1, 1)

    for m in range(planes + 1):
        turn_ref[0, m] = roll(lab_ref[m], 1, 1)

    def layer(m):
        lz = lab_ref[m] + turn_ref[0, m]
        ez = jnp.broadcast_to(edge_ref[pl.ds(m, 1), :], (rows, depth))
        return lz + jnp.where(row_id == first_row, ez, roll(lz, 1, 0))

    def start(own, n, before):
        here = layer(n + 1)
        diag = base + rise * (before + here)
        inv = 1.0 / diag
        inv_ref[n] = inv
        if own:
            d_out[n - lo] = diag[:own_y]
        for comp in range(3):
            t = r_ref[comp, n] * inv
            t_ref[0, comp, n] = t
            if own:
                t_out[0, comp, n - lo] = t[:own_y]
        return here

    before = pairs(0, lo, functools.partial(start, False), layer(0))
    before = pairs(lo, hi, functools.partial(start, True), before)
    pairs(hi, planes, functools.partial(start, False), before)

    tiles = [
        (slice(a, a + 8), slice(b, b + 128)) for a in range(0, rows, 8) for b in range(0, depth, 128)
    ]
    totals = []
    for k in range(ITERS):
        first, last = k, planes - k

        def turn(n):
            for u in range(WIDTH):
                for comp in range(3):
                    turn_ref[comp, n + u] = roll(t_ref[k, comp, n + u], -1, 1)

        def forward(n, _):
            turn(n + WIDTH)
            for u in range(WIDTH):
                for comp in range(3):
                    out = gather_modes(t_ref[k, comp, n + u], turn_ref[comp, n + u])
                    for i, (cc, by, bz) in enumerate(MODES):
                        if cc == comp:
                            for j, tile in enumerate(tiles):
                                q_ref[n + u, i, j] = out[by, bz][tile]
            return _

        turn(first)
        strides(first, last, WIDTH, forward, 0)

        for j, tile in enumerate(tiles):

            def voxels(n, carry):
                near, behind = carry
                far = [q_ref[n + 1, i, j] for i in range(len(MODES))]
                c = {}
                for i, (comp, by, bz) in enumerate(MODES):
                    if (by, bz) != (0, 0):
                        c[comp, 0, by, bz] = near[i] + far[i]
                    c[comp, 1, by, bz] = far[i] - near[i]
                f = voxel_forces(c, lab_ref[n + 1, tile[0], tile[1]])
                ahead = []
                for i, (comp, by, bz) in enumerate(MODES):
                    up = f[comp, 1, by, bz]
                    if (by, bz) != (0, 0):
                        flat = f[comp, 0, by, bz]
                        f_ref[n, i, j] = behind[i] + (flat - up)
                        ahead.append(flat + up)
                    else:
                        f_ref[n, i, j] = behind[i] - up
                        ahead.append(up)
                return far, ahead

            near = [q_ref[first, i, j] for i in range(len(MODES))]
            pairs(first, last - 1, voxels, (near, [jnp.zeros_like(v) for v in near]))

        def modes_at(n, comp):
            out = {}
            for i, (cc, by, bz) in enumerate(MODES):
                if cc == comp:
                    v = [f_ref[n, i, j] for j in range(len(tiles))]
                    across = depth // 128
                    out[by, bz] = jnp.concatenate(
                        [
                            jnp.concatenate(v[a * across : (a + 1) * across], 1)
                            for a in range(rows // 8)
                        ],
                        0,
                    )
            return out

        def collect(n):
            for comp in range(3):
                kept, moved = scatter_modes(modes_at(n, comp))
                image_ref[comp, n] = kept + roll(moved, 1, 1)

        def advance(n, own, acc):
            acc = list(acc)
            inv = inv_ref[n]
            for comp in range(3):
                t = t_ref[k, comp, n]
                image = image_ref[comp, n] + KAPPA * t
                if own:
                    for j in range(k + 1):
                        acc[j] += t_ref[j, comp, n, :own_y] * image[:own_y]
                    acc[k + 1] += t[:own_y] * r_ref[comp, n, :own_y]
                new = image * inv
                if k == 1:
                    new = (new - CENTRE * t) * (1 / HALF)
                elif k > 1:
                    new = (new - CENTRE * t) * (2 / HALF) - t_ref[k - 1, comp, n]
                if k + 1 < ITERS:
                    t_ref[k + 1, comp, n] = new
                if own:
                    t_out[k + 1, comp, n - lo] = new[:own_y]
            return tuple(acc)

        def own_planes(n, acc):
            for u in range(WIDTH):
                collect(n + WIDTH + u)
            for u in range(WIDTH):
                acc = advance(n + u, True, acc)
            return acc

        beside = [*range(first + 1, lo), *range(hi, last - 1)] if k + 1 < ITERS else []
        for n in [*beside, *range(lo, lo + WIDTH)]:
            collect(n)
        for n in beside:
            advance(n, False, ())
        zero = jnp.zeros((own_y, depth), jnp.float32)
        totals.extend(strides(lo, hi, WIDTH, own_planes, (zero,) * (k + 2)))

    lane = lax.broadcasted_iota(jnp.int32, (1, 128), 1)
    packed = jnp.zeros((1, 128), jnp.float32)
    for i, v in enumerate(totals):
        s = jnp.sum(jnp.sum(v, axis=0, keepdims=True), axis=1, keepdims=True)
        packed = jnp.where(lane == i, s, packed)
    sums_out[...] = jnp.broadcast_to(packed[None], sums_out.shape)


def pack_kernel(
    r_hbm, lab_hbm, r_out, lab_out, up_out, down_out, next_out, previous_out, lab_in, arrived
):
    h = HALO
    own_x, own_y = lab_in.shape[:2]
    copies = [
        pltpu.make_async_copy(r_hbm, r_out, arrived.at[0]),
        pltpu.make_async_copy(lab_hbm, lab_in, arrived.at[1]),
    ]
    for copy in copies:
        copy.start()
    for copy in copies:
        copy.wait()

    def body(n, _):
        l = lab_in[n].astype(jnp.float32)
        lab_out[n] = l
        up_out[3 * own_x + n] = l[own_y - h :]
        up_out[4 * own_x + n // h, pl.ds(n % h, 1)] = l[own_y - h - 1 : own_y - h]
        down_out[3 * own_x + n] = l[:h]
        for comp in range(3):
            r = r_out[comp, n]
            up_out[comp * own_x + n] = r[own_y - h :]
            down_out[comp * own_x + n] = r[:h]
        return _

    pairs(0, own_x, body, 0)
    for i in range(h):
        for comp in range(3):
            next_out[comp * h + i] = r_out[comp, own_x - h + i]
            previous_out[comp * h + i] = r_out[comp, i]
        previous_out[3 * h + i] = lab_in[i].astype(jnp.float32)
    for i in range(h + 1):
        next_out[3 * h + i] = lab_in[own_x - h - 1 + i].astype(jnp.float32)


def combine_kernel(sums_ref, t_ref, d_ref, x_out, r_out):
    total = jnp.sum(sums_ref[...], axis=0, keepdims=True)
    lane = lax.broadcasted_iota(jnp.int32, total.shape, 1)
    entry = [
        jnp.sum(jnp.where(lane == i, total, 0.0), axis=1, keepdims=True) for i in range(SUMS)
    ]
    gram, right = {}, []
    place = 0
    for k in range(ITERS):
        for j in range(k + 1):
            gram[j, k] = gram[k, j] = entry[place]
            place += 1
        right.append(entry[place])
        place += 1
    scale = [gram[k, k] for k in range(ITERS)]
    inv, low = [], {}
    for k in range(ITERS):
        pivot = gram[k, k]
        good = pivot > 1e-7 * scale[k]
        inv.append(jnp.where(good, 1.0 / jnp.where(good, pivot, 1.0), 0.0))
        for i in range(k + 1, ITERS):
            low[i, k] = gram[i, k] * inv[k]
        for i in range(k + 1, ITERS):
            for j in range(k + 1, i + 1):
                gram[i, j] = gram[j, i] = gram[i, j] - low[i, k] * gram[j, k]
            right[i] = right[i] - low[i, k] * right[k]
    y = [None] * ITERS
    for k in reversed(range(ITERS)):
        y[k] = right[k] * inv[k]
        for i in range(k + 1, ITERS):
            y[k] = y[k] - low[i, k] * y[i]
    e = [jnp.ones_like(y[0])] + [jnp.zeros_like(y[0]) for _ in range(ITERS)]
    for k in range(ITERS):
        if k == 0:
            e[1] = e[1] - y[0]
        elif k == 1:
            e[2] = e[2] - HALF * y[1]
            e[1] = e[1] - CENTRE * y[1]
        else:
            e[k + 1] = e[k + 1] - (HALF / 2) * y[k]
            e[k - 1] = e[k - 1] - (HALF / 2) * y[k]
            e[k] = e[k] - CENTRE * y[k]
    shape = d_ref.shape[1:]
    y = [jnp.broadcast_to(v, shape) for v in y]
    e = [jnp.broadcast_to(v, shape) for v in e]

    def body(n, _):
        diag = d_ref[n]
        for comp in range(3):
            t = [t_ref[k, comp, n] for k in range(ITERS + 1)]
            x, r = y[0] * t[0], e[0] * t[0]
            for k in range(1, ITERS):
                x = x + y[k] * t[k]
                r = r + e[k] * t[k]
            r = r + e[ITERS] * t[ITERS]
            x_out[comp, n] = x
            r_out[comp, n] = r * diag
        return _

    lax.fori_loop(0, d_ref.shape[0], body, 0)


def local(right_side, labels):
    own_x, own_y, depth = labels.shape
    h = HALO
    f32 = jnp.float32
    devices = lax.axis_size("gx") * lax.axis_size("gy")
    small = pltpu.CompilerParams(vmem_limit_bytes=16 * 2**20)
    right_side, lab, up, down, to_next, to_previous = pl.pallas_call(
        pack_kernel,
        out_shape=(
            jax.ShapeDtypeStruct(right_side.shape, f32),
            jax.ShapeDtypeStruct(labels.shape, f32),
            jax.ShapeDtypeStruct((4 * own_x + own_x // h, h, depth), f32),
            jax.ShapeDtypeStruct((4 * own_x, h, depth), f32),
            jax.ShapeDtypeStruct((4 * h + 1, own_y, depth), f32),
            jax.ShapeDtypeStruct((4 * h, own_y, depth), f32),
        ),
        in_specs=[pl.BlockSpec(memory_space=pltpu.HBM)] * 2,
        scratch_shapes=[pltpu.VMEM(labels.shape, jnp.int32), pltpu.SemaphoreType.DMA((2,))],
        compiler_params=small,
        name="pack",
    )(right_side, labels)

    from_minus = shifted(up, "gy", 1)
    from_plus = shifted(down, "gy", -1)
    below = shifted(to_next, "gx", 1)
    above = shifted(to_previous, "gx", -1)

    from_minus, from_plus, below, above = lax.optimization_barrier(
        (from_minus, from_plus, below, above)
    )

    side = jnp.concatenate(
        [
            from_plus.reshape(4, own_x, h, depth),
            from_minus[: 4 * own_x].reshape(4, own_x, h, depth),
        ],
        2,
    )
    edge = from_minus[4 * own_x :].reshape(own_x, depth)

    def block(start, voxel_start, stop):
        rows = edge[voxel_start:stop]
        return jnp.concatenate(
            [
                side[:3, start:stop].reshape(3 * h, 2 * h, depth),
                side[3, voxel_start:stop],
                jnp.pad(rows, ((0, 2 * h - rows.shape[0]), (0, 0)))[None],
            ],
            0,
        )

    below_side = shifted(block(own_x - h, own_x - h - 1, own_x), "gx", 1)
    above_side = shifted(block(0, 0, h), "gx", -1)

    planes, rows = own_x + 2 * h, own_y + 2 * h
    tiles = (rows // 8) * (depth // 128)
    basis, diagonal, sums = pl.pallas_call(
        basis_kernel,
        out_shape=(
            jax.ShapeDtypeStruct((ITERS + 1, 3, own_x, own_y, depth), f32),
            jax.ShapeDtypeStruct((own_x, own_y, depth), f32),
            jax.ShapeDtypeStruct((devices, 1, 128), f32),
        ),
        scratch_shapes=[
            pltpu.VMEM((3, planes, rows, depth), f32),
            pltpu.VMEM((planes + 1, rows, depth), f32),
            pltpu.VMEM((planes + 8, depth), f32),
            pltpu.VMEM((ITERS, 3, planes + 2 * WIDTH, rows, depth), f32),
            pltpu.VMEM((planes, rows, depth), f32),
            pltpu.VMEM((3, planes + 2 * WIDTH, rows, depth), f32),
            pltpu.VMEM((3, planes, rows, depth), f32),
            pltpu.VMEM((planes + WIDTH, len(MODES), tiles + 1, 8, 128), f32),
            pltpu.VMEM((planes + WIDTH, len(MODES), tiles + 1, 8, 128), f32),
        ],
        compiler_params=pltpu.CompilerParams(vmem_limit_bytes=32 * 2**20),
        name="basis",
    )(right_side, lab, side, edge, below, above, below_side, above_side)

    everyone = lax.all_to_all(sums, ("gx", "gy"), 0, 0)
    out = jax.ShapeDtypeStruct(right_side.shape, f32)
    return pl.pallas_call(combine_kernel, out_shape=(out, out), compiler_params=small, name="combine")(
        everyone.reshape(devices, 128), basis, diagonal
    )


def solution(mesh):
    in_specs = (P(None, "gx", "gy", None), P("gx", "gy", None))
    out_specs = (P(None, "gx", "gy", None), P(None, "gx", "gy", None))
    return jax.shard_map(local, mesh=mesh, in_specs=in_specs, out_specs=out_specs, check_vma=False)
```

```python
import functools

import jax
import jax.numpy as jnp
from jax import lax
from jax.experimental import pallas as pl
from jax.experimental.pallas import tpu as pltpu
from jax.sharding import PartitionSpec as P


ITERS = 4
HALO = ITERS
LAMBDA_SOFT = 0.5769231
LAMBDA_RISE = 1.6452991
SHEAR_SOFT = 0.3846154
SHEAR_RISE = 2.9487179
KAPPA = 0.05
CENTRE = 0.5 * (0.5 + 2.6)
HALF = 0.5 * (2.6 - 0.5)
SUMS = 14
WIDTH = 4


def shifted(shard, axis, by):
    size = lax.axis_size(axis)
    return lax.ppermute(shard, axis, [(i, (i + by) % size) for i in range(size)])


def roll(v, by, axis):
    return pltpu.roll(v, by % v.shape[axis], axis)


def gather_modes(v, ahead):
    out = {}
    for bz, a in ((0, v + ahead), (1, ahead - v)):
        up = roll(a, -1, 0)
        out[0, bz] = a + up
        out[1, bz] = up - a
    return out


def scatter_modes(r):
    part = []
    for bz in (0, 1):
        part.append((r[0, bz] - r[1, bz]) + roll(r[0, bz] + r[1, bz], 1, 0))
    return part[0] - part[1], part[0] + part[1]


def voxel_forces(c, stiff):
    lam = (LAMBDA_SOFT / 16) + (LAMBDA_RISE / 16) * stiff
    mu = (SHEAR_SOFT / 16) + (SHEAR_RISE / 16) * stiff
    mu2 = mu + mu
    lam3 = lam * (1.0 / 3)
    mu3 = mu * (1.0 / 3)
    top = ((LAMBDA_SOFT + 4 * SHEAR_SOFT) / 144) + ((LAMBDA_RISE + 4 * SHEAR_RISE) / 144) * stiff
    f = {}
    normal = ((0, 1, 0, 0), (1, 0, 1, 0), (2, 0, 0, 1))
    t = lam * (c[normal[0]] + c[normal[1]] + c[normal[2]])
    for p in normal:
        f[p] = t + mu2 * c[p]
    for p, q in (
        ((0, 1, 1, 0), (2, 0, 1, 1)),
        ((0, 1, 0, 1), (1, 0, 1, 1)),
        ((1, 1, 1, 0), (2, 1, 0, 1)),
    ):
        t = lam3 * (c[p] + c[q])
        f[p] = t + mu * c[p]
        f[q] = t + mu * c[q]
    for comp in range(3):
        p = (comp, 1, 1, 1)
        f[p] = top * c[p]
    for p, q in (
        ((0, 0, 1, 0), (1, 1, 0, 0)),
        ((0, 0, 0, 1), (2, 1, 0, 0)),
        ((1, 0, 0, 1), (2, 0, 1, 0)),
    ):
        f[p] = f[q] = mu * (c[p] + c[q])
    bend = ((0, 0, 1, 1), (1, 1, 0, 1), (2, 1, 1, 0))
    t = c[bend[0]] + c[bend[1]] + c[bend[2]]
    for p in bend:
        f[p] = mu3 * (t + c[p])
    return f


MODES = [(comp, by, bz) for comp in range(3) for by in (0, 1) for bz in (0, 1)]


def strides(start, stop, width, body, carry):
    def several(i, carry):
        return body(start + width * i, carry)

    return lax.fori_loop(0, -((start - stop) // width), several, carry)


def pairs(start, stop, body, carry):
    return strides(start, stop, 2, lambda n, c: body(n + 1, body(n, c)), carry)


def tiles_of(rows, depth):
    return [(slice(a, a + 8), slice(b, b + 128)) for a in range(0, rows, 8) for b in range(0, depth, 128)]


def diagonal_layer(cells, turned, edge, first_row):
    lz = cells + turned
    row_id = lax.broadcasted_iota(jnp.int32, lz.shape, 0)
    return lz + jnp.where(row_id == first_row, jnp.broadcast_to(edge, lz.shape), roll(lz, 1, 0))


def diagonal_from(two_layers):
    base = 8 * (LAMBDA_SOFT + 4 * SHEAR_SOFT) / 9 + KAPPA
    return base + ((LAMBDA_RISE + 4 * SHEAR_RISE) / 9) * two_layers


def forward_planes(first, last, width, node_ref, turn_ref, q_ref):
    tiles = tiles_of(*node_ref.shape[2:])

    def turn(n):
        for u in range(width):
            for comp in range(3):
                turn_ref[comp, n + u] = roll(node_ref[comp, n + u], -1, 1)

    def forward(n, _):
        turn(n + width)
        for u in range(width):
            for comp in range(3):
                out = gather_modes(node_ref[comp, n + u], turn_ref[comp, n + u])
                for i, (cc, by, bz) in enumerate(MODES):
                    if cc == comp:
                        for j, tile in enumerate(tiles):
                            q_ref[n + u, i, j] = out[by, bz][tile]
        return _

    turn(first)
    strides(first, last, width, forward, 0)


def voxel_layers(j, first, last, cells_at, q_ref, f_ref):
    def voxels(n, carry):
        near, behind = carry
        far = [q_ref[n + 1, i, j] for i in range(len(MODES))]
        c = {}
        for i, (comp, by, bz) in enumerate(MODES):
            if (by, bz) != (0, 0):
                c[comp, 0, by, bz] = near[i] + far[i]
            c[comp, 1, by, bz] = far[i] - near[i]
        f = voxel_forces(c, cells_at(n))
        ahead = []
        for i, (comp, by, bz) in enumerate(MODES):
            up = f[comp, 1, by, bz]
            if (by, bz) != (0, 0):
                flat = f[comp, 0, by, bz]
                f_ref[n, i, j] = behind[i] + (flat - up)
                ahead.append(flat + up)
            else:
                f_ref[n, i, j] = behind[i] - up
                ahead.append(up)
        return far, ahead

    near = [q_ref[first, i, j] for i in range(len(MODES))]
    pairs(first, last, voxels, (near, [jnp.zeros_like(v) for v in near]))


def collect(n, f_ref, image_ref):
    rows, depth = image_ref.shape[2:]
    across = depth // 128
    for comp in range(3):
        modes = {}
        for i, (cc, by, bz) in enumerate(MODES):
            if cc == comp:
                v = [f_ref[n, i, j] for j in range((rows // 8) * across)]
                lines = [jnp.concatenate(v[a : a + across], 1) for a in range(0, len(v), across)]
                modes[by, bz] = jnp.concatenate(lines, 0)
        kept, moved = scatter_modes(modes)
        image_ref[comp, n] = kept + roll(moved, 1, 1)


def next_basis(k, image, t, inv, older):
    new = image * inv
    if k == 1:
        new = (new - CENTRE * t) * (1 / HALF)
    elif k > 1:
        new = (new - CENTRE * t) * (2 / HALF) - older()
    return new


def packed_sums(totals):
    lane = lax.broadcasted_iota(jnp.int32, (1, 128), 1)
    packed = jnp.zeros((1, 128), jnp.float32)
    for i, v in enumerate(totals):
        s = jnp.sum(jnp.sum(v, axis=0, keepdims=True), axis=1, keepdims=True)
        packed = jnp.where(lane == i, s, packed)
    return packed


def inside_kernel(
    r_own, lab_own, side_ref, edge_own,
    t_out, d_out, inv_out, edge_out, sums_out,
    t_ref, edge_ref, turn_ref, image_ref, q_ref, f_ref,
):
    own_x, own_y, depth = r_own.shape[1:]
    rows = own_y + side_ref.shape[2]
    tiles = tiles_of(rows, depth)
    count = own_x - 1

    def both(block, side):
        return jnp.concatenate([block, side], 0)

    edges = edge_own[...]
    edge_ref[...] = edges + roll(edges, 1, 1)
    for m in range(own_x):
        turn_ref[0, m] = roll(both(lab_own[m], side_ref[3, m]), 1, 1)

    def layer(m):
        cells = both(lab_own[m], side_ref[3, m])
        return diagonal_layer(cells, turn_ref[0, m], edge_ref[pl.ds(m, 1), :], own_y + HALO)

    def start(p, before):
        here = layer(p + 1)
        diag = diagonal_from(before + here)
        inv = 1.0 / diag
        inv_out[p + 1] = inv
        d_out[p + 1] = diag[:own_y]
        for comp in range(3):
            t = both(r_own[comp, p + 1], side_ref[comp, p + 1]) * inv
            t_ref[0, comp, p] = t
            t_out[0, comp, p + 1] = t[:own_y]
        return here

    before = pairs(0, count - 1, start, layer(0))
    start(count - 1, before)

    totals = []
    for k in range(ITERS):
        first, last = k, count - k
        for i, p in enumerate((first, first + 1, last - 2, last - 1)):
            for comp in range(3):
                edge_out[k, comp, i] = t_ref[k, comp, p]
        forward_planes(first, last, WIDTH, t_ref.at[k], turn_ref, q_ref)
        for j, (line, lanes) in enumerate(tiles):

            def cells_at(n):
                if line.start < own_y:
                    return lab_own[n + 1, line, lanes]
                return side_ref[3, n + 1, line.start - own_y : line.stop - own_y, lanes]

            voxel_layers(j, first, last - 1, cells_at, q_ref, f_ref)

        def advance(p, acc):
            acc = list(acc)
            inv = inv_out[p + 1]
            for comp in range(3):
                t = t_ref[k, comp, p]
                image = image_ref[comp, p] + KAPPA * t
                for j in range(k + 1):
                    acc[j] += t_ref[j, comp, p, :own_y] * image[:own_y]
                acc[k + 1] += t[:own_y] * r_own[comp, p + 1]
                new = next_basis(k, image, t, inv, lambda: t_ref[k - 1, comp, p])
                if k + 1 < ITERS:
                    t_ref[k + 1, comp, p] = new
                t_out[k + 1, comp, p + 1] = new[:own_y]
            return tuple(acc)

        def several(n, acc):
            for u in range(WIDTH):
                collect(n + WIDTH + u, f_ref, image_ref)
            for u in range(WIDTH):
                acc = advance(n + u, acc)
            return acc

        begin, end = first + 1, last - 1
        whole = begin + (end - begin) // WIDTH * WIDTH
        for p in range(begin, begin + WIDTH):
            collect(p, f_ref, image_ref)
        acc = (jnp.zeros((own_y, depth), jnp.float32),) * (k + 2)
        acc = strides(begin, whole, WIDTH, several, acc)
        for p in range(whole, end):
            acc = advance(p, acc)
        totals.extend(acc)
    sums_out[...] = packed_sums(totals)


def finish_kernel(
    r_own, lab_own, side_ref, edge_own, below, above, below_side, above_side,
    t_in, inv_in, edge_in, sums_in,
    t_out, d_out, sums_out,
    u_ref, cell_ref, inv_ref, turn_ref, image_ref, q_ref, f_ref,
):
    h = HALO
    own_x, own_y, depth = r_own.shape[1:]
    rows = own_y + side_ref.shape[2]
    tiles = tiles_of(rows, depth)
    left, right = h + 3, h + 2

    def nodes(comp, x):
        if x < 0:
            return jnp.concatenate([below[comp * h + h + x], below_side[comp * h + h + x]], 0)
        if x >= own_x:
            i = comp * h + x - own_x
            return jnp.concatenate([above[i], above_side[i]], 0)
        return jnp.concatenate([r_own[comp, x], side_ref[comp, x]], 0)

    def cells(x):
        if x < 0:
            i = 3 * h + h + 1 + x
            return jnp.concatenate([below[i], below_side[i]], 0)
        if x >= own_x:
            i = 3 * h + x - own_x
            return jnp.concatenate([above[i], above_side[i]], 0)
        return jnp.concatenate([lab_own[x], side_ref[3, x]], 0)

    def edge(x):
        if x < 0:
            return below_side[4 * h + 1, h + 1 + x : h + 2 + x]
        if x >= own_x:
            return above_side[4 * h, x - own_x : x - own_x + 1]
        return edge_own[x : x + 1]

    for x in [*range(-h - 1, ITERS + 1), *range(own_x - 1 - ITERS, own_x + h)]:
        cell_ref[x + h + 1] = cells(x)

    def layer(x):
        e = edge(x)
        c = cell_ref[x + h + 1]
        return diagonal_layer(c, roll(c, 1, 1), e + roll(e, 1, 1), own_y + h)

    def place(k, x):
        return x - (k - h) if x < own_x // 2 else left + x - (own_x - 2 - k)

    for start, stop in ((-h, 1), (own_x, own_x + h)):
        layers = [layer(x) for x in range(start - 1, stop)]
        for x in range(start, stop):
            diag = diagonal_from(layers[x - start] + layers[x - start + 1])
            inv = 1.0 / diag
            inv_ref[x + h] = inv
            if x == 0:
                d_out[...] = diag[:own_y]
            for comp in range(3):
                t = nodes(comp, x) * inv
                u_ref[0, comp, place(0, x)] = t
                if x == 0:
                    t_out[0, comp, 0] = t[:own_y]
    for x in [*range(1, ITERS + 1), *range(own_x - ITERS, own_x)]:
        inv_ref[x + h] = inv_in[x]

    def own_rows(j, comp, x):
        ref = t_out if x <= j or x >= own_x - j else t_in
        return ref[j, comp, x]

    totals = []
    for k in range(ITERS):
        for comp in range(3):
            for i, p in enumerate((left - 2, left - 1, left, left + 1)):
                u_ref[k, comp, p] = edge_in[k, comp, i]
        forward_planes(0, left + right, left, u_ref.at[k], turn_ref, q_ref)
        for j, (line, lanes) in enumerate(tiles):
            voxel_layers(j, 0, left - 1, lambda n: cell_ref[n + k + 1, line, lanes], q_ref, f_ref)
            shift = own_x - 2 - k - left + h + 1
            voxel_layers(
                j, left, left + right - 1, lambda n: cell_ref[n + shift, line, lanes], q_ref, f_ref
            )
        planes = [*range(k - h + 1, k + 2), *range(own_x - 1 - k, own_x + h - 1 - k)]
        if k + 1 == ITERS:
            planes = [x for x in planes if 0 <= x < own_x]
        for x in planes:
            collect(place(k, x), f_ref, image_ref)
        acc = [jnp.zeros((own_y, depth), jnp.float32)] * (k + 2)
        for x in planes:
            inv = inv_ref[x + h]
            for comp in range(3):
                t = u_ref[k, comp, place(k, x)]
                image = image_ref[comp, place(k, x)] + KAPPA * t
                if 0 <= x < own_x:
                    for j in range(k + 1):
                        acc[j] += own_rows(j, comp, x) * image[:own_y]
                    acc[k + 1] += t[:own_y] * r_own[comp, x]
                new = next_basis(k, image, t, inv, lambda: u_ref[k - 1, comp, place(k - 1, x)])
                if k + 1 < ITERS:
                    u_ref[k + 1, comp, place(k + 1, x)] = new
                if 0 <= x < own_x:
                    t_out[k + 1, comp, x] = new[:own_y]
        totals.extend(acc)
    sums_out[...] = jnp.broadcast_to((packed_sums(totals) + sums_in[...])[None], sums_out.shape)


def pack_kernel(
    r_hbm, lab_hbm, r_out, lab_out, up_out, down_out, next_out, previous_out, lab_in, arrived
):
    h = HALO
    own_x, own_y = lab_in.shape[:2]
    copies = [
        pltpu.make_async_copy(r_hbm, r_out, arrived.at[0]),
        pltpu.make_async_copy(lab_hbm, lab_in, arrived.at[1]),
    ]
    for copy in copies:
        copy.start()
    for copy in copies:
        copy.wait()

    def body(n, _):
        l = lab_in[n].astype(jnp.float32)
        lab_out[n] = l
        up_out[3 * own_x + n] = l[own_y - h :]
        up_out[4 * own_x + n // h, pl.ds(n % h, 1)] = l[own_y - h - 1 : own_y - h]
        down_out[3 * own_x + n] = l[:h]
        for comp in range(3):
            r = r_out[comp, n]
            up_out[comp * own_x + n] = r[own_y - h :]
            down_out[comp * own_x + n] = r[:h]
        return _

    pairs(0, own_x, body, 0)
    for i in range(h):
        for comp in range(3):
            next_out[comp * h + i] = r_out[comp, own_x - h + i]
            previous_out[comp * h + i] = r_out[comp, i]
        previous_out[3 * h + i] = lab_in[i].astype(jnp.float32)
    for i in range(h + 1):
        next_out[3 * h + i] = lab_in[own_x - h - 1 + i].astype(jnp.float32)


def combine_kernel(sums_ref, inner_ref, outer_ref, d_inner, d_outer, x_out, r_out):
    total = jnp.sum(sums_ref[...], axis=0, keepdims=True)
    lane = lax.broadcasted_iota(jnp.int32, total.shape, 1)
    entry = [
        jnp.sum(jnp.where(lane == i, total, 0.0), axis=1, keepdims=True) for i in range(SUMS)
    ]
    gram, right = {}, []
    place = 0
    for k in range(ITERS):
        for j in range(k + 1):
            gram[j, k] = gram[k, j] = entry[place]
            place += 1
        right.append(entry[place])
        place += 1
    scale = [gram[k, k] for k in range(ITERS)]
    inv, low = [], {}
    for k in range(ITERS):
        pivot = gram[k, k]
        good = pivot > 1e-7 * scale[k]
        inv.append(jnp.where(good, 1.0 / jnp.where(good, pivot, 1.0), 0.0))
        for i in range(k + 1, ITERS):
            low[i, k] = gram[i, k] * inv[k]
        for i in range(k + 1, ITERS):
            for j in range(k + 1, i + 1):
                gram[i, j] = gram[j, i] = gram[i, j] - low[i, k] * gram[j, k]
            right[i] = right[i] - low[i, k] * right[k]
    y = [None] * ITERS
    for k in reversed(range(ITERS)):
        y[k] = right[k] * inv[k]
        for i in range(k + 1, ITERS):
            y[k] = y[k] - low[i, k] * y[i]
    e = [jnp.ones_like(y[0])] + [jnp.zeros_like(y[0]) for _ in range(ITERS)]
    for k in range(ITERS):
        if k == 0:
            e[1] = e[1] - y[0]
        elif k == 1:
            e[2] = e[2] - HALF * y[1]
            e[1] = e[1] - CENTRE * y[1]
        else:
            e[k + 1] = e[k + 1] - (HALF / 2) * y[k]
            e[k - 1] = e[k - 1] - (HALF / 2) * y[k]
            e[k] = e[k] - CENTRE * y[k]
    y = [jnp.broadcast_to(v, d_outer.shape) for v in y]
    e = [jnp.broadcast_to(v, d_outer.shape) for v in e]

    own_x = d_inner.shape[0]

    def plane(n, outer):
        diag = d_inner[n] if outer is None or n > 0 else d_outer[...]
        for comp in range(3):
            t = []
            for k in range(ITERS + 1):
                edge = outer is not None and (n <= k or n >= own_x - k)
                t.append((outer_ref if edge else inner_ref)[k, comp, n])
            x, r = y[0] * t[0], e[0] * t[0]
            for k in range(1, ITERS):
                x = x + y[k] * t[k]
                r = r + e[k] * t[k]
            r = r + e[ITERS] * t[ITERS]
            x_out[comp, n] = x
            r_out[comp, n] = r * diag

    for n in [*range(ITERS + 1), *range(own_x - ITERS, own_x)]:
        plane(n, True)

    def body(n, _):
        plane(n, None)
        return _

    lax.fori_loop(ITERS + 1, own_x - ITERS, body, 0)


def local(right_side, labels):
    own_x, own_y, depth = labels.shape
    h = HALO
    f32 = jnp.float32
    devices = lax.axis_size("gx") * lax.axis_size("gy")
    small = pltpu.CompilerParams(vmem_limit_bytes=16 * 2**20)
    right_side, lab, up, down, to_next, to_previous = pl.pallas_call(
        pack_kernel,
        out_shape=(
            jax.ShapeDtypeStruct(right_side.shape, f32),
            jax.ShapeDtypeStruct(labels.shape, f32),
            jax.ShapeDtypeStruct((4 * own_x + own_x // h, h, depth), f32),
            jax.ShapeDtypeStruct((4 * own_x, h, depth), f32),
            jax.ShapeDtypeStruct((4 * h + 1, own_y, depth), f32),
            jax.ShapeDtypeStruct((4 * h, own_y, depth), f32),
        ),
        in_specs=[pl.BlockSpec(memory_space=pltpu.HBM)] * 2,
        scratch_shapes=[pltpu.VMEM(labels.shape, jnp.int32), pltpu.SemaphoreType.DMA((2,))],
        compiler_params=small,
        name="pack",
    )(*(pltpu.with_memory_space_constraint(v, pltpu.HBM) for v in (right_side, labels)))

    from_minus = shifted(up, "gy", 1)
    from_plus = shifted(down, "gy", -1)
    below = shifted(to_next, "gx", 1)
    above = shifted(to_previous, "gx", -1)

    from_minus, from_plus, below, above = lax.optimization_barrier(
        (from_minus, from_plus, below, above)
    )

    side = jnp.concatenate(
        [
            from_plus.reshape(4, own_x, h, depth),
            from_minus[: 4 * own_x].reshape(4, own_x, h, depth),
        ],
        2,
    )
    edge = from_minus[4 * own_x :].reshape(own_x, depth)

    def block(start, voxel_start, stop):
        rows = edge[voxel_start:stop]
        return jnp.concatenate(
            [
                side[:3, start:stop].reshape(3 * h, 2 * h, depth),
                side[3, voxel_start:stop],
                jnp.pad(rows, ((0, 2 * h - rows.shape[0]), (0, 0)))[None],
            ],
            0,
        )

    below_side = shifted(block(own_x - h, own_x - h - 1, own_x), "gx", 1)
    above_side = shifted(block(0, 0, h), "gx", -1)

    rows = own_y + 2 * h
    tiles = (rows // 8) * (depth // 128)

    def scratch(planes):
        return [
            pltpu.VMEM((3, planes, rows, depth), f32),
            pltpu.VMEM((3, planes, rows, depth), f32),
            pltpu.VMEM((planes, len(MODES), tiles + 1, 8, 128), f32),
            pltpu.VMEM((planes, len(MODES), tiles + 1, 8, 128), f32),
        ]

    planes = own_x + 2 * WIDTH
    own_basis = jax.ShapeDtypeStruct((ITERS + 1, 3, own_x, own_y, depth), f32)
    inner, d_inner, inverse, borders, inner_sums = pl.pallas_call(
        inside_kernel,
        out_shape=(
            own_basis,
            jax.ShapeDtypeStruct((own_x, own_y, depth), f32),
            jax.ShapeDtypeStruct((own_x, rows, depth), f32),
            jax.ShapeDtypeStruct((ITERS, 3, 4, rows, depth), f32),
            jax.ShapeDtypeStruct((1, 128), f32),
        ),
        scratch_shapes=[
            pltpu.VMEM((ITERS, 3, planes, rows, depth), f32),
            pltpu.VMEM((own_x, depth), f32),
            *scratch(planes),
        ],
        compiler_params=pltpu.CompilerParams(vmem_limit_bytes=28 * 2**20),
        name="inside",
    )(right_side, lab, side, edge)

    strips = 4 * h + 12
    outer, d_outer, sums = pl.pallas_call(
        finish_kernel,
        out_shape=(
            own_basis,
            jax.ShapeDtypeStruct((own_y, depth), f32),
            jax.ShapeDtypeStruct((devices, 1, 128), f32),
        ),
        scratch_shapes=[
            pltpu.VMEM((ITERS, 3, strips, rows, depth), f32),
            pltpu.VMEM((own_x + 2 * h + 2, rows, depth), f32),
            pltpu.VMEM((own_x + 2 * h, rows, depth), f32),
            *scratch(strips),
        ],
        compiler_params=pltpu.CompilerParams(vmem_limit_bytes=28 * 2**20),
        name="finish",
    )(
        right_side, lab, side, edge, below, above, below_side, above_side,
        inner, inverse, borders, inner_sums,
    )

    everyone = lax.all_to_all(sums, ("gx", "gy"), 0, 0)
    out = jax.ShapeDtypeStruct(right_side.shape, f32)
    return pl.pallas_call(combine_kernel, out_shape=(out, out), compiler_params=small, name="combine")(
        everyone.reshape(devices, 128), inner, outer, d_inner, d_outer
    )


def solution(mesh):
    in_specs = (P(None, "gx", "gy", None), P("gx", "gy", None))
    out_specs = (P(None, "gx", "gy", None), P(None, "gx", "gy", None))
    return jax.shard_map(local, mesh=mesh, in_specs=in_specs, out_specs=out_specs, check_vma=False)
```

```python
import functools

import jax
import jax.numpy as jnp
from jax import lax
from jax.experimental import pallas as pl
from jax.experimental.pallas import tpu as pltpu
from jax.sharding import PartitionSpec as P


ITERS = 4
HALO = ITERS
LAMBDA_SOFT = 0.5769231
LAMBDA_RISE = 1.6452991
SHEAR_SOFT = 0.3846154
SHEAR_RISE = 2.9487179
KAPPA = 0.05
SHIFT = (0.25, 1.6, 1.5, 1.5)
STEP = (1.0, 0.6, 0.6, 0.6)
SUMS = 14
WIDTH = 4


def shifted(shard, axis, by):
    size = lax.axis_size(axis)
    return lax.ppermute(shard, axis, [(i, (i + by) % size) for i in range(size)])


def roll(v, by, axis):
    return pltpu.roll(v, by % v.shape[axis], axis)


def get(ref, *index, row=0, rows=None):
    rows = ref.shape[-2] - 8 if rows is None else rows
    parts = [ref[(*index, i, slice(row, row + rows))] for i in range(ref.shape[-3])]
    return jnp.concatenate(parts, 1)


def put(ref, *index, value):
    rows = value.shape[0]
    for i in range(ref.shape[-3]):
        part = value[:, 128 * i : 128 * (i + 1)]
        ref[(*index, i, slice(0, rows))] = part
        ref[(*index, i, slice(rows, rows + 8))] = part[:8]


def gather_modes(v, up, ahead, ahead_up):
    near = (v + up, up - v)
    far = (ahead + ahead_up, ahead_up - ahead)
    out = {}
    for by in (0, 1):
        out[by, 0] = near[by] + far[by]
        out[by, 1] = far[by] - near[by]
    return out


def scatter_modes(r, below):
    part = []
    for bz in (0, 1):
        part.append((r[0, bz] - r[1, bz]) + (below[0, bz] + below[1, bz]))
    return part[0] - part[1], part[0] + part[1]


def voxel_forces(c, stiff):
    lam = (LAMBDA_SOFT / 16) + (LAMBDA_RISE / 16) * stiff
    mu = (SHEAR_SOFT / 16) + (SHEAR_RISE / 16) * stiff
    mu2 = mu + mu
    lam3 = lam * (1.0 / 3)
    mu3 = mu * (1.0 / 3)
    top = ((LAMBDA_SOFT + 4 * SHEAR_SOFT) / 144) + ((LAMBDA_RISE + 4 * SHEAR_RISE) / 144) * stiff
    f = {}
    normal = ((0, 1, 0, 0), (1, 0, 1, 0), (2, 0, 0, 1))
    t = lam * (c[normal[0]] + c[normal[1]] + c[normal[2]])
    for p in normal:
        f[p] = t + mu2 * c[p]
    for p, q in (
        ((0, 1, 1, 0), (2, 0, 1, 1)),
        ((0, 1, 0, 1), (1, 0, 1, 1)),
        ((1, 1, 1, 0), (2, 1, 0, 1)),
    ):
        t = lam3 * (c[p] + c[q])
        f[p] = t + mu * c[p]
        f[q] = t + mu * c[q]
    for comp in range(3):
        p = (comp, 1, 1, 1)
        f[p] = top * c[p]
    for p, q in (
        ((0, 0, 1, 0), (1, 1, 0, 0)),
        ((0, 0, 0, 1), (2, 1, 0, 0)),
        ((1, 0, 0, 1), (2, 0, 1, 0)),
    ):
        f[p] = f[q] = mu * (c[p] + c[q])
    bend = ((0, 0, 1, 1), (1, 1, 0, 1), (2, 1, 1, 0))
    t = c[bend[0]] + c[bend[1]] + c[bend[2]]
    for p in bend:
        f[p] = mu3 * (t + c[p])
    return f


MODES = [(comp, by, bz) for comp in range(3) for by in (0, 1) for bz in (0, 1)]


def strides(start, stop, width, body, carry):
    def several(i, carry):
        return body(start + width * i, carry)

    return lax.fori_loop(0, -((start - stop) // width), several, carry)


def pairs(start, stop, body, carry):
    return strides(start, stop, 2, lambda n, c: body(n + 1, body(n, c)), carry)


def tiles_of(rows, depth):
    return [(slice(a, a + 8), slice(b, b + 128)) for a in range(0, rows, 8) for b in range(0, depth, 128)]


def diagonal_layer(cells, turned, edge, first_row):
    lz = cells + turned
    row_id = lax.broadcasted_iota(jnp.int32, lz.shape, 0)
    return lz + jnp.where(row_id == first_row, jnp.broadcast_to(edge, lz.shape), roll(lz, 1, 0))


def diagonal_from(two_layers):
    base = 8 * (LAMBDA_SOFT + 4 * SHEAR_SOFT) / 9 + KAPPA
    return base + ((LAMBDA_RISE + 4 * SHEAR_RISE) / 9) * two_layers


def forward_planes(first, last, node_ref, turn_ref, q_ref):
    rows = node_ref.shape[-2] - 8
    tiles = tiles_of(rows, 128 * node_ref.shape[-3])
    for n in range(first, last):
        for comp in range(3):
            put(turn_ref, comp, n, value=roll(get(node_ref, comp, n), -1, 1))

    def forward(n, _):
        for comp in range(3):
            out = gather_modes(
                get(node_ref, comp, n),
                get(node_ref, comp, n, row=1, rows=rows),
                get(turn_ref, comp, n),
                get(turn_ref, comp, n, row=1, rows=rows),
            )
            for i, (cc, by, bz) in enumerate(MODES):
                if cc == comp:
                    for j, tile in enumerate(tiles):
                        q_ref[n, i, j] = out[by, bz][tile]
        return _

    pairs(first, last, forward, 0)


def voxel_layers(j, first, last, cells_at, q_ref, f_ref):
    across, tall = f_ref.shape[-3], f_ref.shape[-2]
    line, lanes = divmod(j, across)
    row = 8 * (line + 1)

    def store(n, i, value):
        f_ref[n, i, lanes, row : row + 8] = value
        if row + 8 == tall:
            f_ref[n, i, lanes, 0:8] = value

    def voxels(n, carry):
        near, behind = carry
        far = [q_ref[n + 1, i, j] for i in range(len(MODES))]
        c = {}
        for i, (comp, by, bz) in enumerate(MODES):
            if (by, bz) != (0, 0):
                c[comp, 0, by, bz] = near[i] + far[i]
            c[comp, 1, by, bz] = far[i] - near[i]
        f = voxel_forces(c, cells_at(n))
        ahead = []
        for i, (comp, by, bz) in enumerate(MODES):
            up = f[comp, 1, by, bz]
            if (by, bz) != (0, 0):
                flat = f[comp, 0, by, bz]
                store(n, i, behind[i] + (flat - up))
                ahead.append(flat + up)
            else:
                store(n, i, behind[i] - up)
                ahead.append(up)
        return far, ahead

    near = [q_ref[first, i, j] for i in range(len(MODES))]
    pairs(first, last, voxels, (near, [jnp.zeros_like(v) for v in near]))


def collect(n, f_ref, image_ref):
    rows = f_ref.shape[-2] - 8
    for comp in range(3):
        here, below = {}, {}
        for i, (cc, by, bz) in enumerate(MODES):
            if cc == comp:
                here[by, bz] = get(f_ref, n, i, row=8, rows=rows)
                below[by, bz] = get(f_ref, n, i, row=7, rows=rows)
        kept, moved = scatter_modes(here, below)
        image_ref[comp, n] = kept + roll(moved, 1, 1)


def update(k, inv):
    gain = inv * (1 / STEP[k])
    own = KAPPA * gain - SHIFT[k] / STEP[k]

    def new(force, t, older):
        out = force * gain + t * own
        return out - (STEP[k - 1] / STEP[k]) * older() if k > 1 else out

    return new


def packed_sums(totals):
    lane = lax.broadcasted_iota(jnp.int32, (1, 128), 1)
    packed = jnp.zeros((1, 128), jnp.float32)
    for i, v in enumerate(totals):
        s = jnp.sum(jnp.sum(v, axis=0, keepdims=True), axis=1, keepdims=True)
        packed = jnp.where(lane == i, s, packed)
    return packed


def inside_kernel(
    r_own, lab_own, side_ref, edge_own,
    t_out, d_out, inv_out, edge_out, sums_out,
    edge_ref, t_ref, turn_ref, image_ref, q_ref, f_ref,
):
    own_x, own_y, depth = r_own.shape[1:]
    rows = own_y + side_ref.shape[2]
    tiles = tiles_of(rows, depth)
    count = own_x - 1

    def both(block, side):
        return jnp.concatenate([block, side], 0)

    edges = edge_own[...]
    edge_ref[...] = edges + roll(edges, 1, 1)
    for m in range(own_x):
        put(turn_ref, 0, m, value=roll(both(lab_own[m], side_ref[3, m]), 1, 1))

    def layer(m):
        cells = both(lab_own[m], side_ref[3, m])
        return diagonal_layer(cells, get(turn_ref, 0, m), edge_ref[pl.ds(m, 1), :], own_y + HALO)

    def start(p, before):
        here = layer(p + 1)
        diag = diagonal_from(before + here)
        inv = 1.0 / diag
        inv_out[p + 1] = inv
        d_out[p + 1] = diag[:own_y]
        for comp in range(3):
            t = both(r_own[comp, p + 1], side_ref[comp, p + 1]) * inv
            put(t_ref, 0, comp, p, value=t)
            t_out[0, comp, p + 1] = t[:own_y]
        return here

    before = pairs(0, count - 1, start, layer(0))
    start(count - 1, before)

    totals = []
    for k in range(ITERS):
        first, last = k, count - k
        for i, p in enumerate((first, first + 1, last - 2, last - 1)):
            for comp in range(3):
                edge_out[k, comp, i] = get(t_ref, k, comp, p)
        forward_planes(first, last, t_ref.at[k], turn_ref, q_ref)
        for j, (line, lanes) in enumerate(tiles):

            def cells_at(n):
                if line.start < own_y:
                    return lab_own[n + 1, line, lanes]
                return side_ref[3, n + 1, line.start - own_y : line.stop - own_y, lanes]

            voxel_layers(j, first, last - 1, cells_at, q_ref, f_ref)

        def advance(p, acc):
            acc = list(acc)
            new = update(k, inv_out[p + 1])
            for comp in range(3):
                t = get(t_ref, k, comp, p)
                force = image_ref[comp, p]
                image = force[:own_y] + KAPPA * t[:own_y]
                for j in range(k + 1):
                    acc[j] += get(t_ref, j, comp, p, rows=own_y) * image
                acc[k + 1] += t[:own_y] * r_own[comp, p + 1]
                t = new(force, t, lambda: get(t_ref, k - 1, comp, p))
                if k + 1 < ITERS:
                    put(t_ref, k + 1, comp, p, value=t)
                t_out[k + 1, comp, p + 1] = t[:own_y]
            return tuple(acc)

        def several(n, acc):
            for u in range(WIDTH):
                acc = advance(n + u, acc)
            for u in range(WIDTH):
                collect(n + WIDTH + u, f_ref, image_ref)
            return acc

        begin, end = first + 1, last - 1
        whole = begin + (end - begin) // WIDTH * WIDTH
        for p in range(begin, begin + WIDTH):
            collect(p, f_ref, image_ref)
        acc = (jnp.zeros((own_y, depth), jnp.float32),) * (k + 2)
        acc = strides(begin, whole, WIDTH, several, acc)
        for p in range(whole, end):
            acc = advance(p, acc)
        totals.extend(acc)
    sums_out[...] = packed_sums(totals)


def finish_kernel(
    r_own, lab_own, side_ref, edge_own, below, above, below_side, above_side,
    t_in, inv_in, edge_in, sums_in,
    t_out, d_out, sums_out,
    cell_ref, inv_ref, u_ref, turn_ref, image_ref, q_ref, f_ref,
):
    h = HALO
    own_x, own_y, depth = r_own.shape[1:]
    rows = own_y + side_ref.shape[2]
    tiles = tiles_of(rows, depth)
    left, right = h + 3, h + 2

    def nodes(comp, x):
        if x < 0:
            return jnp.concatenate([below[comp * h + h + x], below_side[comp * h + h + x]], 0)
        if x >= own_x:
            i = comp * h + x - own_x
            return jnp.concatenate([above[i], above_side[i]], 0)
        return jnp.concatenate([r_own[comp, x], side_ref[comp, x]], 0)

    def cells(x):
        if x < 0:
            i = 3 * h + h + 1 + x
            return jnp.concatenate([below[i], below_side[i]], 0)
        if x >= own_x:
            i = 3 * h + x - own_x
            return jnp.concatenate([above[i], above_side[i]], 0)
        return jnp.concatenate([lab_own[x], side_ref[3, x]], 0)

    def edge(x):
        if x < 0:
            return below_side[4 * h + 1, h + 1 + x : h + 2 + x]
        if x >= own_x:
            return above_side[4 * h, x - own_x : x - own_x + 1]
        return edge_own[x : x + 1]

    for x in [*range(-h - 1, ITERS + 1), *range(own_x - 1 - ITERS, own_x + h)]:
        cell_ref[x + h + 1] = cells(x)

    def layer(x):
        e = edge(x)
        c = cell_ref[x + h + 1]
        return diagonal_layer(c, roll(c, 1, 1), e + roll(e, 1, 1), own_y + h)

    def place(k, x):
        return x - (k - h) if x < own_x // 2 else left + x - (own_x - 2 - k)

    for start, stop in ((-h, 1), (own_x, own_x + h)):
        layers = [layer(x) for x in range(start - 1, stop)]
        for x in range(start, stop):
            diag = diagonal_from(layers[x - start] + layers[x - start + 1])
            inv = 1.0 / diag
            inv_ref[x + h] = inv
            if x == 0:
                d_out[...] = diag[:own_y]
            for comp in range(3):
                t = nodes(comp, x) * inv
                put(u_ref, 0, comp, place(0, x), value=t)
                if x == 0:
                    t_out[0, comp, 0] = t[:own_y]
    for x in [*range(1, ITERS + 1), *range(own_x - ITERS, own_x)]:
        inv_ref[x + h] = inv_in[x]

    def own_rows(j, comp, x):
        ref = t_out if x <= j or x >= own_x - j else t_in
        return ref[j, comp, x]

    totals = []
    for k in range(ITERS):
        for comp in range(3):
            for i, p in enumerate((left - 2, left - 1, left, left + 1)):
                put(u_ref, k, comp, p, value=edge_in[k, comp, i])
        forward_planes(0, left + right, u_ref.at[k], turn_ref, q_ref)
        for j, (line, lanes) in enumerate(tiles):
            voxel_layers(j, 0, left - 1, lambda n: cell_ref[n + k + 1, line, lanes], q_ref, f_ref)
            shift = own_x - 2 - k - left + h + 1
            voxel_layers(
                j, left, left + right - 1, lambda n: cell_ref[n + shift, line, lanes], q_ref, f_ref
            )
        planes = [*range(k - h + 1, k + 2), *range(own_x - 1 - k, own_x + h - 1 - k)]
        if k + 1 == ITERS:
            planes = [x for x in planes if 0 <= x < own_x]
        for x in planes:
            collect(place(k, x), f_ref, image_ref)
        acc = [jnp.zeros((own_y, depth), jnp.float32)] * (k + 2)
        for x in planes:
            new = update(k, inv_ref[x + h])
            own = 0 <= x < own_x
            for comp in range(3):
                t = get(u_ref, k, comp, place(k, x))
                force = image_ref[comp, place(k, x)]
                if own:
                    image = force[:own_y] + KAPPA * t[:own_y]
                    for j in range(k + 1):
                        acc[j] += own_rows(j, comp, x) * image
                    acc[k + 1] += t[:own_y] * r_own[comp, x]
                t = new(force, t, lambda: get(u_ref, k - 1, comp, place(k - 1, x)))
                if k + 1 < ITERS:
                    put(u_ref, k + 1, comp, place(k + 1, x), value=t)
                if own:
                    t_out[k + 1, comp, x] = t[:own_y]
        totals.extend(acc)
    sums_out[...] = jnp.broadcast_to((packed_sums(totals) + sums_in[...])[None], sums_out.shape)


def pack_kernel(
    r_hbm, lab_hbm, r_out, lab_out, up_out, down_out, next_out, previous_out, lab_in, arrived
):
    h = HALO
    own_x, own_y = lab_in.shape[:2]
    copies = [
        pltpu.make_async_copy(r_hbm, r_out, arrived.at[0]),
        pltpu.make_async_copy(lab_hbm, lab_in, arrived.at[1]),
    ]
    for copy in copies:
        copy.start()
    for copy in copies:
        copy.wait()

    def body(n, _):
        l = lab_in[n].astype(jnp.float32)
        lab_out[n] = l
        up_out[3 * own_x + n] = l[own_y - h :]
        up_out[4 * own_x + n // h, pl.ds(n % h, 1)] = l[own_y - h - 1 : own_y - h]
        down_out[3 * own_x + n] = l[:h]
        for comp in range(3):
            r = r_out[comp, n]
            up_out[comp * own_x + n] = r[own_y - h :]
            down_out[comp * own_x + n] = r[:h]
        return _

    pairs(0, own_x, body, 0)
    for i in range(h):
        for comp in range(3):
            next_out[comp * h + i] = r_out[comp, own_x - h + i]
            previous_out[comp * h + i] = r_out[comp, i]
        previous_out[3 * h + i] = lab_in[i].astype(jnp.float32)
    for i in range(h + 1):
        next_out[3 * h + i] = lab_in[own_x - h - 1 + i].astype(jnp.float32)


def combine_kernel(sums_ref, inner_ref, outer_ref, d_inner, d_outer, x_out, r_out):
    total = jnp.sum(sums_ref[...], axis=0, keepdims=True)
    lane = lax.broadcasted_iota(jnp.int32, total.shape, 1)
    entry = [
        jnp.sum(jnp.where(lane == i, total, 0.0), axis=1, keepdims=True) for i in range(SUMS)
    ]
    gram, right = {}, []
    place = 0
    for k in range(ITERS):
        for j in range(k + 1):
            gram[j, k] = gram[k, j] = entry[place]
            place += 1
        right.append(entry[place])
        place += 1
    scale = [gram[k, k] for k in range(ITERS)]
    inv, low = [], {}
    for k in range(ITERS):
        pivot = gram[k, k]
        good = pivot > 1e-7 * scale[k]
        inv.append(jnp.where(good, 1.0 / jnp.where(good, pivot, 1.0), 0.0))
        for i in range(k + 1, ITERS):
            low[i, k] = gram[i, k] * inv[k]
        for i in range(k + 1, ITERS):
            for j in range(k + 1, i + 1):
                gram[i, j] = gram[j, i] = gram[i, j] - low[i, k] * gram[j, k]
            right[i] = right[i] - low[i, k] * right[k]
    y = [None] * ITERS
    for k in reversed(range(ITERS)):
        y[k] = right[k] * inv[k]
        for i in range(k + 1, ITERS):
            y[k] = y[k] - low[i, k] * y[i]
    e = [jnp.ones_like(y[0])] + [jnp.zeros_like(y[0]) for _ in range(ITERS)]
    for k in range(ITERS):
        e[k + 1] = e[k + 1] - STEP[k] * y[k]
        e[k] = e[k] - SHIFT[k] * y[k]
        if k > 1:
            e[k - 1] = e[k - 1] - STEP[k - 1] * y[k]
    y = [jnp.broadcast_to(v, d_outer.shape) for v in y]
    e = [jnp.broadcast_to(v, d_outer.shape) for v in e]

    own_x = d_inner.shape[0]

    def plane(n, outer):
        diag = d_inner[n] if outer is None or n > 0 else d_outer[...]
        for comp in range(3):
            t = []
            for k in range(ITERS + 1):
                edge = outer is not None and (n <= k or n >= own_x - k)
                t.append((outer_ref if edge else inner_ref)[k, comp, n])
            x, r = y[0] * t[0], e[0] * t[0]
            for k in range(1, ITERS):
                x = x + y[k] * t[k]
                r = r + e[k] * t[k]
            r = r + e[ITERS] * t[ITERS]
            x_out[comp, n] = x
            r_out[comp, n] = r * diag

    for n in [*range(ITERS + 1), *range(own_x - ITERS, own_x)]:
        plane(n, True)

    def body(n, _):
        plane(n, None)
        return _

    lax.fori_loop(ITERS + 1, own_x - ITERS, body, 0)


def local(right_side, labels):
    own_x, own_y, depth = labels.shape
    h = HALO
    f32 = jnp.float32
    devices = lax.axis_size("gx") * lax.axis_size("gy")
    small = pltpu.CompilerParams(vmem_limit_bytes=16 * 2**20)
    right_side, lab, up, down, to_next, to_previous = pl.pallas_call(
        pack_kernel,
        out_shape=(
            jax.ShapeDtypeStruct(right_side.shape, f32),
            jax.ShapeDtypeStruct(labels.shape, f32),
            jax.ShapeDtypeStruct((4 * own_x + own_x // h, h, depth), f32),
            jax.ShapeDtypeStruct((4 * own_x, h, depth), f32),
            jax.ShapeDtypeStruct((4 * h + 1, own_y, depth), f32),
            jax.ShapeDtypeStruct((4 * h, own_y, depth), f32),
        ),
        in_specs=[pl.BlockSpec(memory_space=pltpu.HBM)] * 2,
        scratch_shapes=[pltpu.VMEM(labels.shape, jnp.int32), pltpu.SemaphoreType.DMA((2,))],
        compiler_params=small,
        name="pack",
    )(*(pltpu.with_memory_space_constraint(v, pltpu.HBM) for v in (right_side, labels)))

    from_minus = shifted(up, "gy", 1)
    from_plus = shifted(down, "gy", -1)
    below = shifted(to_next, "gx", 1)
    above = shifted(to_previous, "gx", -1)

    from_minus, from_plus, below, above = lax.optimization_barrier(
        (from_minus, from_plus, below, above)
    )

    side = jnp.concatenate(
        [
            from_plus.reshape(4, own_x, h, depth),
            from_minus[: 4 * own_x].reshape(4, own_x, h, depth),
        ],
        2,
    )
    edge = from_minus[4 * own_x :].reshape(own_x, depth)

    def block(start, voxel_start, stop):
        rows = edge[voxel_start:stop]
        return jnp.concatenate(
            [
                side[:3, start:stop].reshape(3 * h, 2 * h, depth),
                side[3, voxel_start:stop],
                jnp.pad(rows, ((0, 2 * h - rows.shape[0]), (0, 0)))[None],
            ],
            0,
        )

    below_side = shifted(block(own_x - h, own_x - h - 1, own_x), "gx", 1)
    above_side = shifted(block(0, 0, h), "gx", -1)

    rows = own_y + 2 * h
    tiles = (rows // 8) * (depth // 128)

    across = depth // 128

    def kept(*lead):
        return pltpu.VMEM((*lead, across, rows + 8, 128), f32)

    def scratch(planes):
        return [
            kept(ITERS, 3, planes),
            kept(3, planes),
            pltpu.VMEM((3, planes, rows, depth), f32),
            pltpu.VMEM((planes, len(MODES), tiles + 1, 8, 128), f32),
            kept(planes, len(MODES)),
        ]

    planes = own_x + 2 * WIDTH
    own_basis = jax.ShapeDtypeStruct((ITERS + 1, 3, own_x, own_y, depth), f32)
    inner, d_inner, inverse, borders, inner_sums = pl.pallas_call(
        inside_kernel,
        out_shape=(
            own_basis,
            jax.ShapeDtypeStruct((own_x, own_y, depth), f32),
            jax.ShapeDtypeStruct((own_x, rows, depth), f32),
            jax.ShapeDtypeStruct((ITERS, 3, 4, rows, depth), f32),
            jax.ShapeDtypeStruct((1, 128), f32),
        ),
        scratch_shapes=[
            pltpu.VMEM((own_x, depth), f32),
            *scratch(planes),
        ],
        compiler_params=pltpu.CompilerParams(vmem_limit_bytes=28 * 2**20),
        name="inside",
    )(right_side, lab, side, edge)

    strips = 4 * h + 12
    outer, d_outer, sums = pl.pallas_call(
        finish_kernel,
        out_shape=(
            own_basis,
            jax.ShapeDtypeStruct((own_y, depth), f32),
            jax.ShapeDtypeStruct((devices, 1, 128), f32),
        ),
        scratch_shapes=[
            pltpu.VMEM((own_x + 2 * h + 2, rows, depth), f32),
            pltpu.VMEM((own_x + 2 * h, rows, depth), f32),
            *scratch(strips),
        ],
        compiler_params=pltpu.CompilerParams(vmem_limit_bytes=28 * 2**20),
        name="finish",
    )(
        right_side, lab, side, edge, below, above, below_side, above_side,
        inner, inverse, borders, inner_sums,
    )

    everyone = lax.all_to_all(sums, ("gx", "gy"), 0, 0)
    out = jax.ShapeDtypeStruct(right_side.shape, f32)
    return pl.pallas_call(combine_kernel, out_shape=(out, out), compiler_params=small, name="combine")(
        everyone.reshape(devices, 128), inner, outer, d_inner, d_outer
    )


def solution(mesh):
    in_specs = (P(None, "gx", "gy", None), P("gx", "gy", None))
    out_specs = (P(None, "gx", "gy", None), P(None, "gx", "gy", None))
    return jax.shard_map(local, mesh=mesh, in_specs=in_specs, out_specs=out_specs, check_vma=False)
```

```python
import jax
import jax.numpy as jnp
from jax import lax
from jax.experimental import pallas as pl
from jax.experimental.pallas import tpu as pltpu
from jax.sharding import PartitionSpec as P


ITERS = 4
HALO = ITERS
LAMBDA_SOFT = 0.5769231
LAMBDA_RISE = 1.6452991
SHEAR_SOFT = 0.3846154
SHEAR_RISE = 2.9487179
KAPPA = 0.05
SHIFT = (0.25, 1.6, 1.5, 1.5)
STEP = (1.0, 0.6, 0.6, 0.6)
SUMS = 14
WIDTH = 4


def shifted(shard, axis, by):
    size = lax.axis_size(axis)
    return lax.ppermute(shard, axis, [(i, (i + by) % size) for i in range(size)])


def roll(v, by, axis):
    return pltpu.roll(v, by % v.shape[axis], axis)


def get(ref, *index, row=0, rows=None):
    rows = ref.shape[-2] - 8 if rows is None else rows
    parts = [ref[(*index, i, slice(row, row + rows))] for i in range(ref.shape[-3])]
    return jnp.concatenate(parts, 1)


def put(ref, *index, value):
    rows = value.shape[0]
    for i in range(ref.shape[-3]):
        part = value[:, 128 * i : 128 * (i + 1)]
        ref[(*index, i, slice(0, rows))] = part
        ref[(*index, i, slice(rows, rows + 8))] = part[:8]


def gather_modes(v, up, ahead, ahead_up):
    near = (v + up, up - v)
    far = (ahead + ahead_up, ahead_up - ahead)
    out = {}
    for by in (0, 1):
        out[by, 0] = near[by] + far[by]
        out[by, 1] = far[by] - near[by]
    return out


def scatter_modes(r, below):
    part = []
    for bz in (0, 1):
        part.append((r[0, bz] - r[1, bz]) + (below[0, bz] + below[1, bz]))
    return part[0] - part[1], part[0] + part[1]


def voxel_forces(c, stiff):
    lam = (LAMBDA_SOFT / 16) + (LAMBDA_RISE / 16) * stiff
    mu = (SHEAR_SOFT / 16) + (SHEAR_RISE / 16) * stiff
    mu2 = mu + mu
    lam3 = lam * (1.0 / 3)
    mu3 = mu * (1.0 / 3)
    top = ((LAMBDA_SOFT + 4 * SHEAR_SOFT) / 144) + ((LAMBDA_RISE + 4 * SHEAR_RISE) / 144) * stiff
    f = {}
    normal = ((0, 1, 0, 0), (1, 0, 1, 0), (2, 0, 0, 1))
    t = lam * (c[normal[0]] + c[normal[1]] + c[normal[2]])
    for p in normal:
        f[p] = t + mu2 * c[p]
    for p, q in (
        ((0, 1, 1, 0), (2, 0, 1, 1)),
        ((0, 1, 0, 1), (1, 0, 1, 1)),
        ((1, 1, 1, 0), (2, 1, 0, 1)),
    ):
        t = lam3 * (c[p] + c[q])
        f[p] = t + mu * c[p]
        f[q] = t + mu * c[q]
    for comp in range(3):
        p = (comp, 1, 1, 1)
        f[p] = top * c[p]
    for p, q in (
        ((0, 0, 1, 0), (1, 1, 0, 0)),
        ((0, 0, 0, 1), (2, 1, 0, 0)),
        ((1, 0, 0, 1), (2, 0, 1, 0)),
    ):
        f[p] = f[q] = mu * (c[p] + c[q])
    bend = ((0, 0, 1, 1), (1, 1, 0, 1), (2, 1, 1, 0))
    t = c[bend[0]] + c[bend[1]] + c[bend[2]]
    for p in bend:
        f[p] = mu3 * (t + c[p])
    return f


MODES = [(comp, by, bz) for comp in range(3) for by in (0, 1) for bz in (0, 1)]


def strides(start, stop, width, body, carry):
    def several(i, carry):
        return body(start + width * i, carry)

    return lax.fori_loop(0, -((start - stop) // width), several, carry)


def pairs(start, stop, body, carry):
    return strides(start, stop, 2, lambda n, c: body(n + 1, body(n, c)), carry)


def tiles_of(rows, depth):
    return [(slice(a, a + 8), slice(b, b + 128)) for a in range(0, rows, 8) for b in range(0, depth, 128)]


def diagonal_layer(cells, turned, edge, first_row):
    lz = cells + turned
    row_id = lax.broadcasted_iota(jnp.int32, lz.shape, 0)
    return lz + jnp.where(row_id == first_row, jnp.broadcast_to(edge, lz.shape), roll(lz, 1, 0))


def diagonal_from(two_layers):
    base = 8 * (LAMBDA_SOFT + 4 * SHEAR_SOFT) / 9 + KAPPA
    return base + ((LAMBDA_RISE + 4 * SHEAR_RISE) / 9) * two_layers


def forward_planes(first, last, node_ref, turn_ref, q_ref):
    rows = node_ref.shape[-2] - 8
    tiles = tiles_of(rows, 128 * node_ref.shape[-3])
    for n in range(first, last):
        for comp in range(3):
            put(turn_ref, comp, n, value=roll(get(node_ref, comp, n), -1, 1))

    def forward(n, _):
        for comp in range(3):
            out = gather_modes(
                get(node_ref, comp, n),
                get(node_ref, comp, n, row=1, rows=rows),
                get(turn_ref, comp, n),
                get(turn_ref, comp, n, row=1, rows=rows),
            )
            for i, (cc, by, bz) in enumerate(MODES):
                if cc == comp:
                    for j, tile in enumerate(tiles):
                        q_ref[n, i, j] = out[by, bz][tile]
        return _

    pairs(first, last, forward, 0)


def voxel_layers(j, first, last, cells_at, q_ref, f_ref):
    across, tall = f_ref.shape[-3], f_ref.shape[-2]
    line, lanes = divmod(j, across)
    row = 8 * (line + 1)

    def store(n, i, value):
        f_ref[n, i, lanes, row : row + 8] = value
        if row + 8 == tall:
            f_ref[n, i, lanes, 0:8] = value

    def voxels(n, carry):
        near, behind = carry
        far = [q_ref[n + 1, i, j] for i in range(len(MODES))]
        c = {}
        for i, (comp, by, bz) in enumerate(MODES):
            if (by, bz) != (0, 0):
                c[comp, 0, by, bz] = near[i] + far[i]
            c[comp, 1, by, bz] = far[i] - near[i]
        f = voxel_forces(c, cells_at(n))
        ahead = []
        for i, (comp, by, bz) in enumerate(MODES):
            up = f[comp, 1, by, bz]
            if (by, bz) != (0, 0):
                flat = f[comp, 0, by, bz]
                store(n, i, behind[i] + (flat - up))
                ahead.append(flat + up)
            else:
                store(n, i, behind[i] - up)
                ahead.append(up)
        return far, ahead

    near = [q_ref[first, i, j] for i in range(len(MODES))]
    pairs(first, last, voxels, (near, [jnp.zeros_like(v) for v in near]))


def collect(n, f_ref, image_ref):
    rows = f_ref.shape[-2] - 8
    for comp in range(3):
        here, below = {}, {}
        for i, (cc, by, bz) in enumerate(MODES):
            if cc == comp:
                here[by, bz] = get(f_ref, n, i, row=8, rows=rows)
                below[by, bz] = get(f_ref, n, i, row=7, rows=rows)
        kept, moved = scatter_modes(here, below)
        image_ref[comp, n] = kept + roll(moved, 1, 1)


def update(k, inv):
    gain = inv * (1 / STEP[k])
    own = KAPPA * gain - SHIFT[k] / STEP[k]

    def new(force, t, older):
        out = force * gain + t * own
        return out - (STEP[k - 1] / STEP[k]) * older() if k > 1 else out

    return new


def packed_sums(totals):
    lane = lax.broadcasted_iota(jnp.int32, (1, 128), 1)
    packed = jnp.zeros((1, 128), jnp.float32)
    for i, v in enumerate(totals):
        s = jnp.sum(jnp.sum(v, axis=0, keepdims=True), axis=1, keepdims=True)
        packed = jnp.where(lane == i, s, packed)
    return packed


def y_parts(own_x):
    h = HALO
    mid = own_x - 2 * h

    def node(comp, x):
        if x < h:
            return 0, 4 * h + 1 + comp * h + x
        if x >= own_x - h:
            return 0, comp * h + x - (own_x - h)
        return 1, comp * mid + x - h

    def cell(x):
        if x < h:
            return 0, 7 * h + 1 + x
        if x >= own_x - h - 1:
            return 0, 3 * h + x - (own_x - h - 1)
        return 1, 3 * mid + x - h

    def edge(x):
        if x < h:
            return 0, h + 1 + x
        if x >= own_x - h - 1:
            return 0, x - (own_x - h - 1)
        return 1, x - h

    blocks = (8 * h + 1, 4 * mid - 1)
    edge_blocks = (-(-(2 * h + 1) // h), -(-(mid - 1) // h))
    return node, cell, edge, blocks, edge_blocks


def inside_kernel(
    r_own, lab_own, side_a, side_b, edge_a, edge_b,
    t_out, d_out, inv_out, edge_out, sums_out,
    side_ref, edge_ref, t_ref, turn_ref, image_ref, q_ref, f_ref,
):
    own_x, own_y, depth = r_own.shape[1:]
    rows = own_y + side_ref.shape[2]
    tiles = tiles_of(rows, depth)
    count = own_x - 1

    def both(block, side):
        return jnp.concatenate([block, side], 0)

    node_at, cell_at, edge_at = y_parts(own_x)[:3]
    sides, edges = (side_a, side_b), (edge_a, edge_b)
    for x in range(own_x):
        for comp in range(3):
            part, place = node_at(comp, x)
            side_ref[comp, x] = sides[part][place]
        part, place = cell_at(x)
        side_ref[3, x] = sides[part][place]
        part, place = edge_at(x)
        edge_ref[x : x + 1] = edges[part][place : place + 1]
    lines = edge_ref[...]
    edge_ref[...] = lines + roll(lines, 1, 1)
    for m in range(own_x):
        put(turn_ref, 0, m, value=roll(both(lab_own[m], side_ref[3, m]), 1, 1))

    def layer(m):
        cells = both(lab_own[m], side_ref[3, m])
        return diagonal_layer(cells, get(turn_ref, 0, m), edge_ref[pl.ds(m, 1), :], own_y + HALO)

    def start(p, before):
        here = layer(p + 1)
        diag = diagonal_from(before + here)
        inv = 1.0 / diag
        inv_out[p + 1] = inv
        d_out[p + 1] = diag[:own_y]
        for comp in range(3):
            t = both(r_own[comp, p + 1], side_ref[comp, p + 1]) * inv
            put(t_ref, 0, comp, p, value=t)
            t_out[0, comp, p + 1] = t[:own_y]
        return here

    before = pairs(0, count - 1, start, layer(0))
    start(count - 1, before)

    totals = []
    for k in range(ITERS):
        first, last = k, count - k
        for i, p in enumerate((first, first + 1, last - 2, last - 1)):
            for comp in range(3):
                edge_out[k, comp, i] = get(t_ref, k, comp, p)
        forward_planes(first, last, t_ref.at[k], turn_ref, q_ref)
        for j, (line, lanes) in enumerate(tiles):

            def cells_at(n):
                if line.start < own_y:
                    return lab_own[n + 1, line, lanes]
                return side_ref[3, n + 1, line.start - own_y : line.stop - own_y, lanes]

            voxel_layers(j, first, last - 1, cells_at, q_ref, f_ref)

        def advance(p, acc):
            acc = list(acc)
            new = update(k, inv_out[p + 1])
            for comp in range(3):
                t = get(t_ref, k, comp, p)
                force = image_ref[comp, p]
                image = force[:own_y] + KAPPA * t[:own_y]
                for j in range(k + 1):
                    acc[j] += get(t_ref, j, comp, p, rows=own_y) * image
                acc[k + 1] += t[:own_y] * r_own[comp, p + 1]
                t = new(force, t, lambda: get(t_ref, k - 1, comp, p))
                if k + 1 < ITERS:
                    put(t_ref, k + 1, comp, p, value=t)
                t_out[k + 1, comp, p + 1] = t[:own_y]
            return tuple(acc)

        def several(n, acc):
            for u in range(WIDTH):
                acc = advance(n + u, acc)
            for u in range(WIDTH):
                collect(n + WIDTH + u, f_ref, image_ref)
            return acc

        begin, end = first + 1, last - 1
        whole = begin + (end - begin) // WIDTH * WIDTH
        for p in range(begin, begin + WIDTH):
            collect(p, f_ref, image_ref)
        acc = (jnp.zeros((own_y, depth), jnp.float32),) * (k + 2)
        acc = strides(begin, whole, WIDTH, several, acc)
        for p in range(whole, end):
            acc = advance(p, acc)
        totals.extend(acc)
    sums_out[...] = packed_sums(totals)


def finish_kernel(
    r_own, lab_own, side_a, side_b, edge_a, below, above, below_side, above_side,
    t_in, inv_in, edge_in, sums_in,
    t_out, d_out, sums_out,
    cell_ref, inv_ref, u_ref, turn_ref, image_ref, q_ref, f_ref,
):
    h = HALO
    own_x, own_y, depth = r_own.shape[1:]
    rows = own_y + side_a.shape[1]
    tiles = tiles_of(rows, depth)
    left, right = h + 3, h + 2
    node_at, cell_at, edge_at = y_parts(own_x)[:3]
    sides = (side_a, side_b)

    def nodes(comp, x):
        if x < 0:
            return jnp.concatenate([below[comp * h + h + x], below_side[comp * h + h + x]], 0)
        if x >= own_x:
            i = comp * h + x - own_x
            return jnp.concatenate([above[i], above_side[i]], 0)
        part, place = node_at(comp, x)
        return jnp.concatenate([r_own[comp, x], sides[part][place]], 0)

    def cells(x):
        if x < 0:
            i = 3 * h + h + 1 + x
            return jnp.concatenate([below[i], below_side[i]], 0)
        if x >= own_x:
            i = 3 * h + x - own_x
            return jnp.concatenate([above[i], above_side[i]], 0)
        part, place = cell_at(x)
        return jnp.concatenate([lab_own[x], sides[part][place]], 0)

    def edge(x):
        if x < 0:
            return below_side[4 * h + 1, h + 1 + x : h + 2 + x]
        if x >= own_x:
            return above_side[4 * h, x - own_x : x - own_x + 1]
        place = edge_at(x)[1]
        return edge_a[place : place + 1]

    for x in [*range(-h - 1, ITERS + 1), *range(own_x - 1 - ITERS, own_x + h)]:
        cell_ref[x + h + 1] = cells(x)

    def layer(x):
        e = edge(x)
        c = cell_ref[x + h + 1]
        return diagonal_layer(c, roll(c, 1, 1), e + roll(e, 1, 1), own_y + h)

    def place(k, x):
        return x - (k - h) if x < own_x // 2 else left + x - (own_x - 2 - k)

    for start, stop in ((-h, 1), (own_x, own_x + h)):
        layers = [layer(x) for x in range(start - 1, stop)]
        for x in range(start, stop):
            diag = diagonal_from(layers[x - start] + layers[x - start + 1])
            inv = 1.0 / diag
            inv_ref[x + h] = inv
            if x == 0:
                d_out[...] = diag[:own_y]
            for comp in range(3):
                t = nodes(comp, x) * inv
                put(u_ref, 0, comp, place(0, x), value=t)
                if x == 0:
                    t_out[0, comp, 0] = t[:own_y]
    for x in [*range(1, ITERS + 1), *range(own_x - ITERS, own_x)]:
        inv_ref[x + h] = inv_in[x]

    def own_rows(j, comp, x):
        ref = t_out if x <= j or x >= own_x - j else t_in
        return ref[j, comp, x]

    totals = []
    for k in range(ITERS):
        for comp in range(3):
            for i, p in enumerate((left - 2, left - 1, left, left + 1)):
                put(u_ref, k, comp, p, value=edge_in[k, comp, i])
        forward_planes(0, left + right, u_ref.at[k], turn_ref, q_ref)
        for j, (line, lanes) in enumerate(tiles):
            voxel_layers(j, 0, left - 1, lambda n: cell_ref[n + k + 1, line, lanes], q_ref, f_ref)
            shift = own_x - 2 - k - left + h + 1
            voxel_layers(
                j, left, left + right - 1, lambda n: cell_ref[n + shift, line, lanes], q_ref, f_ref
            )
        planes = [*range(k - h + 1, k + 2), *range(own_x - 1 - k, own_x + h - 1 - k)]
        if k + 1 == ITERS:
            planes = [x for x in planes if 0 <= x < own_x]
        for x in planes:
            collect(place(k, x), f_ref, image_ref)
        acc = [jnp.zeros((own_y, depth), jnp.float32)] * (k + 2)
        for x in planes:
            new = update(k, inv_ref[x + h])
            own = 0 <= x < own_x
            for comp in range(3):
                t = get(u_ref, k, comp, place(k, x))
                force = image_ref[comp, place(k, x)]
                if own:
                    image = force[:own_y] + KAPPA * t[:own_y]
                    for j in range(k + 1):
                        acc[j] += own_rows(j, comp, x) * image
                    acc[k + 1] += t[:own_y] * r_own[comp, x]
                t = new(force, t, lambda: get(u_ref, k - 1, comp, place(k - 1, x)))
                if k + 1 < ITERS:
                    put(u_ref, k + 1, comp, place(k + 1, x), value=t)
                if own:
                    t_out[k + 1, comp, x] = t[:own_y]
        totals.extend(acc)
    sums_out[...] = jnp.broadcast_to((packed_sums(totals) + sums_in[...])[None], sums_out.shape)


def pack_kernel(
    r_hbm, lab_hbm, r_out, lab_out, up_a, down_a, up_b, down_b, next_out, previous_out, lab_in, arrived
):
    h = HALO
    own_x, own_y = lab_in.shape[:2]
    copies = [
        pltpu.make_async_copy(r_hbm, r_out, arrived.at[0]),
        pltpu.make_async_copy(lab_hbm, lab_in, arrived.at[1]),
    ]
    for copy in copies:
        copy.start()
    for copy in copies:
        copy.wait()

    ups, downs = (up_a, up_b), (down_a, down_b)
    node_at, cell_at, edge_at, blocks, _ = y_parts(own_x)
    for x in range(own_x):
        l = lab_in[x].astype(jnp.float32)
        lab_out[x] = l
        part, place = cell_at(x)
        ups[part][place] = l[own_y - h :]
        downs[part][place] = l[:h]
        part, place = edge_at(x)
        ups[part][blocks[part] + place // h, place % h : place % h + 1] = l[own_y - h - 1 : own_y - h]
        if x < h:
            previous_out[3 * h + x] = l
        if x >= own_x - h - 1:
            next_out[3 * h + x - (own_x - h - 1)] = l
        for comp in range(3):
            r = r_out[comp, x]
            part, place = node_at(comp, x)
            ups[part][place] = r[own_y - h :]
            downs[part][place] = r[:h]
            if x < h:
                previous_out[comp * h + x] = r
            if x >= own_x - h:
                next_out[comp * h + x - (own_x - h)] = r


def combine_kernel(sums_ref, inner_ref, outer_ref, d_inner, d_outer, x_out, r_out):
    total = jnp.sum(sums_ref[...], axis=0, keepdims=True)
    lane = lax.broadcasted_iota(jnp.int32, total.shape, 1)
    entry = [
        jnp.sum(jnp.where(lane == i, total, 0.0), axis=1, keepdims=True) for i in range(SUMS)
    ]
    gram, right = {}, []
    place = 0
    for k in range(ITERS):
        for j in range(k + 1):
            gram[j, k] = gram[k, j] = entry[place]
            place += 1
        right.append(entry[place])
        place += 1
    scale = [gram[k, k] for k in range(ITERS)]
    inv, low = [], {}
    for k in range(ITERS):
        pivot = gram[k, k]
        good = pivot > 1e-7 * scale[k]
        inv.append(jnp.where(good, 1.0 / jnp.where(good, pivot, 1.0), 0.0))
        for i in range(k + 1, ITERS):
            low[i, k] = gram[i, k] * inv[k]
        for i in range(k + 1, ITERS):
            for j in range(k + 1, i + 1):
                gram[i, j] = gram[j, i] = gram[i, j] - low[i, k] * gram[j, k]
            right[i] = right[i] - low[i, k] * right[k]
    y = [None] * ITERS
    for k in reversed(range(ITERS)):
        y[k] = right[k] * inv[k]
        for i in range(k + 1, ITERS):
            y[k] = y[k] - low[i, k] * y[i]
    e = [jnp.ones_like(y[0])] + [jnp.zeros_like(y[0]) for _ in range(ITERS)]
    for k in range(ITERS):
        e[k + 1] = e[k + 1] - STEP[k] * y[k]
        e[k] = e[k] - SHIFT[k] * y[k]
        if k > 1:
            e[k - 1] = e[k - 1] - STEP[k - 1] * y[k]
    y = [jnp.broadcast_to(v, d_outer.shape) for v in y]
    e = [jnp.broadcast_to(v, d_outer.shape) for v in e]

    own_x = d_inner.shape[0]

    def plane(n, outer):
        diag = d_inner[n] if outer is None or n > 0 else d_outer[...]
        for comp in range(3):
            t = []
            for k in range(ITERS + 1):
                edge = outer is not None and (n <= k or n >= own_x - k)
                t.append((outer_ref if edge else inner_ref)[k, comp, n])
            x, r = y[0] * t[0], e[0] * t[0]
            for k in range(1, ITERS):
                x = x + y[k] * t[k]
                r = r + e[k] * t[k]
            r = r + e[ITERS] * t[ITERS]
            x_out[comp, n] = x
            r_out[comp, n] = r * diag

    for n in [*range(ITERS + 1), *range(own_x - ITERS, own_x)]:
        plane(n, True)

    def body(n, _):
        plane(n, None)
        return _

    lax.fori_loop(ITERS + 1, own_x - ITERS, body, 0)


def local(right_side, labels):
    own_x, own_y, depth = labels.shape
    h = HALO
    f32 = jnp.float32
    devices = lax.axis_size("gx") * lax.axis_size("gy")
    small = pltpu.CompilerParams(vmem_limit_bytes=16 * 2**20)
    blocks, edge_blocks = y_parts(own_x)[3:]
    right_side, lab, up_a, down_a, up_b, down_b, to_next, to_previous = pl.pallas_call(
        pack_kernel,
        out_shape=(
            jax.ShapeDtypeStruct(right_side.shape, f32),
            jax.ShapeDtypeStruct(labels.shape, f32),
            jax.ShapeDtypeStruct((blocks[0] + edge_blocks[0], h, depth), f32),
            jax.ShapeDtypeStruct((blocks[0], h, depth), f32),
            jax.ShapeDtypeStruct((blocks[1] + edge_blocks[1], h, depth), f32),
            jax.ShapeDtypeStruct((blocks[1], h, depth), f32),
            jax.ShapeDtypeStruct((4 * h + 1, own_y, depth), f32),
            jax.ShapeDtypeStruct((4 * h, own_y, depth), f32),
        ),
        in_specs=[pl.BlockSpec(memory_space=pltpu.HBM)] * 2,
        scratch_shapes=[pltpu.VMEM(labels.shape, jnp.int32), pltpu.SemaphoreType.DMA((2,))],
        compiler_params=small,
        name="pack",
    )(*(pltpu.with_memory_space_constraint(v, pltpu.HBM) for v in (right_side, labels)))

    minus_a, plus_a = shifted(up_a, "gy", 1), shifted(down_a, "gy", -1)
    minus_b, plus_b = shifted(up_b, "gy", 1), shifted(down_b, "gy", -1)
    below = shifted(to_next, "gx", 1)
    above = shifted(to_previous, "gx", -1)
    minus_a, plus_a, below, above = lax.optimization_barrier((minus_a, plus_a, below, above))

    def stack(minus, plus, count):
        side = jnp.concatenate([plus[:count], minus[:count]], 1)
        return side, minus[count:].reshape(-1, depth)

    def corner(block, rows):
        rows = jnp.pad(rows, ((0, 2 * h - rows.shape[0]), (0, 0)))
        return jnp.concatenate([block, rows[None]], 0)

    side_a, edge_a = stack(minus_a, plus_a, blocks[0])
    below_side = shifted(corner(side_a[: 4 * h + 1], edge_a[: h + 1]), "gx", 1)
    last = corner(side_a[4 * h + 1 :], edge_a[h + 1 : 2 * h + 1])
    above_side = shifted(last, "gx", -1)
    side_b, edge_b = stack(minus_b, plus_b, blocks[1])

    rows = own_y + 2 * h
    tiles = (rows // 8) * (depth // 128)

    across = depth // 128

    def kept(*lead):
        return pltpu.VMEM((*lead, across, rows + 8, 128), f32)

    def scratch(planes):
        return [
            kept(ITERS, 3, planes),
            kept(3, planes),
            pltpu.VMEM((3, planes, rows, depth), f32),
            pltpu.VMEM((planes, len(MODES), tiles + 1, 8, 128), f32),
            kept(planes, len(MODES)),
        ]

    planes = own_x + 2 * WIDTH
    own_basis = jax.ShapeDtypeStruct((ITERS + 1, 3, own_x, own_y, depth), f32)
    inner, d_inner, inverse, borders, inner_sums = pl.pallas_call(
        inside_kernel,
        out_shape=(
            own_basis,
            jax.ShapeDtypeStruct((own_x, own_y, depth), f32),
            jax.ShapeDtypeStruct((own_x, rows, depth), f32),
            jax.ShapeDtypeStruct((ITERS, 3, 4, rows, depth), f32),
            jax.ShapeDtypeStruct((1, 128), f32),
        ),
        scratch_shapes=[
            pltpu.VMEM((4, own_x, 2 * h, depth), f32),
            pltpu.VMEM((own_x, depth), f32),
            *scratch(planes),
        ],
        compiler_params=pltpu.CompilerParams(vmem_limit_bytes=28 * 2**20),
        name="inside",
    )(right_side, lab, side_a, side_b, edge_a, edge_b)

    strips = 4 * h + 12
    outer, d_outer, sums = pl.pallas_call(
        finish_kernel,
        out_shape=(
            own_basis,
            jax.ShapeDtypeStruct((own_y, depth), f32),
            jax.ShapeDtypeStruct((devices, 1, 128), f32),
        ),
        scratch_shapes=[
            pltpu.VMEM((own_x + 2 * h + 2, rows, depth), f32),
            pltpu.VMEM((own_x + 2 * h, rows, depth), f32),
            *scratch(strips),
        ],
        compiler_params=pltpu.CompilerParams(vmem_limit_bytes=28 * 2**20),
        name="finish",
    )(
        right_side, lab, side_a, side_b, edge_a, below, above, below_side, above_side,
        inner, inverse, borders, inner_sums,
    )

    everyone = lax.all_to_all(sums, ("gx", "gy"), 0, 0)
    out = jax.ShapeDtypeStruct(right_side.shape, f32)
    return pl.pallas_call(combine_kernel, out_shape=(out, out), compiler_params=small, name="combine")(
        everyone.reshape(devices, 128), inner, outer, d_inner, d_outer
    )


def solution(mesh):
    in_specs = (P(None, "gx", "gy", None), P("gx", "gy", None))
    out_specs = (P(None, "gx", "gy", None), P(None, "gx", "gy", None))
    return jax.shard_map(local, mesh=mesh, in_specs=in_specs, out_specs=out_specs, check_vma=False)
```

```python
import jax
import jax.numpy as jnp
from jax import lax
from jax.experimental import pallas as pl
from jax.experimental.pallas import tpu as pltpu
from jax.sharding import PartitionSpec as P


ITERS = 4
HALO = ITERS
LAMBDA_SOFT = 0.5769231
LAMBDA_RISE = 1.6452991
SHEAR_SOFT = 0.3846154
SHEAR_RISE = 2.9487179
KAPPA = 0.05
SHIFT = (0.25, 1.6, 1.5, 1.5)
STEP = (1.0, 0.6, 0.6, 0.6)
SUMS = 14
WIDTH = 4


def shifted(shard, axis, by):
    size = lax.axis_size(axis)
    return lax.ppermute(shard, axis, [(i, (i + by) % size) for i in range(size)])


def roll(v, by, axis):
    return pltpu.roll(v, by % v.shape[axis], axis)


def get(ref, *index, row=0, rows=None):
    rows = ref.shape[-2] - 8 if rows is None else rows
    parts = [ref[(*index, i, slice(row, row + rows))] for i in range(ref.shape[-3])]
    return jnp.concatenate(parts, 1)


def put(ref, *index, value):
    rows = value.shape[0]
    for i in range(ref.shape[-3]):
        part = value[:, 128 * i : 128 * (i + 1)]
        ref[(*index, i, slice(0, rows))] = part
        ref[(*index, i, slice(rows, rows + 8))] = part[:8]


def gather_modes(v, up, ahead, ahead_up):
    near = (v + up, up - v)
    far = (ahead + ahead_up, ahead_up - ahead)
    out = {}
    for by in (0, 1):
        out[by, 0] = near[by] + far[by]
        out[by, 1] = far[by] - near[by]
    return out


def scatter_modes(r, below):
    part = []
    for bz in (0, 1):
        part.append((r[0, bz] - r[1, bz]) + (below[0, bz] + below[1, bz]))
    return part[0] - part[1], part[0] + part[1]


def voxel_forces(c, stiff):
    lam = (LAMBDA_SOFT / 16) + (LAMBDA_RISE / 16) * stiff
    mu = (SHEAR_SOFT / 16) + (SHEAR_RISE / 16) * stiff
    mu2 = mu + mu
    lam3 = lam * (1.0 / 3)
    mu3 = mu * (1.0 / 3)
    top = ((LAMBDA_SOFT + 4 * SHEAR_SOFT) / 144) + ((LAMBDA_RISE + 4 * SHEAR_RISE) / 144) * stiff
    f = {}
    normal = ((0, 1, 0, 0), (1, 0, 1, 0), (2, 0, 0, 1))
    t = lam * (c[normal[0]] + c[normal[1]] + c[normal[2]])
    for p in normal:
        f[p] = t + mu2 * c[p]
    for p, q in (
        ((0, 1, 1, 0), (2, 0, 1, 1)),
        ((0, 1, 0, 1), (1, 0, 1, 1)),
        ((1, 1, 1, 0), (2, 1, 0, 1)),
    ):
        t = lam3 * (c[p] + c[q])
        f[p] = t + mu * c[p]
        f[q] = t + mu * c[q]
    for comp in range(3):
        p = (comp, 1, 1, 1)
        f[p] = top * c[p]
    for p, q in (
        ((0, 0, 1, 0), (1, 1, 0, 0)),
        ((0, 0, 0, 1), (2, 1, 0, 0)),
        ((1, 0, 0, 1), (2, 0, 1, 0)),
    ):
        f[p] = f[q] = mu * (c[p] + c[q])
    bend = ((0, 0, 1, 1), (1, 1, 0, 1), (2, 1, 1, 0))
    t = c[bend[0]] + c[bend[1]] + c[bend[2]]
    for p in bend:
        f[p] = mu3 * (t + c[p])
    return f


MODES = [(comp, by, bz) for comp in range(3) for by in (0, 1) for bz in (0, 1)]


def strides(start, stop, width, body, carry):
    def several(i, carry):
        return body(start + width * i, carry)

    return lax.fori_loop(0, -((start - stop) // width), several, carry)


def pairs(start, stop, body, carry):
    return strides(start, stop, 2, lambda n, c: body(n + 1, body(n, c)), carry)


def tiles_of(rows, depth):
    return [(slice(a, a + 8), slice(b, b + 128)) for a in range(0, rows, 8) for b in range(0, depth, 128)]


def diagonal_layer(cells, turned, edge, first_row):
    lz = cells + turned
    row_id = lax.broadcasted_iota(jnp.int32, lz.shape, 0)
    return lz + jnp.where(row_id == first_row, jnp.broadcast_to(edge, lz.shape), roll(lz, 1, 0))


def diagonal_from(two_layers):
    base = 8 * (LAMBDA_SOFT + 4 * SHEAR_SOFT) / 9 + KAPPA
    return base + ((LAMBDA_RISE + 4 * SHEAR_RISE) / 9) * two_layers


def forward_planes(first, last, node_ref, turn_ref, q_ref):
    rows = node_ref.shape[-2] - 8
    tiles = tiles_of(rows, 128 * node_ref.shape[-3])
    for n in range(first, last):
        for comp in range(3):
            put(turn_ref, comp, n, value=roll(get(node_ref, comp, n), -1, 1))

    def forward(n, _):
        for comp in range(3):
            out = gather_modes(
                get(node_ref, comp, n),
                get(node_ref, comp, n, row=1, rows=rows),
                get(turn_ref, comp, n),
                get(turn_ref, comp, n, row=1, rows=rows),
            )
            for i, (cc, by, bz) in enumerate(MODES):
                if cc == comp:
                    for j, tile in enumerate(tiles):
                        q_ref[n, i, j] = out[by, bz][tile]
        return _

    pairs(first, last, forward, 0)


def voxel_layers(j, first, last, cells_at, q_ref, f_ref):
    across, tall = f_ref.shape[-3], f_ref.shape[-2]
    line, lanes = divmod(j, across)
    row = 8 * (line + 1)

    def store(n, i, value):
        f_ref[n, i, lanes, row : row + 8] = value
        if row + 8 == tall:
            f_ref[n, i, lanes, 0:8] = value

    def voxels(n, carry):
        near, behind = carry
        far = [q_ref[n + 1, i, j] for i in range(len(MODES))]
        c = {}
        for i, (comp, by, bz) in enumerate(MODES):
            if (by, bz) != (0, 0):
                c[comp, 0, by, bz] = near[i] + far[i]
            c[comp, 1, by, bz] = far[i] - near[i]
        f = voxel_forces(c, cells_at(n))
        ahead = []
        for i, (comp, by, bz) in enumerate(MODES):
            up = f[comp, 1, by, bz]
            if (by, bz) != (0, 0):
                flat = f[comp, 0, by, bz]
                store(n, i, behind[i] + (flat - up))
                ahead.append(flat + up)
            else:
                store(n, i, behind[i] - up)
                ahead.append(up)
        return far, ahead

    near = [q_ref[first, i, j] for i in range(len(MODES))]
    carry = near, [jnp.zeros_like(v) for v in near]
    even = first + (last - first) // 2 * 2
    carry = pairs(first, even, voxels, carry)
    for n in range(even, last):
        carry = voxels(n, carry)


def collect(n, f_ref, image_ref):
    rows = f_ref.shape[-2] - 8
    for comp in range(3):
        here, below = {}, {}
        for i, (cc, by, bz) in enumerate(MODES):
            if cc == comp:
                here[by, bz] = get(f_ref, n, i, row=8, rows=rows)
                below[by, bz] = get(f_ref, n, i, row=7, rows=rows)
        kept, moved = scatter_modes(here, below)
        image_ref[comp, n] = kept + roll(moved, 1, 1)


def update(k, inv):
    gain = inv * (1 / STEP[k])
    own = KAPPA * gain - SHIFT[k] / STEP[k]

    def new(force, t, older):
        out = force * gain + t * own
        return out - (STEP[k - 1] / STEP[k]) * older() if k > 1 else out

    return new


def packed_sums(totals):
    lane = lax.broadcasted_iota(jnp.int32, (1, 128), 1)
    packed = jnp.zeros((1, 128), jnp.float32)
    for i, v in enumerate(totals):
        s = jnp.sum(jnp.sum(v, axis=0, keepdims=True), axis=1, keepdims=True)
        packed = jnp.where(lane == i, s, packed)
    return packed


def y_parts(own_x):
    h = HALO
    mid = own_x - 2 * h

    def node(comp, x):
        if x < h:
            return 0, 4 * h + 1 + comp * h + x
        if x >= own_x - h:
            return 0, comp * h + x - (own_x - h)
        return 1, comp * mid + x - h

    def cell(x):
        if x < h:
            return 0, 7 * h + 1 + x
        if x >= own_x - h - 1:
            return 0, 3 * h + x - (own_x - h - 1)
        return 1, 3 * mid + x - h

    def edge(x):
        if x < h:
            return 0, h + 1 + x
        if x >= own_x - h - 1:
            return 0, x - (own_x - h - 1)
        return 1, x - h

    blocks = (8 * h + 1, 4 * mid - 1)
    edge_blocks = (-(-(2 * h + 1) // h), -(-(mid - 1) // h))
    return node, cell, edge, blocks, edge_blocks


def begin_kernel(
    r_own, lab_own, side_a, side_b, edge_a, edge_b,
    side_out, t_out, inv_out, d_out,
    edge_ref, turn_ref,
):
    own_x, own_y, depth = r_own.shape[1:]

    def both(block, side):
        return jnp.concatenate([block, side], 0)

    node_at, cell_at, edge_at = y_parts(own_x)[:3]
    sides, edges = (side_a, side_b), (edge_a, edge_b)
    for x in range(own_x):
        for comp in range(3):
            part, place = node_at(comp, x)
            side_out[comp, x] = sides[part][place]
        part, place = cell_at(x)
        side_out[3, x] = sides[part][place]
        part, place = edge_at(x)
        edge_ref[x : x + 1] = edges[part][place : place + 1]
    lines = edge_ref[...]
    edge_ref[...] = lines + roll(lines, 1, 1)
    for m in range(own_x):
        turn_ref[m] = roll(both(lab_own[m], side_out[3, m]), 1, 1)

    def layer(m):
        cells = both(lab_own[m], side_out[3, m])
        return diagonal_layer(cells, turn_ref[m], edge_ref[pl.ds(m, 1), :], own_y + HALO)

    def start(x, before):
        here = layer(x)
        diag = diagonal_from(before + here)
        inv = 1.0 / diag
        inv_out[x] = inv
        d_out[x] = diag[:own_y]
        for comp in range(3):
            put(t_out, comp, x, value=both(r_own[comp, x], side_out[comp, x]) * inv)
        return here

    before = pairs(1, own_x - 1, start, layer(0))
    start(own_x - 1, before)


def basis_kernel(
    r_own, lab_own, side_ref, edge_a, below, above, below_side, above_side, t0_in, inv_in,
    t_out, d_out, sums_out,
    cell_ref, inv_ref, t_ref, turn_ref, image_ref, q_ref, f_ref,
):
    h = HALO
    own_x, own_y, depth = r_own.shape[1:]
    rows = own_y + side_ref.shape[2]
    tiles = tiles_of(rows, depth)
    planes = own_x + 2 * h
    lo, hi = h, h + own_x
    edge_at = y_parts(own_x)[2]

    def nodes(comp, x):
        if x < 0:
            return jnp.concatenate([below[comp * h + h + x], below_side[comp * h + h + x]], 0)
        if x >= own_x:
            i = comp * h + x - own_x
            return jnp.concatenate([above[i], above_side[i]], 0)
        return jnp.concatenate([r_own[comp, x], side_ref[comp, x]], 0)

    def edge(x):
        if x < 0:
            return below_side[4 * h + 1, h + 1 + x : h + 2 + x]
        if x >= own_x:
            return above_side[4 * h, x - own_x : x - own_x + 1]
        place = edge_at(x)[1]
        return edge_a[place : place + 1]

    for i in range(h + 1):
        cell_ref[i] = jnp.concatenate([below[3 * h + i], below_side[3 * h + i]], 0)
    for i in range(h):
        cell_ref[h + 1 + own_x + i] = jnp.concatenate([above[3 * h + i], above_side[3 * h + i]], 0)

    def copy(x, _):
        cell_ref[x + h + 1] = jnp.concatenate([lab_own[x], side_ref[3, x]], 0)
        inv_ref[x + h] = inv_in[x]
        for comp in range(3):
            t = get(t0_in, comp, x)
            put(t_ref, 0, comp, x + h, value=t)
            t_out[0, comp, x] = t[:own_y]
        return _

    pairs(0, own_x, copy, 0)

    def layer(x):
        e = edge(x)
        c = cell_ref[x + h + 1]
        return diagonal_layer(c, roll(c, 1, 1), e + roll(e, 1, 1), own_y + h)

    for start, stop in ((-h, 1), (own_x, own_x + h)):
        layers = [layer(x) for x in range(start - 1, stop)]
        for x in range(start, stop):
            diag = diagonal_from(layers[x - start] + layers[x - start + 1])
            inv = 1.0 / diag
            inv_ref[x + h] = inv
            if x == 0:
                d_out[...] = diag[:own_y]
            for comp in range(3):
                t = nodes(comp, x) * inv
                put(t_ref, 0, comp, x + h, value=t)
                if x == 0:
                    t_out[0, comp, 0] = t[:own_y]

    totals = []
    for k in range(ITERS):
        first, last = k, planes - k
        forward_planes(first, last, t_ref.at[k], turn_ref, q_ref)
        for j, (line, lanes) in enumerate(tiles):
            voxel_layers(j, first, last - 1, lambda n: cell_ref[n + 1, line, lanes], q_ref, f_ref)

        def advance(n, own, acc):
            acc = list(acc)
            new = update(k, inv_ref[n])
            for comp in range(3):
                t = get(t_ref, k, comp, n)
                force = image_ref[comp, n]
                if own:
                    image = force[:own_y] + KAPPA * t[:own_y]
                    for j in range(k + 1):
                        acc[j] += get(t_ref, j, comp, n, rows=own_y) * image
                    acc[k + 1] += t[:own_y] * r_own[comp, n - lo]
                t = new(force, t, lambda: get(t_ref, k - 1, comp, n))
                if k + 1 < ITERS:
                    put(t_ref, k + 1, comp, n, value=t)
                if own:
                    t_out[k + 1, comp, n - lo] = t[:own_y]
            return tuple(acc)

        def several(n, acc):
            for u in range(WIDTH):
                acc = advance(n + u, True, acc)
            for u in range(WIDTH):
                collect(n + WIDTH + u, f_ref, image_ref)
            return acc

        beside = [*range(first + 1, lo), *range(hi, last - 1)] if k + 1 < ITERS else []
        for n in [*beside, *range(lo, lo + WIDTH)]:
            collect(n, f_ref, image_ref)
        for n in beside:
            advance(n, False, ())
        acc = (jnp.zeros((own_y, depth), jnp.float32),) * (k + 2)
        whole = lo + own_x // WIDTH * WIDTH
        acc = strides(lo, whole, WIDTH, several, acc)
        for n in range(whole, hi):
            acc = advance(n, True, acc)
        totals.extend(acc)
    sums_out[...] = jnp.broadcast_to(packed_sums(totals)[None], sums_out.shape)


def pack_kernel(
    r_hbm, lab_hbm, r_out, lab_out, up_a, down_a, up_b, down_b, next_out, previous_out, lab_in, arrived
):
    h = HALO
    own_x, own_y = lab_in.shape[:2]
    copies = [
        pltpu.make_async_copy(r_hbm, r_out, arrived.at[0]),
        pltpu.make_async_copy(lab_hbm, lab_in, arrived.at[1]),
    ]
    for copy in copies:
        copy.start()
    for copy in copies:
        copy.wait()

    ups, downs = (up_a, up_b), (down_a, down_b)
    node_at, cell_at, edge_at, blocks, _ = y_parts(own_x)
    for x in range(own_x):
        l = lab_in[x].astype(jnp.float32)
        lab_out[x] = l
        part, place = cell_at(x)
        ups[part][place] = l[own_y - h :]
        downs[part][place] = l[:h]
        part, place = edge_at(x)
        ups[part][blocks[part] + place // h, place % h : place % h + 1] = l[own_y - h - 1 : own_y - h]
        if x < h:
            previous_out[3 * h + x] = l
        if x >= own_x - h - 1:
            next_out[3 * h + x - (own_x - h - 1)] = l
        for comp in range(3):
            r = r_out[comp, x]
            part, place = node_at(comp, x)
            ups[part][place] = r[own_y - h :]
            downs[part][place] = r[:h]
            if x < h:
                previous_out[comp * h + x] = r
            if x >= own_x - h:
                next_out[comp * h + x - (own_x - h)] = r


def combine_kernel(sums_ref, t_ref, d_ref, d_first, x_out, r_out):
    total = jnp.sum(sums_ref[...], axis=0, keepdims=True)
    lane = lax.broadcasted_iota(jnp.int32, total.shape, 1)
    entry = [
        jnp.sum(jnp.where(lane == i, total, 0.0), axis=1, keepdims=True) for i in range(SUMS)
    ]
    gram, right = {}, []
    place = 0
    for k in range(ITERS):
        for j in range(k + 1):
            gram[j, k] = gram[k, j] = entry[place]
            place += 1
        right.append(entry[place])
        place += 1
    scale = [gram[k, k] for k in range(ITERS)]
    inv, low = [], {}
    for k in range(ITERS):
        pivot = gram[k, k]
        good = pivot > 1e-7 * scale[k]
        inv.append(jnp.where(good, 1.0 / jnp.where(good, pivot, 1.0), 0.0))
        for i in range(k + 1, ITERS):
            low[i, k] = gram[i, k] * inv[k]
        for i in range(k + 1, ITERS):
            for j in range(k + 1, i + 1):
                gram[i, j] = gram[j, i] = gram[i, j] - low[i, k] * gram[j, k]
            right[i] = right[i] - low[i, k] * right[k]
    y = [None] * ITERS
    for k in reversed(range(ITERS)):
        y[k] = right[k] * inv[k]
        for i in range(k + 1, ITERS):
            y[k] = y[k] - low[i, k] * y[i]
    e = [jnp.ones_like(y[0])] + [jnp.zeros_like(y[0]) for _ in range(ITERS)]
    for k in range(ITERS):
        e[k + 1] = e[k + 1] - STEP[k] * y[k]
        e[k] = e[k] - SHIFT[k] * y[k]
        if k > 1:
            e[k - 1] = e[k - 1] - STEP[k - 1] * y[k]
    y = [jnp.broadcast_to(v, d_first.shape) for v in y]
    e = [jnp.broadcast_to(v, d_first.shape) for v in e]

    def plane(n, diag):
        for comp in range(3):
            t = [t_ref[k, comp, n] for k in range(ITERS + 1)]
            x, r = y[0] * t[0], e[0] * t[0]
            for k in range(1, ITERS):
                x = x + y[k] * t[k]
                r = r + e[k] * t[k]
            r = r + e[ITERS] * t[ITERS]
            x_out[comp, n] = x
            r_out[comp, n] = r * diag

    def body(n, _):
        plane(n, d_ref[n])
        return _

    plane(0, d_first[...])
    pairs(1, d_ref.shape[0] - 1, body, 0)
    plane(d_ref.shape[0] - 1, d_ref[d_ref.shape[0] - 1])


def local(right_side, labels):
    own_x, own_y, depth = labels.shape
    h = HALO
    f32 = jnp.float32
    devices = lax.axis_size("gx") * lax.axis_size("gy")
    small = pltpu.CompilerParams(vmem_limit_bytes=16 * 2**20)
    blocks, edge_blocks = y_parts(own_x)[3:]
    right_side, lab, up_a, down_a, up_b, down_b, to_next, to_previous = pl.pallas_call(
        pack_kernel,
        out_shape=(
            jax.ShapeDtypeStruct(right_side.shape, f32),
            jax.ShapeDtypeStruct(labels.shape, f32),
            jax.ShapeDtypeStruct((blocks[0] + edge_blocks[0], h, depth), f32),
            jax.ShapeDtypeStruct((blocks[0], h, depth), f32),
            jax.ShapeDtypeStruct((blocks[1] + edge_blocks[1], h, depth), f32),
            jax.ShapeDtypeStruct((blocks[1], h, depth), f32),
            jax.ShapeDtypeStruct((4 * h + 1, own_y, depth), f32),
            jax.ShapeDtypeStruct((4 * h, own_y, depth), f32),
        ),
        in_specs=[pl.BlockSpec(memory_space=pltpu.HBM)] * 2,
        scratch_shapes=[pltpu.VMEM(labels.shape, jnp.int32), pltpu.SemaphoreType.DMA((2,))],
        compiler_params=small,
        name="pack",
    )(*(pltpu.with_memory_space_constraint(v, pltpu.HBM) for v in (right_side, labels)))

    minus_a, plus_a = shifted(up_a, "gy", 1), shifted(down_a, "gy", -1)
    minus_b, plus_b = shifted(up_b, "gy", 1), shifted(down_b, "gy", -1)
    below = shifted(to_next, "gx", 1)
    above = shifted(to_previous, "gx", -1)
    minus_a, plus_a, below, above = lax.optimization_barrier((minus_a, plus_a, below, above))

    def stack(minus, plus, count):
        side = jnp.concatenate([plus[:count], minus[:count]], 1)
        return side, minus[count:].reshape(-1, depth)

    def corner(block, rows):
        rows = jnp.pad(rows, ((0, 2 * h - rows.shape[0]), (0, 0)))
        return jnp.concatenate([block, rows[None]], 0)

    side_a, edge_a = stack(minus_a, plus_a, blocks[0])
    below_side = shifted(corner(side_a[: 4 * h + 1], edge_a[: h + 1]), "gx", 1)
    last = corner(side_a[4 * h + 1 :], edge_a[h + 1 : 2 * h + 1])
    above_side = shifted(last, "gx", -1)
    side_b, edge_b = stack(minus_b, plus_b, blocks[1])

    rows = own_y + 2 * h
    tiles = (rows // 8) * (depth // 128)

    across = depth // 128

    def kept(*lead):
        return pltpu.VMEM((*lead, across, rows + 8, 128), f32)

    def scratch(planes):
        return [
            kept(ITERS, 3, planes),
            kept(3, planes),
            pltpu.VMEM((3, planes, rows, depth), f32),
            pltpu.VMEM((planes, len(MODES), tiles + 1, 8, 128), f32),
            kept(planes, len(MODES)),
        ]

    side, t0, inverse, diagonal = pl.pallas_call(
        begin_kernel,
        out_shape=(
            jax.ShapeDtypeStruct((4, own_x, 2 * h, depth), f32),
            jax.ShapeDtypeStruct((3, own_x, across, rows + 8, 128), f32),
            jax.ShapeDtypeStruct((own_x, rows, depth), f32),
            jax.ShapeDtypeStruct((own_x, own_y, depth), f32),
        ),
        scratch_shapes=[
            pltpu.VMEM((own_x, depth), f32),
            pltpu.VMEM((own_x, rows, depth), f32),
        ],
        compiler_params=small,
        name="begin",
    )(right_side, lab, side_a, side_b, edge_a, edge_b)

    planes = own_x + 2 * h
    basis, d_first, sums = pl.pallas_call(
        basis_kernel,
        out_shape=(
            jax.ShapeDtypeStruct((ITERS + 1, 3, own_x, own_y, depth), f32),
            jax.ShapeDtypeStruct((own_y, depth), f32),
            jax.ShapeDtypeStruct((devices, 1, 128), f32),
        ),
        scratch_shapes=[
            pltpu.VMEM((planes + 2, rows, depth), f32),
            pltpu.VMEM((planes, rows, depth), f32),
            *scratch(planes + 1),
        ],
        compiler_params=pltpu.CompilerParams(vmem_limit_bytes=34 * 2**20),
        name="basis",
    )(right_side, lab, side, edge_a, below, above, below_side, above_side, t0, inverse)

    everyone = lax.all_to_all(sums, ("gx", "gy"), 0, 0)
    out = jax.ShapeDtypeStruct(right_side.shape, f32)
    return pl.pallas_call(combine_kernel, out_shape=(out, out), compiler_params=small, name="combine")(
        everyone.reshape(devices, 128), basis, diagonal, d_first
    )


def solution(mesh):
    in_specs = (P(None, "gx", "gy", None), P("gx", "gy", None))
    out_specs = (P(None, "gx", "gy", None), P(None, "gx", "gy", None))
    return jax.shard_map(local, mesh=mesh, in_specs=in_specs, out_specs=out_specs, check_vma=False)
```

```python
import jax
import jax.numpy as jnp
from jax import lax
from jax.experimental import pallas as pl
from jax.experimental.pallas import tpu as pltpu
from jax.sharding import PartitionSpec as P


ITERS = 4
HALO = ITERS
LAMBDA_SOFT = 0.5769231
LAMBDA_RISE = 1.6452991
SHEAR_SOFT = 0.3846154
SHEAR_RISE = 2.9487179
KAPPA = 0.05
SHIFT = (0.25, 1.6, 1.5, 1.5)
STEP = (1.0, 0.6, 0.6, 0.6)
SUMS = 14
WIDTH = 4


def shifted(shard, axis, by):
    size = lax.axis_size(axis)
    return lax.ppermute(shard, axis, [(i, (i + by) % size) for i in range(size)])


def roll(v, by, axis):
    return pltpu.roll(v, by % v.shape[axis], axis)


def get(ref, *index, row=0, rows=None):
    rows = ref.shape[-2] - 8 if rows is None else rows
    parts = [ref[(*index, i, slice(row, row + rows))] for i in range(ref.shape[-3])]
    return jnp.concatenate(parts, 1)


def put(ref, *index, value):
    rows = value.shape[0]
    for i in range(ref.shape[-3]):
        part = value[:, 128 * i : 128 * (i + 1)]
        ref[(*index, i, slice(0, rows))] = part
        ref[(*index, i, slice(rows, rows + 8))] = part[:8]


def gather_modes(v, up, ahead, ahead_up):
    near = (v + up, up - v)
    far = (ahead + ahead_up, ahead_up - ahead)
    out = {}
    for by in (0, 1):
        out[by, 0] = near[by] + far[by]
        out[by, 1] = far[by] - near[by]
    return out


def scatter_modes(r, below):
    part = []
    for bz in (0, 1):
        part.append((r[0, bz] - r[1, bz]) + (below[0, bz] + below[1, bz]))
    return part[0] - part[1], part[0] + part[1]


def voxel_forces(c, stiff):
    lam = (LAMBDA_SOFT / 16) + (LAMBDA_RISE / 16) * stiff
    mu = (SHEAR_SOFT / 16) + (SHEAR_RISE / 16) * stiff
    mu2 = mu + mu
    lam3 = lam * (1.0 / 3)
    mu3 = mu * (1.0 / 3)
    top = ((LAMBDA_SOFT + 4 * SHEAR_SOFT) / 144) + ((LAMBDA_RISE + 4 * SHEAR_RISE) / 144) * stiff
    f = {}
    normal = ((0, 1, 0, 0), (1, 0, 1, 0), (2, 0, 0, 1))
    t = lam * (c[normal[0]] + c[normal[1]] + c[normal[2]])
    for p in normal:
        f[p] = t + mu2 * c[p]
    for p, q in (
        ((0, 1, 1, 0), (2, 0, 1, 1)),
        ((0, 1, 0, 1), (1, 0, 1, 1)),
        ((1, 1, 1, 0), (2, 1, 0, 1)),
    ):
        t = lam3 * (c[p] + c[q])
        f[p] = t + mu * c[p]
        f[q] = t + mu * c[q]
    for comp in range(3):
        p = (comp, 1, 1, 1)
        f[p] = top * c[p]
    for p, q in (
        ((0, 0, 1, 0), (1, 1, 0, 0)),
        ((0, 0, 0, 1), (2, 1, 0, 0)),
        ((1, 0, 0, 1), (2, 0, 1, 0)),
    ):
        f[p] = f[q] = mu * (c[p] + c[q])
    bend = ((0, 0, 1, 1), (1, 1, 0, 1), (2, 1, 1, 0))
    t = c[bend[0]] + c[bend[1]] + c[bend[2]]
    for p in bend:
        f[p] = mu3 * (t + c[p])
    return f


MODES = [(comp, by, bz) for comp in range(3) for by in (0, 1) for bz in (0, 1)]


def strides(start, stop, width, body, carry):
    def several(i, carry):
        return body(start + width * i, carry)

    return lax.fori_loop(0, -((start - stop) // width), several, carry)


def pairs(start, stop, body, carry):
    return strides(start, stop, 2, lambda n, c: body(n + 1, body(n, c)), carry)


def tiles_of(rows, depth):
    return [(slice(a, a + 8), slice(b, b + 128)) for a in range(0, rows, 8) for b in range(0, depth, 128)]


def diagonal_layer(cells, turned, edge, first_row):
    lz = cells + turned
    row_id = lax.broadcasted_iota(jnp.int32, lz.shape, 0)
    return lz + jnp.where(row_id == first_row, jnp.broadcast_to(edge, lz.shape), roll(lz, 1, 0))


def diagonal_from(two_layers):
    base = 8 * (LAMBDA_SOFT + 4 * SHEAR_SOFT) / 9 + KAPPA
    return base + ((LAMBDA_RISE + 4 * SHEAR_RISE) / 9) * two_layers


def forward_planes(first, last, node_ref, turn_ref, q_ref):
    rows = node_ref.shape[-2] - 8
    tiles = tiles_of(rows, 128 * node_ref.shape[-3])
    for n in range(first, last):
        for comp in range(3):
            put(turn_ref, comp, n, value=roll(get(node_ref, comp, n), -1, 1))

    def forward(n, _):
        for comp in range(3):
            out = gather_modes(
                get(node_ref, comp, n),
                get(node_ref, comp, n, row=1, rows=rows),
                get(turn_ref, comp, n),
                get(turn_ref, comp, n, row=1, rows=rows),
            )
            for i, (cc, by, bz) in enumerate(MODES):
                if cc == comp:
                    for j, tile in enumerate(tiles):
                        q_ref[n, i, j] = out[by, bz][tile]
        return _

    even = first + (last - first) // 2 * 2
    pairs(first, even, forward, 0)
    for n in range(even, last):
        forward(n, 0)


def voxel_layers(j, first, last, cells_at, q_ref, f_ref):
    across, tall = f_ref.shape[-3], f_ref.shape[-2]
    line, lanes = divmod(j, across)
    row = 8 * (line + 1)

    def store(n, i, value):
        f_ref[n, i, lanes, row : row + 8] = value
        if row + 8 == tall:
            f_ref[n, i, lanes, 0:8] = value

    def voxels(n, carry):
        near, behind = carry
        far = [q_ref[n + 1, i, j] for i in range(len(MODES))]
        c = {}
        for i, (comp, by, bz) in enumerate(MODES):
            if (by, bz) != (0, 0):
                c[comp, 0, by, bz] = near[i] + far[i]
            c[comp, 1, by, bz] = far[i] - near[i]
        f = voxel_forces(c, cells_at(n))
        ahead = []
        for i, (comp, by, bz) in enumerate(MODES):
            up = f[comp, 1, by, bz]
            if (by, bz) != (0, 0):
                flat = f[comp, 0, by, bz]
                store(n, i, behind[i] + (flat - up))
                ahead.append(flat + up)
            else:
                store(n, i, behind[i] - up)
                ahead.append(up)
        return far, ahead

    near = [q_ref[first, i, j] for i in range(len(MODES))]
    carry = near, [jnp.zeros_like(v) for v in near]
    even = first + (last - first) // 2 * 2
    carry = pairs(first, even, voxels, carry)
    for n in range(even, last):
        carry = voxels(n, carry)


def collect(n, f_ref, image_ref):
    rows = f_ref.shape[-2] - 8
    for comp in range(3):
        here, below = {}, {}
        for i, (cc, by, bz) in enumerate(MODES):
            if cc == comp:
                here[by, bz] = get(f_ref, n, i, row=8, rows=rows)
                below[by, bz] = get(f_ref, n, i, row=7, rows=rows)
        kept, moved = scatter_modes(here, below)
        image_ref[comp, n] = kept + roll(moved, 1, 1)


def update(k, inv):
    gain = inv * (1 / STEP[k])
    own = KAPPA * gain - SHIFT[k] / STEP[k]

    def new(force, t, older):
        out = force * gain + t * own
        return out - (STEP[k - 1] / STEP[k]) * older() if k > 1 else out

    return new


def packed_sums(totals):
    lane = lax.broadcasted_iota(jnp.int32, (1, 128), 1)
    packed = jnp.zeros((1, 128), jnp.float32)
    for i, v in enumerate(totals):
        s = jnp.sum(jnp.sum(v, axis=0, keepdims=True), axis=1, keepdims=True)
        packed = jnp.where(lane == i, s, packed)
    return packed


def y_parts(own_x):
    h = HALO
    mid = own_x - 2 * h

    def node(comp, x):
        if x < h:
            return 0, 4 * h + 1 + comp * h + x
        if x >= own_x - h:
            return 0, comp * h + x - (own_x - h)
        return 1, comp * mid + x - h

    def cell(x):
        if x < h:
            return 0, 7 * h + 1 + x
        if x >= own_x - h - 1:
            return 0, 3 * h + x - (own_x - h - 1)
        return 1, 3 * mid + x - h

    def edge(x):
        if x < h:
            return 0, h + 1 + x
        if x >= own_x - h - 1:
            return 0, x - (own_x - h - 1)
        return 1, x - h

    blocks = (8 * h + 1, 4 * mid - 1)
    edge_blocks = (-(-(2 * h + 1) // h), -(-(mid - 1) // h))
    return node, cell, edge, blocks, edge_blocks


def begin_kernel(
    r_own, lab_own, side_a, side_b, edge_a, edge_b,
    side_out, t_out, next_out, inv_out, d_out, sums_out,
    edge_ref, turn_ref, image_ref, q_ref, f_ref,
):
    own_x, own_y, depth = r_own.shape[1:]

    def both(block, side):
        return jnp.concatenate([block, side], 0)

    node_at, cell_at, edge_at = y_parts(own_x)[:3]
    sides, edges = (side_a, side_b), (edge_a, edge_b)
    for x in range(own_x):
        for comp in range(3):
            part, place = node_at(comp, x)
            side_out[comp, x] = sides[part][place]
        part, place = cell_at(x)
        side_out[3, x] = sides[part][place]
        part, place = edge_at(x)
        edge_ref[x : x + 1] = edges[part][place : place + 1]
    lines = edge_ref[...]
    edge_ref[...] = lines + roll(lines, 1, 1)
    for m in range(own_x):
        image_ref[0, m] = roll(both(lab_own[m], side_out[3, m]), 1, 1)

    def layer(m):
        cells = both(lab_own[m], side_out[3, m])
        return diagonal_layer(cells, image_ref[0, m], edge_ref[pl.ds(m, 1), :], own_y + HALO)

    def start(x, before):
        here = layer(x)
        diag = diagonal_from(before + here)
        inv = 1.0 / diag
        inv_out[x] = inv
        d_out[x] = diag[:own_y]
        for comp in range(3):
            put(t_out, comp, x, value=both(r_own[comp, x], side_out[comp, x]) * inv)
        return here

    before = pairs(1, own_x - 1, start, layer(0))
    start(own_x - 1, before)

    forward_planes(1, own_x, t_out, turn_ref, q_ref)
    for j, (line, lanes) in enumerate(tiles_of(own_y + side_a.shape[1], depth)):

        def cells_at(n):
            if line.start < own_y:
                return lab_own[n, line, lanes]
            return side_out[3, n, line.start - own_y : line.stop - own_y, lanes]

        voxel_layers(j, 1, own_x - 1, cells_at, q_ref, f_ref)

    def advance(x, acc):
        energy, right = acc
        new = update(0, inv_out[x])
        for comp in range(3):
            t = get(t_out, comp, x)
            force = image_ref[comp, x]
            energy += t[:own_y] * (force[:own_y] + KAPPA * t[:own_y])
            right += t[:own_y] * r_own[comp, x]
            put(next_out, comp, x, value=new(force, t, None))
        return energy, right

    def several(n, acc):
        for u in range(WIDTH):
            acc = advance(n + u, acc)
        for u in range(WIDTH):
            collect(n + WIDTH + u, f_ref, image_ref)
        return acc

    for x in range(2, 2 + WIDTH):
        collect(x, f_ref, image_ref)
    whole = 2 + (own_x - 3) // WIDTH * WIDTH
    acc = strides(2, whole, WIDTH, several, (jnp.zeros((own_y, depth), jnp.float32),) * 2)
    for x in range(whole, own_x - 1):
        acc = advance(x, acc)
    sums_out[...] = packed_sums(acc)


def basis_kernel(
    r_own, lab_own, side_ref, edge_a, below, above, below_side, above_side, t0_in, t1_in, inv_in, sums_in,
    t_out, d_out, sums_out,
    cell_ref, inv_ref, t_ref, turn_ref, image_ref, q_ref, f_ref,
):
    h = HALO
    own_x, own_y, depth = r_own.shape[1:]
    rows = own_y + side_ref.shape[2]
    tiles = tiles_of(rows, depth)
    planes = own_x + 2 * h
    lo, hi = h, h + own_x
    edge_at = y_parts(own_x)[2]

    def nodes(comp, x):
        if x < 0:
            return jnp.concatenate([below[comp * h + h + x], below_side[comp * h + h + x]], 0)
        if x >= own_x:
            i = comp * h + x - own_x
            return jnp.concatenate([above[i], above_side[i]], 0)
        return jnp.concatenate([r_own[comp, x], side_ref[comp, x]], 0)

    def edge(x):
        if x < 0:
            return below_side[4 * h + 1, h + 1 + x : h + 2 + x]
        if x >= own_x:
            return above_side[4 * h, x - own_x : x - own_x + 1]
        place = edge_at(x)[1]
        return edge_a[place : place + 1]

    for i in range(h + 1):
        cell_ref[i] = jnp.concatenate([below[3 * h + i], below_side[3 * h + i]], 0)
    for i in range(h):
        cell_ref[h + 1 + own_x + i] = jnp.concatenate([above[3 * h + i], above_side[3 * h + i]], 0)

    def copy(x, _):
        cell_ref[x + h + 1] = jnp.concatenate([lab_own[x], side_ref[3, x]], 0)
        inv_ref[x + h] = inv_in[x]
        for comp in range(3):
            t = get(t0_in, comp, x)
            put(t_ref, 0, comp, x + h, value=t)
            t_out[0, comp, x] = t[:own_y]
            t = get(t1_in, comp, x)
            put(t_ref, 1, comp, x + h, value=t)
            t_out[1, comp, x] = t[:own_y]
        return _

    pairs(0, own_x, copy, 0)

    def layer(x):
        e = edge(x)
        c = cell_ref[x + h + 1]
        return diagonal_layer(c, roll(c, 1, 1), e + roll(e, 1, 1), own_y + h)

    for start, stop in ((-h, 1), (own_x, own_x + h)):
        layers = [layer(x) for x in range(start - 1, stop)]
        for x in range(start, stop):
            diag = diagonal_from(layers[x - start] + layers[x - start + 1])
            inv = 1.0 / diag
            inv_ref[x + h] = inv
            if x == 0:
                d_out[...] = diag[:own_y]
            for comp in range(3):
                t = nodes(comp, x) * inv
                put(t_ref, 0, comp, x + h, value=t)
                if x == 0:
                    t_out[0, comp, 0] = t[:own_y]

    totals = []
    for k in range(ITERS):
        first, last = k, planes - k
        runs = [(first, last)] if k > 0 else [(0, h + 3), (planes - h - 2, planes)]
        for start, stop in runs:
            forward_planes(start, stop, t_ref.at[k], turn_ref, q_ref)
        for j, (line, lanes) in enumerate(tiles):
            for start, stop in runs:
                cells_at = lambda n: cell_ref[n + 1, line, lanes]
                voxel_layers(j, start, stop - 1, cells_at, q_ref, f_ref)

        def advance(n, own, acc):
            acc = list(acc)
            new = update(k, inv_ref[n])
            for comp in range(3):
                t = get(t_ref, k, comp, n)
                force = image_ref[comp, n]
                if own:
                    image = force[:own_y] + KAPPA * t[:own_y]
                    for j in range(k + 1):
                        acc[j] += get(t_ref, j, comp, n, rows=own_y) * image
                    acc[k + 1] += t[:own_y] * r_own[comp, n - lo]
                t = new(force, t, lambda: get(t_ref, k - 1, comp, n))
                if k + 1 < ITERS:
                    put(t_ref, k + 1, comp, n, value=t)
                if own:
                    t_out[k + 1, comp, n - lo] = t[:own_y]
            return tuple(acc)

        def several(n, acc):
            for u in range(WIDTH):
                acc = advance(n + u, True, acc)
            for u in range(WIDTH):
                collect(n + WIDTH + u, f_ref, image_ref)
            return acc

        if k == 0:
            ends = [n for start, stop in runs for n in range(start + 1, stop - 1)]
            for n in ends:
                collect(n, f_ref, image_ref)
            acc = (jnp.zeros((own_y, depth), jnp.float32),) * 2
            for n in ends:
                acc = advance(n, lo <= n < hi, acc)
            totals.extend(acc)
            continue

        beside = [*range(first + 1, lo), *range(hi, last - 1)] if k + 1 < ITERS else []
        for n in [*beside, *range(lo, lo + WIDTH)]:
            collect(n, f_ref, image_ref)
        for n in beside:
            advance(n, False, ())
        acc = (jnp.zeros((own_y, depth), jnp.float32),) * (k + 2)
        whole = lo + own_x // WIDTH * WIDTH
        acc = strides(lo, whole, WIDTH, several, acc)
        for n in range(whole, hi):
            acc = advance(n, True, acc)
        totals.extend(acc)
    sums_out[...] = jnp.broadcast_to((packed_sums(totals) + sums_in[...])[None], sums_out.shape)


def pack_kernel(
    r_hbm, lab_hbm, r_out, lab_out, up_a, down_a, up_b, down_b, next_out, previous_out, lab_in, arrived
):
    h = HALO
    own_x, own_y = lab_in.shape[:2]
    copies = [
        pltpu.make_async_copy(r_hbm, r_out, arrived.at[0]),
        pltpu.make_async_copy(lab_hbm, lab_in, arrived.at[1]),
    ]
    for copy in copies:
        copy.start()
    for copy in copies:
        copy.wait()

    ups, downs = (up_a, up_b), (down_a, down_b)
    node_at, cell_at, edge_at, blocks, _ = y_parts(own_x)
    for x in range(own_x):
        l = lab_in[x].astype(jnp.float32)
        lab_out[x] = l
        part, place = cell_at(x)
        ups[part][place] = l[own_y - h :]
        downs[part][place] = l[:h]
        part, place = edge_at(x)
        ups[part][blocks[part] + place // h, place % h : place % h + 1] = l[own_y - h - 1 : own_y - h]
        if x < h:
            previous_out[3 * h + x] = l
        if x >= own_x - h - 1:
            next_out[3 * h + x - (own_x - h - 1)] = l
        for comp in range(3):
            r = r_out[comp, x]
            part, place = node_at(comp, x)
            ups[part][place] = r[own_y - h :]
            downs[part][place] = r[:h]
            if x < h:
                previous_out[comp * h + x] = r
            if x >= own_x - h:
                next_out[comp * h + x - (own_x - h)] = r


def combine_kernel(sums_ref, t_ref, d_ref, d_first, x_out, r_out):
    total = jnp.sum(sums_ref[...], axis=0, keepdims=True)
    lane = lax.broadcasted_iota(jnp.int32, total.shape, 1)
    entry = [
        jnp.sum(jnp.where(lane == i, total, 0.0), axis=1, keepdims=True) for i in range(SUMS)
    ]
    gram, right = {}, []
    place = 0
    for k in range(ITERS):
        for j in range(k + 1):
            gram[j, k] = gram[k, j] = entry[place]
            place += 1
        right.append(entry[place])
        place += 1
    scale = [gram[k, k] for k in range(ITERS)]
    inv, low = [], {}
    for k in range(ITERS):
        pivot = gram[k, k]
        good = pivot > 1e-7 * scale[k]
        inv.append(jnp.where(good, 1.0 / jnp.where(good, pivot, 1.0), 0.0))
        for i in range(k + 1, ITERS):
            low[i, k] = gram[i, k] * inv[k]
        for i in range(k + 1, ITERS):
            for j in range(k + 1, i + 1):
                gram[i, j] = gram[j, i] = gram[i, j] - low[i, k] * gram[j, k]
            right[i] = right[i] - low[i, k] * right[k]
    y = [None] * ITERS
    for k in reversed(range(ITERS)):
        y[k] = right[k] * inv[k]
        for i in range(k + 1, ITERS):
            y[k] = y[k] - low[i, k] * y[i]
    e = [jnp.ones_like(y[0])] + [jnp.zeros_like(y[0]) for _ in range(ITERS)]
    for k in range(ITERS):
        e[k + 1] = e[k + 1] - STEP[k] * y[k]
        e[k] = e[k] - SHIFT[k] * y[k]
        if k > 1:
            e[k - 1] = e[k - 1] - STEP[k - 1] * y[k]
    y = [jnp.broadcast_to(v, d_first.shape) for v in y]
    e = [jnp.broadcast_to(v, d_first.shape) for v in e]

    def plane(n, diag):
        for comp in range(3):
            t = [t_ref[k, comp, n] for k in range(ITERS + 1)]
            x, r = y[0] * t[0], e[0] * t[0]
            for k in range(1, ITERS):
                x = x + y[k] * t[k]
                r = r + e[k] * t[k]
            r = r + e[ITERS] * t[ITERS]
            x_out[comp, n] = x
            r_out[comp, n] = r * diag

    def body(n, _):
        plane(n, d_ref[n])
        return _

    plane(0, d_first[...])
    pairs(1, d_ref.shape[0] - 1, body, 0)
    plane(d_ref.shape[0] - 1, d_ref[d_ref.shape[0] - 1])


def local(right_side, labels):
    own_x, own_y, depth = labels.shape
    h = HALO
    f32 = jnp.float32
    devices = lax.axis_size("gx") * lax.axis_size("gy")
    small = pltpu.CompilerParams(vmem_limit_bytes=16 * 2**20)
    blocks, edge_blocks = y_parts(own_x)[3:]
    right_side, lab, up_a, down_a, up_b, down_b, to_next, to_previous = pl.pallas_call(
        pack_kernel,
        out_shape=(
            jax.ShapeDtypeStruct(right_side.shape, f32),
            jax.ShapeDtypeStruct(labels.shape, f32),
            jax.ShapeDtypeStruct((blocks[0] + edge_blocks[0], h, depth), f32),
            jax.ShapeDtypeStruct((blocks[0], h, depth), f32),
            jax.ShapeDtypeStruct((blocks[1] + edge_blocks[1], h, depth), f32),
            jax.ShapeDtypeStruct((blocks[1], h, depth), f32),
            jax.ShapeDtypeStruct((4 * h + 1, own_y, depth), f32),
            jax.ShapeDtypeStruct((4 * h, own_y, depth), f32),
        ),
        in_specs=[pl.BlockSpec(memory_space=pltpu.HBM)] * 2,
        scratch_shapes=[pltpu.VMEM(labels.shape, jnp.int32), pltpu.SemaphoreType.DMA((2,))],
        compiler_params=small,
        name="pack",
    )(*(pltpu.with_memory_space_constraint(v, pltpu.HBM) for v in (right_side, labels)))

    minus_a, plus_a = shifted(up_a, "gy", 1), shifted(down_a, "gy", -1)
    minus_b, plus_b = shifted(up_b, "gy", 1), shifted(down_b, "gy", -1)
    below = shifted(to_next, "gx", 1)
    above = shifted(to_previous, "gx", -1)
    minus_a, plus_a, below, above = lax.optimization_barrier((minus_a, plus_a, below, above))

    def stack(minus, plus, count):
        side = jnp.concatenate([plus[:count], minus[:count]], 1)
        return side, minus[count:].reshape(-1, depth)

    def corner(block, rows):
        rows = jnp.pad(rows, ((0, 2 * h - rows.shape[0]), (0, 0)))
        return jnp.concatenate([block, rows[None]], 0)

    side_a, edge_a = stack(minus_a, plus_a, blocks[0])
    below_side = shifted(corner(side_a[: 4 * h + 1], edge_a[: h + 1]), "gx", 1)
    last = corner(side_a[4 * h + 1 :], edge_a[h + 1 : 2 * h + 1])
    above_side = shifted(last, "gx", -1)
    side_b, edge_b = stack(minus_b, plus_b, blocks[1])

    rows = own_y + 2 * h
    tiles = (rows // 8) * (depth // 128)

    across = depth // 128

    def kept(*lead):
        return pltpu.VMEM((*lead, across, rows + 8, 128), f32)

    def scratch(planes):
        return [
            kept(ITERS, 3, planes),
            kept(3, planes),
            pltpu.VMEM((3, planes, rows, depth), f32),
            pltpu.VMEM((planes, len(MODES), tiles + 1, 8, 128), f32),
            kept(planes, len(MODES)),
        ]

    own_kept = jax.ShapeDtypeStruct((3, own_x, across, rows + 8, 128), f32)
    side, t0, t1, inverse, diagonal, first_sums = pl.pallas_call(
        begin_kernel,
        out_shape=(
            jax.ShapeDtypeStruct((4, own_x, 2 * h, depth), f32),
            own_kept,
            own_kept,
            jax.ShapeDtypeStruct((own_x, rows, depth), f32),
            jax.ShapeDtypeStruct((own_x, own_y, depth), f32),
            jax.ShapeDtypeStruct((1, 128), f32),
        ),
        scratch_shapes=[pltpu.VMEM((own_x, depth), f32), *scratch(own_x + WIDTH)[1:]],
        compiler_params=pltpu.CompilerParams(vmem_limit_bytes=24 * 2**20),
        name="begin",
    )(right_side, lab, side_a, side_b, edge_a, edge_b)

    planes = own_x + 2 * h
    basis, d_first, sums = pl.pallas_call(
        basis_kernel,
        out_shape=(
            jax.ShapeDtypeStruct((ITERS + 1, 3, own_x, own_y, depth), f32),
            jax.ShapeDtypeStruct((own_y, depth), f32),
            jax.ShapeDtypeStruct((devices, 1, 128), f32),
        ),
        scratch_shapes=[
            pltpu.VMEM((planes + 2, rows, depth), f32),
            pltpu.VMEM((planes, rows, depth), f32),
            *scratch(planes + 1),
        ],
        compiler_params=pltpu.CompilerParams(vmem_limit_bytes=34 * 2**20),
        name="basis",
    )(
        right_side, lab, side, edge_a, below, above, below_side, above_side,
        t0, t1, inverse, first_sums,
    )

    everyone = lax.all_to_all(sums, ("gx", "gy"), 0, 0)
    out = jax.ShapeDtypeStruct(right_side.shape, f32)
    return pl.pallas_call(combine_kernel, out_shape=(out, out), compiler_params=small, name="combine")(
        everyone.reshape(devices, 128), basis, diagonal, d_first
    )


def solution(mesh):
    in_specs = (P(None, "gx", "gy", None), P("gx", "gy", None))
    out_specs = (P(None, "gx", "gy", None), P(None, "gx", "gy", None))
    return jax.shard_map(local, mesh=mesh, in_specs=in_specs, out_specs=out_specs, check_vma=False)
```

```python
import jax
import jax.numpy as jnp
from jax import lax
from jax.experimental import pallas as pl
from jax.experimental.pallas import tpu as pltpu
from jax.sharding import PartitionSpec as P


ITERS = 4
HALO = ITERS
LAMBDA_SOFT = 0.5769231
LAMBDA_RISE = 1.6452991
SHEAR_SOFT = 0.3846154
SHEAR_RISE = 2.9487179
KAPPA = 0.05
SHIFT = (0.25, 1.6, 1.5, 1.5)
STEP = (1.0, 0.6, 0.6, 0.6)
SUMS = 14
WIDTH = 4


def shifted(shard, axis, by):
    size = lax.axis_size(axis)
    return lax.ppermute(shard, axis, [(i, (i + by) % size) for i in range(size)])


def roll(v, by, axis):
    return pltpu.roll(v, by % v.shape[axis], axis)


def get(ref, *index, row=0, rows=None):
    rows = ref.shape[-2] - 8 if rows is None else rows
    parts = [ref[(*index, i, slice(row, row + rows))] for i in range(ref.shape[-3])]
    return jnp.concatenate(parts, 1)


def put(ref, *index, value):
    rows = value.shape[0]
    for i in range(ref.shape[-3]):
        part = value[:, 128 * i : 128 * (i + 1)]
        ref[(*index, i, slice(0, rows))] = part
        ref[(*index, i, slice(rows, rows + 8))] = part[:8]


def gather_modes(v, up, ahead, ahead_up):
    near = (v + up, up - v)
    far = (ahead + ahead_up, ahead_up - ahead)
    out = {}
    for by in (0, 1):
        out[by, 0] = near[by] + far[by]
        out[by, 1] = far[by] - near[by]
    return out


def scatter_modes(r, below):
    part = []
    for bz in (0, 1):
        part.append((r[0, bz] - r[1, bz]) + (below[0, bz] + below[1, bz]))
    return part[0] - part[1], part[0] + part[1]


def voxel_forces(c, stiff):
    lam = (LAMBDA_SOFT / 16) + (LAMBDA_RISE / 16) * stiff
    mu = (SHEAR_SOFT / 16) + (SHEAR_RISE / 16) * stiff
    mu2 = mu + mu
    lam3 = lam * (1.0 / 3)
    mu3 = mu * (1.0 / 3)
    top = ((LAMBDA_SOFT + 4 * SHEAR_SOFT) / 144) + ((LAMBDA_RISE + 4 * SHEAR_RISE) / 144) * stiff
    f = {}
    normal = ((0, 1, 0, 0), (1, 0, 1, 0), (2, 0, 0, 1))
    t = lam * (c[normal[0]] + c[normal[1]] + c[normal[2]])
    for p in normal:
        f[p] = t + mu2 * c[p]
    for p, q in (
        ((0, 1, 1, 0), (2, 0, 1, 1)),
        ((0, 1, 0, 1), (1, 0, 1, 1)),
        ((1, 1, 1, 0), (2, 1, 0, 1)),
    ):
        t = lam3 * (c[p] + c[q])
        f[p] = t + mu * c[p]
        f[q] = t + mu * c[q]
    for comp in range(3):
        p = (comp, 1, 1, 1)
        f[p] = top * c[p]
    for p, q in (
        ((0, 0, 1, 0), (1, 1, 0, 0)),
        ((0, 0, 0, 1), (2, 1, 0, 0)),
        ((1, 0, 0, 1), (2, 0, 1, 0)),
    ):
        f[p] = f[q] = mu * (c[p] + c[q])
    bend = ((0, 0, 1, 1), (1, 1, 0, 1), (2, 1, 1, 0))
    t = c[bend[0]] + c[bend[1]] + c[bend[2]]
    for p in bend:
        f[p] = mu3 * (t + c[p])
    return f


MODES = [(comp, by, bz) for comp in range(3) for by in (0, 1) for bz in (0, 1)]


def strides(start, stop, width, body, carry):
    def several(i, carry):
        return body(start + width * i, carry)

    return lax.fori_loop(0, -((start - stop) // width), several, carry)


def pairs(start, stop, body, carry):
    return strides(start, stop, 2, lambda n, c: body(n + 1, body(n, c)), carry)


def tiles_of(rows, depth):
    return [(slice(a, a + 8), slice(b, b + 128)) for a in range(0, rows, 8) for b in range(0, depth, 128)]


def diagonal_layer(cells, turned, edge, first_row):
    lz = cells + turned
    row_id = lax.broadcasted_iota(jnp.int32, lz.shape, 0)
    return lz + jnp.where(row_id == first_row, jnp.broadcast_to(edge, lz.shape), roll(lz, 1, 0))


def diagonal_from(two_layers):
    base = 8 * (LAMBDA_SOFT + 4 * SHEAR_SOFT) / 9 + KAPPA
    return base + ((LAMBDA_RISE + 4 * SHEAR_RISE) / 9) * two_layers


def turn_plane(n, node_ref, turn_ref):
    for comp in range(3):
        put(turn_ref, comp, n, value=roll(get(node_ref, comp, n), -1, 1))


def forward_planes(first, last, node_ref, turn_ref, q_ref):
    rows = node_ref.shape[-2] - 8
    tiles = tiles_of(rows, 128 * node_ref.shape[-3])

    def forward(n, _):
        for comp in range(3):
            out = gather_modes(
                get(node_ref, comp, n),
                get(node_ref, comp, n, row=1, rows=rows),
                get(turn_ref, comp, n),
                get(turn_ref, comp, n, row=1, rows=rows),
            )
            for i, (cc, by, bz) in enumerate(MODES):
                if cc == comp:
                    for j, tile in enumerate(tiles):
                        q_ref[n, i, j] = out[by, bz][tile]
        return _

    even = first + (last - first) // 2 * 2
    pairs(first, even, forward, 0)
    for n in range(even, last):
        forward(n, 0)


def voxel_layers(j, first, last, cells_at, q_ref, f_ref):
    across, tall = f_ref.shape[-3], f_ref.shape[-2]
    line, lanes = divmod(j, across)
    row = 8 * (line + 1)

    def store(n, i, value):
        f_ref[n, i, lanes, row : row + 8] = value
        if row + 8 == tall:
            f_ref[n, i, lanes, 0:8] = value

    def voxels(n, carry):
        near, behind = carry
        far = [q_ref[n + 1, i, j] for i in range(len(MODES))]
        c = {}
        for i, (comp, by, bz) in enumerate(MODES):
            if (by, bz) != (0, 0):
                c[comp, 0, by, bz] = near[i] + far[i]
            c[comp, 1, by, bz] = far[i] - near[i]
        f = voxel_forces(c, cells_at(n))
        ahead = []
        for i, (comp, by, bz) in enumerate(MODES):
            up = f[comp, 1, by, bz]
            if (by, bz) != (0, 0):
                flat = f[comp, 0, by, bz]
                store(n, i, behind[i] + (flat - up))
                ahead.append(flat + up)
            else:
                store(n, i, behind[i] - up)
                ahead.append(up)
        return far, ahead

    near = [q_ref[first, i, j] for i in range(len(MODES))]
    pairs(first, last, voxels, (near, [jnp.zeros_like(v) for v in near]))


def collect(n, f_ref, image_ref):
    rows = f_ref.shape[-2] - 8
    for comp in range(3):
        here, below = {}, {}
        for i, (cc, by, bz) in enumerate(MODES):
            if cc == comp:
                here[by, bz] = get(f_ref, n, i, row=8, rows=rows)
                below[by, bz] = get(f_ref, n, i, row=7, rows=rows)
        kept, moved = scatter_modes(here, below)
        image_ref[comp, n] = kept + roll(moved, 1, 1)


def update(k, inv):
    gain = inv * (1 / STEP[k])
    own = KAPPA * gain - SHIFT[k] / STEP[k]

    def new(force, t, older):
        out = force * gain + t * own
        return out - (STEP[k - 1] / STEP[k]) * older() if k > 1 else out

    return new


def packed_sums(totals):
    lane = lax.broadcasted_iota(jnp.int32, (1, 128), 1)
    packed = jnp.zeros((1, 128), jnp.float32)
    for i, v in enumerate(totals):
        s = jnp.sum(jnp.sum(v, axis=0, keepdims=True), axis=1, keepdims=True)
        packed = jnp.where(lane == i, s, packed)
    return packed


def y_parts(own_x):
    h = HALO
    mid = own_x - 2 * h

    def node(comp, x):
        if x < h:
            return 0, 4 * h + 1 + comp * h + x
        if x >= own_x - h:
            return 0, comp * h + x - (own_x - h)
        return 1, comp * mid + x - h

    def cell(x):
        if x < h:
            return 0, 7 * h + 1 + x
        if x >= own_x - h - 1:
            return 0, 3 * h + x - (own_x - h - 1)
        return 1, 3 * mid + x - h

    def edge(x):
        if x < h:
            return 0, h + 1 + x
        if x >= own_x - h - 1:
            return 0, x - (own_x - h - 1)
        return 1, x - h

    blocks = (8 * h + 1, 4 * mid - 1)
    edge_blocks = (-(-(2 * h + 1) // h), -(-(mid - 1) // h))
    return node, cell, edge, blocks, edge_blocks


def begin_kernel(
    r_own, lab_own, side_a, side_b, edge_a, edge_b,
    side_out, t_out, next_out, next_turn, inv_out, d_out, sums_out,
    edge_ref, turn_ref, image_ref, q_ref, f_ref,
):
    own_x, own_y, depth = r_own.shape[1:]

    def both(block, side):
        return jnp.concatenate([block, side], 0)

    node_at, cell_at, edge_at = y_parts(own_x)[:3]
    sides, edges = (side_a, side_b), (edge_a, edge_b)
    for x in range(own_x):
        for comp in range(3):
            part, place = node_at(comp, x)
            side_out[comp, x] = sides[part][place]
        part, place = cell_at(x)
        side_out[3, x] = sides[part][place]
        part, place = edge_at(x)
        edge_ref[x : x + 1] = edges[part][place : place + 1]
    lines = edge_ref[...]
    edge_ref[...] = lines + roll(lines, 1, 1)
    for m in range(own_x):
        image_ref[0, m] = roll(both(lab_own[m], side_out[3, m]), 1, 1)

    def layer(m):
        cells = both(lab_own[m], side_out[3, m])
        return diagonal_layer(cells, image_ref[0, m], edge_ref[pl.ds(m, 1), :], own_y + HALO)

    def start(x, before):
        here = layer(x)
        diag = diagonal_from(before + here)
        inv = 1.0 / diag
        inv_out[x] = inv
        d_out[x] = diag[:own_y]
        for comp in range(3):
            put(t_out, comp, x, value=both(r_own[comp, x], side_out[comp, x]) * inv)
        return here

    before = pairs(1, own_x - 1, start, layer(0))
    start(own_x - 1, before)

    for x in range(1, own_x):
        turn_plane(x, t_out, turn_ref)
    forward_planes(1, own_x, t_out, turn_ref, q_ref)
    for j, (line, lanes) in enumerate(tiles_of(own_y + side_a.shape[1], depth)):

        def cells_at(n):
            if line.start < own_y:
                return lab_own[n, line, lanes]
            return side_out[3, n, line.start - own_y : line.stop - own_y, lanes]

        voxel_layers(j, 1, own_x - 1, cells_at, q_ref, f_ref)

    def advance(x, acc):
        energy, right = acc
        new = update(0, inv_out[x])
        for comp in range(3):
            t = get(t_out, comp, x)
            force = image_ref[comp, x]
            energy += t[:own_y] * (force[:own_y] + KAPPA * t[:own_y])
            right += t[:own_y] * r_own[comp, x]
            put(next_out, comp, x + HALO, value=new(force, t, None))
        return energy, right

    def several(n, acc):
        for u in range(WIDTH):
            turn_plane(n + HALO - WIDTH + u, next_out, next_turn)
        for u in range(WIDTH):
            acc = advance(n + u, acc)
        for u in range(WIDTH):
            collect(n + WIDTH + u, f_ref, image_ref)
        return acc

    for x in range(2, 2 + WIDTH):
        collect(x, f_ref, image_ref)
    whole = 2 + (own_x - 3) // WIDTH * WIDTH
    acc = strides(2, whole, WIDTH, several, (jnp.zeros((own_y, depth), jnp.float32),) * 2)
    for x in range(whole, own_x - 1):
        acc = advance(x, acc)
    for x in range(whole - WIDTH, own_x - 1):
        turn_plane(x + HALO, next_out, next_turn)
    sums_out[...] = packed_sums(acc)


def basis_kernel(
    r_own, lab_own, side_ref, edge_a, below, above, below_side, above_side, t0_in, t1_in, turn1_in, inv_in, sums_in,
    t_out, d_out, sums_out,
    cell_ref, inv_ref, t_ref, turn_ref, image_ref, q_ref, f_ref,
):
    h = HALO
    own_x, own_y, depth = r_own.shape[1:]
    rows = own_y + side_ref.shape[2]
    tiles = tiles_of(rows, depth)
    planes = own_x + 2 * h
    lo, hi = h, h + own_x
    edge_at = y_parts(own_x)[2]

    def nodes(comp, x):
        if x < 0:
            return jnp.concatenate([below[comp * h + h + x], below_side[comp * h + h + x]], 0)
        if x >= own_x:
            i = comp * h + x - own_x
            return jnp.concatenate([above[i], above_side[i]], 0)
        return jnp.concatenate([r_own[comp, x], side_ref[comp, x]], 0)

    def edge(x):
        if x < 0:
            return below_side[4 * h + 1, h + 1 + x : h + 2 + x]
        if x >= own_x:
            return above_side[4 * h, x - own_x : x - own_x + 1]
        place = edge_at(x)[1]
        return edge_a[place : place + 1]

    for i in range(h + 1):
        cell_ref[i] = jnp.concatenate([below[3 * h + i], below_side[3 * h + i]], 0)
    for i in range(h):
        cell_ref[h + 1 + own_x + i] = jnp.concatenate([above[3 * h + i], above_side[3 * h + i]], 0)

    def copy(x, _):
        cell_ref[x + h + 1] = jnp.concatenate([lab_own[x], side_ref[3, x]], 0)
        inv_ref[x + h] = inv_in[x]
        for comp in range(3):
            t = get(t0_in, comp, x)
            put(t_ref, 0, comp, x + h, value=t)
            t_out[0, comp, x] = t[:own_y]
            t = get(t1_in, comp, x + h)
            put(t_ref, 1, comp, x + h, value=t)
            t_out[1, comp, x] = t[:own_y]
        return _

    pairs(0, own_x, copy, 0)

    def layer(x):
        e = edge(x)
        c = cell_ref[x + h + 1]
        return diagonal_layer(c, roll(c, 1, 1), e + roll(e, 1, 1), own_y + h)

    for start, stop in ((-h, 1), (own_x, own_x + h)):
        layers = [layer(x) for x in range(start - 1, stop)]
        for x in range(start, stop):
            diag = diagonal_from(layers[x - start] + layers[x - start + 1])
            inv = 1.0 / diag
            inv_ref[x + h] = inv
            if x == 0:
                d_out[...] = diag[:own_y]
            for comp in range(3):
                t = nodes(comp, x) * inv
                put(t_ref, 0, comp, x + h, value=t)
                if x == 0:
                    t_out[0, comp, 0] = t[:own_y]

    totals = []
    for k in range(ITERS):
        first, last = k, planes - k
        runs = [(first, last)] if k > 0 else [(0, h + 3), (planes - h - 2, planes)]
        if k == 0:
            for start, stop in runs:
                for n in range(start, stop):
                    turn_plane(n, t_ref.at[k], turn_ref)
                forward_planes(start, stop, t_ref.at[k], turn_ref, q_ref)
        elif k == 1:
            for start, stop in ((first, lo + 2), (hi - 1, last)):
                for n in range(start, stop):
                    turn_plane(n, t_ref.at[k], turn_ref)
                forward_planes(start, stop, t_ref.at[k], turn_ref, q_ref)
            forward_planes(lo + 2, hi - 1, t1_in, turn1_in, q_ref)
        else:
            forward_planes(first, last, t_ref.at[k], turn_ref, q_ref)
        for j, (line, lanes) in enumerate(tiles):
            for start, stop in runs:
                cells_at = lambda n: cell_ref[n + 1, line, lanes]
                voxel_layers(j, start, stop - 1, cells_at, q_ref, f_ref)

        def advance(n, own, acc):
            acc = list(acc)
            new = update(k, inv_ref[n])
            for comp in range(3):
                t = get(t_ref, k, comp, n)
                force = image_ref[comp, n]
                if own:
                    image = force[:own_y] + KAPPA * t[:own_y]
                    for j in range(k + 1):
                        acc[j] += get(t_ref, j, comp, n, rows=own_y) * image
                    acc[k + 1] += t[:own_y] * r_own[comp, n - lo]
                t = new(force, t, lambda: get(t_ref, k - 1, comp, n))
                if k + 1 < ITERS:
                    put(t_ref, k + 1, comp, n, value=t)
                if own:
                    t_out[k + 1, comp, n - lo] = t[:own_y]
            return tuple(acc)

        def several(n, acc):
            if k + 1 < ITERS:
                for u in range(WIDTH):
                    turn_plane(n - WIDTH + u, t_ref.at[k + 1], turn_ref)
            for u in range(WIDTH):
                acc = advance(n + u, True, acc)
            for u in range(WIDTH):
                collect(n + WIDTH + u, f_ref, image_ref)
            return acc

        if k == 0:
            ends = [n for start, stop in runs for n in range(start + 1, stop - 1)]
            for n in ends:
                collect(n, f_ref, image_ref)
            acc = (jnp.zeros((own_y, depth), jnp.float32),) * 2
            for n in ends:
                acc = advance(n, lo <= n < hi, acc)
            totals.extend(acc)
            continue

        beside = [*range(first + 1, lo), *range(hi, last - 1)] if k + 1 < ITERS else []
        for n in [*beside, *range(lo, lo + WIDTH)]:
            collect(n, f_ref, image_ref)
        for n in beside:
            advance(n, False, ())
        acc = (jnp.zeros((own_y, depth), jnp.float32),) * (k + 2)
        whole = lo + own_x // WIDTH * WIDTH
        acc = strides(lo, whole, WIDTH, several, acc)
        for n in range(whole, hi):
            acc = advance(n, True, acc)
        if k + 1 < ITERS:
            for n in range(whole - WIDTH, last - 1):
                turn_plane(n, t_ref.at[k + 1], turn_ref)
        totals.extend(acc)
    sums_out[...] = jnp.broadcast_to((packed_sums(totals) + sums_in[...])[None], sums_out.shape)


def pack_kernel(
    r_hbm, lab_hbm, r_out, lab_out, up_a, down_a, up_b, down_b, next_out, previous_out, lab_in, arrived
):
    h = HALO
    own_x, own_y = lab_in.shape[:2]
    copies = [
        pltpu.make_async_copy(r_hbm, r_out, arrived.at[0]),
        pltpu.make_async_copy(lab_hbm, lab_in, arrived.at[1]),
    ]
    for copy in copies:
        copy.start()
    for copy in copies:
        copy.wait()

    ups, downs = (up_a, up_b), (down_a, down_b)
    node_at, cell_at, edge_at, blocks, _ = y_parts(own_x)
    for x in range(own_x):
        l = lab_in[x].astype(jnp.float32)
        lab_out[x] = l
        part, place = cell_at(x)
        ups[part][place] = l[own_y - h :]
        downs[part][place] = l[:h]
        part, place = edge_at(x)
        ups[part][blocks[part] + place // h, place % h : place % h + 1] = l[own_y - h - 1 : own_y - h]
        if x < h:
            previous_out[3 * h + x] = l
        if x >= own_x - h - 1:
            next_out[3 * h + x - (own_x - h - 1)] = l
        for comp in range(3):
            r = r_out[comp, x]
            part, place = node_at(comp, x)
            ups[part][place] = r[own_y - h :]
            downs[part][place] = r[:h]
            if x < h:
                previous_out[comp * h + x] = r
            if x >= own_x - h:
                next_out[comp * h + x - (own_x - h)] = r


def combine_kernel(sums_ref, t_ref, d_ref, d_first, x_out, r_out):
    total = jnp.sum(sums_ref[...], axis=0, keepdims=True)
    lane = lax.broadcasted_iota(jnp.int32, total.shape, 1)
    entry = [
        jnp.sum(jnp.where(lane == i, total, 0.0), axis=1, keepdims=True) for i in range(SUMS)
    ]
    gram, right = {}, []
    place = 0
    for k in range(ITERS):
        for j in range(k + 1):
            gram[j, k] = gram[k, j] = entry[place]
            place += 1
        right.append(entry[place])
        place += 1
    scale = [gram[k, k] for k in range(ITERS)]
    inv, low = [], {}
    for k in range(ITERS):
        pivot = gram[k, k]
        good = pivot > 1e-7 * scale[k]
        inv.append(jnp.where(good, 1.0 / jnp.where(good, pivot, 1.0), 0.0))
        for i in range(k + 1, ITERS):
            low[i, k] = gram[i, k] * inv[k]
        for i in range(k + 1, ITERS):
            for j in range(k + 1, i + 1):
                gram[i, j] = gram[j, i] = gram[i, j] - low[i, k] * gram[j, k]
            right[i] = right[i] - low[i, k] * right[k]
    y = [None] * ITERS
    for k in reversed(range(ITERS)):
        y[k] = right[k] * inv[k]
        for i in range(k + 1, ITERS):
            y[k] = y[k] - low[i, k] * y[i]
    e = [jnp.ones_like(y[0])] + [jnp.zeros_like(y[0]) for _ in range(ITERS)]
    for k in range(ITERS):
        e[k + 1] = e[k + 1] - STEP[k] * y[k]
        e[k] = e[k] - SHIFT[k] * y[k]
        if k > 1:
            e[k - 1] = e[k - 1] - STEP[k - 1] * y[k]
    y = [jnp.broadcast_to(v, d_first.shape) for v in y]
    e = [jnp.broadcast_to(v, d_first.shape) for v in e]

    def plane(n, diag):
        for comp in range(3):
            t = [t_ref[k, comp, n] for k in range(ITERS + 1)]
            x, r = y[0] * t[0], e[0] * t[0]
            for k in range(1, ITERS):
                x = x + y[k] * t[k]
                r = r + e[k] * t[k]
            r = r + e[ITERS] * t[ITERS]
            x_out[comp, n] = x
            r_out[comp, n] = r * diag

    def body(n, _):
        plane(n, d_ref[n])
        return _

    plane(0, d_first[...])
    pairs(1, d_ref.shape[0] - 1, body, 0)
    plane(d_ref.shape[0] - 1, d_ref[d_ref.shape[0] - 1])


def local(right_side, labels):
    own_x, own_y, depth = labels.shape
    h = HALO
    f32 = jnp.float32
    devices = lax.axis_size("gx") * lax.axis_size("gy")
    small = pltpu.CompilerParams(vmem_limit_bytes=16 * 2**20)
    blocks, edge_blocks = y_parts(own_x)[3:]
    right_side, lab, up_a, down_a, up_b, down_b, to_next, to_previous = pl.pallas_call(
        pack_kernel,
        out_shape=(
            jax.ShapeDtypeStruct(right_side.shape, f32),
            jax.ShapeDtypeStruct(labels.shape, f32),
            jax.ShapeDtypeStruct((blocks[0] + edge_blocks[0], h, depth), f32),
            jax.ShapeDtypeStruct((blocks[0], h, depth), f32),
            jax.ShapeDtypeStruct((blocks[1] + edge_blocks[1], h, depth), f32),
            jax.ShapeDtypeStruct((blocks[1], h, depth), f32),
            jax.ShapeDtypeStruct((4 * h + 1, own_y, depth), f32),
            jax.ShapeDtypeStruct((4 * h, own_y, depth), f32),
        ),
        in_specs=[pl.BlockSpec(memory_space=pltpu.HBM)] * 2,
        scratch_shapes=[pltpu.VMEM(labels.shape, jnp.int32), pltpu.SemaphoreType.DMA((2,))],
        compiler_params=small,
        name="pack",
    )(*(pltpu.with_memory_space_constraint(v, pltpu.HBM) for v in (right_side, labels)))

    minus_a, plus_a = shifted(up_a, "gy", 1), shifted(down_a, "gy", -1)
    minus_b, plus_b = shifted(up_b, "gy", 1), shifted(down_b, "gy", -1)
    below = shifted(to_next, "gx", 1)
    above = shifted(to_previous, "gx", -1)
    minus_a, plus_a, below, above = lax.optimization_barrier((minus_a, plus_a, below, above))

    def stack(minus, plus, count):
        side = jnp.concatenate([plus[:count], minus[:count]], 1)
        return side, minus[count:].reshape(-1, depth)

    def corner(block, rows):
        rows = jnp.pad(rows, ((0, 2 * h - rows.shape[0]), (0, 0)))
        return jnp.concatenate([block, rows[None]], 0)

    side_a, edge_a = stack(minus_a, plus_a, blocks[0])
    below_side = shifted(corner(side_a[: 4 * h + 1], edge_a[: h + 1]), "gx", 1)
    last = corner(side_a[4 * h + 1 :], edge_a[h + 1 : 2 * h + 1])
    above_side = shifted(last, "gx", -1)
    side_b, edge_b = stack(minus_b, plus_b, blocks[1])

    rows = own_y + 2 * h
    tiles = (rows // 8) * (depth // 128)

    across = depth // 128

    def kept(*lead):
        return pltpu.VMEM((*lead, across, rows + 8, 128), f32)

    def scratch(planes):
        return [
            kept(ITERS, 3, planes),
            kept(3, planes),
            pltpu.VMEM((3, planes, rows, depth), f32),
            pltpu.VMEM((planes, len(MODES), tiles + 1, 8, 128), f32),
            kept(planes, len(MODES)),
        ]

    own_kept = jax.ShapeDtypeStruct((3, own_x, across, rows + 8, 128), f32)
    next_kept = jax.ShapeDtypeStruct((3, own_x + h, across, rows + 8, 128), f32)
    side, t0, t1, turn1, inverse, diagonal, first_sums = pl.pallas_call(
        begin_kernel,
        out_shape=(
            jax.ShapeDtypeStruct((4, own_x, 2 * h, depth), f32),
            own_kept,
            next_kept,
            next_kept,
            jax.ShapeDtypeStruct((own_x, rows, depth), f32),
            jax.ShapeDtypeStruct((own_x, own_y, depth), f32),
            jax.ShapeDtypeStruct((1, 128), f32),
        ),
        scratch_shapes=[pltpu.VMEM((own_x, depth), f32), *scratch(own_x + WIDTH)[1:]],
        compiler_params=pltpu.CompilerParams(vmem_limit_bytes=24 * 2**20),
        name="begin",
    )(right_side, lab, side_a, side_b, edge_a, edge_b)

    planes = own_x + 2 * h
    basis, d_first, sums = pl.pallas_call(
        basis_kernel,
        out_shape=(
            jax.ShapeDtypeStruct((ITERS + 1, 3, own_x, own_y, depth), f32),
            jax.ShapeDtypeStruct((own_y, depth), f32),
            jax.ShapeDtypeStruct((devices, 1, 128), f32),
        ),
        scratch_shapes=[
            pltpu.VMEM((planes + 2, rows, depth), f32),
            pltpu.VMEM((planes, rows, depth), f32),
            *scratch(planes + 1),
        ],
        compiler_params=pltpu.CompilerParams(vmem_limit_bytes=34 * 2**20),
        name="basis",
    )(
        right_side, lab, side, edge_a, below, above, below_side, above_side,
        t0, t1, turn1, inverse, first_sums,
    )

    everyone = lax.all_to_all(sums, ("gx", "gy"), 0, 0)
    out = jax.ShapeDtypeStruct(right_side.shape, f32)
    return pl.pallas_call(combine_kernel, out_shape=(out, out), compiler_params=small, name="combine")(
        everyone.reshape(devices, 128), basis, diagonal, d_first
    )


def solution(mesh):
    in_specs = (P(None, "gx", "gy", None), P("gx", "gy", None))
    out_specs = (P(None, "gx", "gy", None), P(None, "gx", "gy", None))
    return jax.shard_map(local, mesh=mesh, in_specs=in_specs, out_specs=out_specs, check_vma=False)
```

```python
import jax
import jax.numpy as jnp
from jax import lax
from jax.experimental import pallas as pl
from jax.experimental.pallas import tpu as pltpu
from jax.sharding import PartitionSpec as P


ITERS = 4
HALO = ITERS
LAMBDA_SOFT = 0.5769231
LAMBDA_RISE = 1.6452991
SHEAR_SOFT = 0.3846154
SHEAR_RISE = 2.9487179
KAPPA = 0.05
SHIFT = (0.25, 1.6, 1.5, 1.5)
STEP = (1.0, 0.6, 0.6, 0.6)
SUMS = 14
WIDTH = 4


def shifted(shard, axis, by):
    size = lax.axis_size(axis)
    return lax.ppermute(shard, axis, [(i, (i + by) % size) for i in range(size)])


def roll(v, by, axis):
    return pltpu.roll(v, by % v.shape[axis], axis)


def get(ref, *index, row=0, rows=None):
    rows = ref.shape[-2] - 8 if rows is None else rows
    parts = [ref[(*index, i, slice(row, row + rows))] for i in range(ref.shape[-3])]
    return jnp.concatenate(parts, 1)


def put(ref, *index, value):
    rows = value.shape[0]
    for i in range(ref.shape[-3]):
        part = value[:, 128 * i : 128 * (i + 1)]
        ref[(*index, i, slice(0, rows))] = part
        ref[(*index, i, slice(rows, rows + 8))] = part[:8]


def gather_modes(v, up, ahead, ahead_up):
    near = (v + up, up - v)
    far = (ahead + ahead_up, ahead_up - ahead)
    out = {}
    for by in (0, 1):
        out[by, 0] = near[by] + far[by]
        out[by, 1] = far[by] - near[by]
    return out


def scatter_modes(r, below):
    part = []
    for bz in (0, 1):
        part.append((r[0, bz] - r[1, bz]) + (below[0, bz] + below[1, bz]))
    return part[0] - part[1], part[0] + part[1]


def voxel_forces(c, stiff):
    lam = (LAMBDA_SOFT / 16) + (LAMBDA_RISE / 16) * stiff
    mu = (SHEAR_SOFT / 16) + (SHEAR_RISE / 16) * stiff
    mu2 = mu + mu
    lam3 = lam * (1.0 / 3)
    mu3 = mu * (1.0 / 3)
    top = ((LAMBDA_SOFT + 4 * SHEAR_SOFT) / 144) + ((LAMBDA_RISE + 4 * SHEAR_RISE) / 144) * stiff
    f = {}
    normal = ((0, 1, 0, 0), (1, 0, 1, 0), (2, 0, 0, 1))
    t = lam * (c[normal[0]] + c[normal[1]] + c[normal[2]])
    for p in normal:
        f[p] = t + mu2 * c[p]
    for p, q in (
        ((0, 1, 1, 0), (2, 0, 1, 1)),
        ((0, 1, 0, 1), (1, 0, 1, 1)),
        ((1, 1, 1, 0), (2, 1, 0, 1)),
    ):
        t = lam3 * (c[p] + c[q])
        f[p] = t + mu * c[p]
        f[q] = t + mu * c[q]
    for comp in range(3):
        p = (comp, 1, 1, 1)
        f[p] = top * c[p]
    for p, q in (
        ((0, 0, 1, 0), (1, 1, 0, 0)),
        ((0, 0, 0, 1), (2, 1, 0, 0)),
        ((1, 0, 0, 1), (2, 0, 1, 0)),
    ):
        f[p] = f[q] = mu * (c[p] + c[q])
    bend = ((0, 0, 1, 1), (1, 1, 0, 1), (2, 1, 1, 0))
    t = c[bend[0]] + c[bend[1]] + c[bend[2]]
    for p in bend:
        f[p] = mu3 * (t + c[p])
    return f


MODES = [(comp, by, bz) for comp in range(3) for by in (0, 1) for bz in (0, 1)]


def strides(start, stop, width, body, carry):
    def several(i, carry):
        return body(start + width * i, carry)

    return lax.fori_loop(0, -((start - stop) // width), several, carry)


def pairs(start, stop, body, carry):
    return strides(start, stop, 2, lambda n, c: body(n + 1, body(n, c)), carry)


def tiles_of(rows, depth):
    return [(slice(a, a + 8), slice(b, b + 128)) for a in range(0, rows, 8) for b in range(0, depth, 128)]


def diagonal_layer(cells, turned, edge, first_row):
    lz = cells + turned
    row_id = lax.broadcasted_iota(jnp.int32, lz.shape, 0)
    return lz + jnp.where(row_id == first_row, jnp.broadcast_to(edge, lz.shape), roll(lz, 1, 0))


def diagonal_from(two_layers):
    base = 8 * (LAMBDA_SOFT + 4 * SHEAR_SOFT) / 9 + KAPPA
    return base + ((LAMBDA_RISE + 4 * SHEAR_RISE) / 9) * two_layers


def forward_planes(first, last, node_ref, turn_ref, q_ref):
    rows = node_ref.shape[-2] - 8
    tiles = tiles_of(rows, 128 * node_ref.shape[-3])
    for n in range(first, last):
        for comp in range(3):
            put(turn_ref, comp, n, value=roll(get(node_ref, comp, n), -1, 1))

    def forward(n, _):
        for comp in range(3):
            out = gather_modes(
                get(node_ref, comp, n),
                get(node_ref, comp, n, row=1, rows=rows),
                get(turn_ref, comp, n),
                get(turn_ref, comp, n, row=1, rows=rows),
            )
            for i, (cc, by, bz) in enumerate(MODES):
                if cc == comp:
                    for j, tile in enumerate(tiles):
                        q_ref[n, i, j] = out[by, bz][tile]
        return _

    even = first + (last - first) // 2 * 2
    pairs(first, even, forward, 0)
    for n in range(even, last):
        forward(n, 0)


def voxel_layers(j, first, last, cells_at, q_ref, f_ref):
    across, tall = f_ref.shape[-3], f_ref.shape[-2]
    line, lanes = divmod(j, across)
    row = 8 * (line + 1)

    def store(n, i, value):
        f_ref[n, i, lanes, row : row + 8] = value
        if row + 8 == tall:
            f_ref[n, i, lanes, 0:8] = value

    def voxels(n, carry):
        near, behind = carry
        far = [q_ref[n + 1, i, j] for i in range(len(MODES))]
        c = {}
        for i, (comp, by, bz) in enumerate(MODES):
            if (by, bz) != (0, 0):
                c[comp, 0, by, bz] = near[i] + far[i]
            c[comp, 1, by, bz] = far[i] - near[i]
        f = voxel_forces(c, cells_at(n))
        ahead = []
        for i, (comp, by, bz) in enumerate(MODES):
            up = f[comp, 1, by, bz]
            if (by, bz) != (0, 0):
                flat = f[comp, 0, by, bz]
                store(n, i, behind[i] + (flat - up))
                ahead.append(flat + up)
            else:
                store(n, i, behind[i] - up)
                ahead.append(up)
        return far, ahead

    near = [q_ref[first, i, j] for i in range(len(MODES))]
    pairs(first, last, voxels, (near, [jnp.zeros_like(v) for v in near]))


def collect(n, f_ref, image_ref):
    rows = f_ref.shape[-2] - 8
    for comp in range(3):
        here, below = {}, {}
        for i, (cc, by, bz) in enumerate(MODES):
            if cc == comp:
                here[by, bz] = get(f_ref, n, i, row=8, rows=rows)
                below[by, bz] = get(f_ref, n, i, row=7, rows=rows)
        kept, moved = scatter_modes(here, below)
        image_ref[comp, n] = kept + roll(moved, 1, 1)


def update(k, inv):
    gain = inv * (1 / STEP[k])
    own = KAPPA * gain - SHIFT[k] / STEP[k]

    def new(force, t, older):
        out = force * gain + t * own
        return out - (STEP[k - 1] / STEP[k]) * older() if k > 1 else out

    return new


def packed_sums(totals):
    lane = lax.broadcasted_iota(jnp.int32, (1, 128), 1)
    packed = jnp.zeros((1, 128), jnp.float32)
    for i, v in enumerate(totals):
        s = jnp.sum(jnp.sum(v, axis=0, keepdims=True), axis=1, keepdims=True)
        packed = jnp.where(lane == i, s, packed)
    return packed


def y_parts(own_x):
    h = HALO
    mid = own_x - 2 * h

    def node(comp, x):
        if x < h:
            return 0, 4 * h + 1 + comp * h + x
        if x >= own_x - h:
            return 0, comp * h + x - (own_x - h)
        return 1, comp * mid + x - h

    def cell(x):
        if x < h:
            return 0, 7 * h + 1 + x
        if x >= own_x - h - 1:
            return 0, 3 * h + x - (own_x - h - 1)
        return 1, 3 * mid + x - h

    def edge(x):
        if x < h:
            return 0, h + 1 + x
        if x >= own_x - h - 1:
            return 0, x - (own_x - h - 1)
        return 1, x - h

    blocks = (8 * h + 1, 4 * mid - 1)
    edge_blocks = (-(-(2 * h + 1) // h), -(-(mid - 1) // h))
    return node, cell, edge, blocks, edge_blocks


def begin_kernel(
    r_own, lab_own, side_a, side_b, edge_a, edge_b,
    side_out, t_out, next_out, inv_out, d_out, sums_out,
    edge_ref, turn_ref, image_ref, q_ref, f_ref,
):
    own_x, own_y, depth = r_own.shape[1:]

    def both(block, side):
        return jnp.concatenate([block, side], 0)

    node_at, cell_at, edge_at = y_parts(own_x)[:3]
    sides, edges = (side_a, side_b), (edge_a, edge_b)
    for x in range(own_x):
        for comp in range(3):
            part, place = node_at(comp, x)
            side_out[comp, x] = sides[part][place]
        part, place = cell_at(x)
        side_out[3, x] = sides[part][place]
        part, place = edge_at(x)
        edge_ref[x : x + 1] = edges[part][place : place + 1]
    lines = edge_ref[...]
    edge_ref[...] = lines + roll(lines, 1, 1)
    for m in range(own_x):
        image_ref[0, m] = roll(both(lab_own[m], side_out[3, m]), 1, 1)

    def layer(m):
        cells = both(lab_own[m], side_out[3, m])
        return diagonal_layer(cells, image_ref[0, m], edge_ref[pl.ds(m, 1), :], own_y + HALO)

    def start(x, before):
        here = layer(x)
        diag = diagonal_from(before + here)
        inv = 1.0 / diag
        inv_out[x] = inv
        d_out[x] = diag[:own_y]
        for comp in range(3):
            put(t_out, comp, x, value=both(r_own[comp, x], side_out[comp, x]) * inv)
        return here

    before = pairs(1, own_x - 1, start, layer(0))
    start(own_x - 1, before)

    forward_planes(1, own_x, t_out, turn_ref, q_ref)
    for j, (line, lanes) in enumerate(tiles_of(own_y + side_a.shape[1], depth)):

        def cells_at(n):
            if line.start < own_y:
                return lab_own[n, line, lanes]
            return side_out[3, n, line.start - own_y : line.stop - own_y, lanes]

        voxel_layers(j, 1, own_x - 1, cells_at, q_ref, f_ref)

    def advance(x, acc):
        energy, right = acc
        new = update(0, inv_out[x])
        for comp in range(3):
            t = get(t_out, comp, x)
            force = image_ref[comp, x]
            energy += t[:own_y] * (force[:own_y] + KAPPA * t[:own_y])
            right += t[:own_y] * r_own[comp, x]
            put(next_out, comp, x, value=new(force, t, None))
        return energy, right

    def several(n, acc):
        for u in range(WIDTH):
            acc = advance(n + u, acc)
        for u in range(WIDTH):
            collect(n + WIDTH + u, f_ref, image_ref)
        return acc

    for x in range(2, 2 + WIDTH):
        collect(x, f_ref, image_ref)
    whole = 2 + (own_x - 3) // WIDTH * WIDTH
    acc = strides(2, whole, WIDTH, several, (jnp.zeros((own_y, depth), jnp.float32),) * 2)
    for x in range(whole, own_x - 1):
        acc = advance(x, acc)
    sums_out[...] = packed_sums(acc)


def basis_kernel(
    r_own, lab_own, side_ref, edge_a, below, above, below_side, above_side, t0_in, t1_in, inv_in, sums_in,
    t_out, d_out, sums_out,
    cell_ref, inv_ref, t_ref, turn_ref, image_ref, q_ref, f_ref,
):
    h = HALO
    own_x, own_y, depth = r_own.shape[1:]
    rows = own_y + side_ref.shape[2]
    tiles = tiles_of(rows, depth)
    planes = own_x + 2 * h
    lo, hi = h, h + own_x
    edge_at = y_parts(own_x)[2]

    def nodes(comp, x):
        if x < 0:
            return jnp.concatenate([below[comp * h + h + x], below_side[comp * h + h + x]], 0)
        if x >= own_x:
            i = comp * h + x - own_x
            return jnp.concatenate([above[i], above_side[i]], 0)
        return jnp.concatenate([r_own[comp, x], side_ref[comp, x]], 0)

    def edge(x):
        if x < 0:
            return below_side[4 * h + 1, h + 1 + x : h + 2 + x]
        if x >= own_x:
            return above_side[4 * h, x - own_x : x - own_x + 1]
        place = edge_at(x)[1]
        return edge_a[place : place + 1]

    for i in range(h + 1):
        cell_ref[i] = jnp.concatenate([below[3 * h + i], below_side[3 * h + i]], 0)
    for i in range(h):
        cell_ref[h + 1 + own_x + i] = jnp.concatenate([above[3 * h + i], above_side[3 * h + i]], 0)

    def copy(x, _):
        cell_ref[x + h + 1] = jnp.concatenate([lab_own[x], side_ref[3, x]], 0)
        inv_ref[x + h] = inv_in[x]
        for comp in range(3):
            t = get(t0_in, comp, x)
            put(t_ref, 0, comp, x + h, value=t)
            t_out[0, comp, x] = t[:own_y]
            t = get(t1_in, comp, x)
            put(t_ref, 1, comp, x + h, value=t)
            t_out[1, comp, x] = t[:own_y]
        return _

    pairs(0, own_x, copy, 0)

    def layer(x):
        e = edge(x)
        c = cell_ref[x + h + 1]
        return diagonal_layer(c, roll(c, 1, 1), e + roll(e, 1, 1), own_y + h)

    for start, stop in ((-h, 1), (own_x, own_x + h)):
        layers = [layer(x) for x in range(start - 1, stop)]
        for x in range(start, stop):
            diag = diagonal_from(layers[x - start] + layers[x - start + 1])
            inv = 1.0 / diag
            inv_ref[x + h] = inv
            if x == 0:
                d_out[...] = diag[:own_y]
            for comp in range(3):
                t = nodes(comp, x) * inv
                put(t_ref, 0, comp, x + h, value=t)
                if x == 0:
                    t_out[0, comp, 0] = t[:own_y]

    totals = []
    for k in range(ITERS):
        first, last = k, planes - k
        runs = [(first, last)] if k > 0 else [(0, h + 3), (planes - h - 2, planes)]
        for start, stop in runs:
            forward_planes(start, stop, t_ref.at[k], turn_ref, q_ref)
        for j, (line, lanes) in enumerate(tiles):
            for start, stop in runs:
                cells_at = lambda n: cell_ref[n + 1, line, lanes]
                voxel_layers(j, start, stop - 1, cells_at, q_ref, f_ref)

        def advance(n, own, acc):
            acc = list(acc)
            new = update(k, inv_ref[n])
            for comp in range(3):
                t = get(t_ref, k, comp, n)
                force = image_ref[comp, n]
                if own:
                    image = force[:own_y] + KAPPA * t[:own_y]
                    for j in range(k + 1):
                        acc[j] += get(t_ref, j, comp, n, rows=own_y) * image
                    acc[k + 1] += t[:own_y] * r_own[comp, n - lo]
                t = new(force, t, lambda: get(t_ref, k - 1, comp, n))
                if k + 1 < ITERS:
                    put(t_ref, k + 1, comp, n, value=t)
                if own:
                    t_out[k + 1, comp, n - lo] = t[:own_y]
            return tuple(acc)

        def several(n, acc):
            for u in range(WIDTH):
                acc = advance(n + u, True, acc)
            for u in range(WIDTH):
                collect(n + WIDTH + u, f_ref, image_ref)
            return acc

        if k == 0:
            ends = [n for start, stop in runs for n in range(start + 1, stop - 1)]
            for n in ends:
                collect(n, f_ref, image_ref)
            acc = (jnp.zeros((own_y, depth), jnp.float32),) * 2
            for n in ends:
                acc = advance(n, lo <= n < hi, acc)
            totals.extend(acc)
            continue

        beside = [*range(first + 1, lo), *range(hi, last - 1)] if k + 1 < ITERS else []
        for n in [*beside, *range(lo, lo + WIDTH)]:
            collect(n, f_ref, image_ref)
        for n in beside:
            advance(n, False, ())
        acc = (jnp.zeros((own_y, depth), jnp.float32),) * (k + 2)
        whole = lo + own_x // WIDTH * WIDTH
        acc = strides(lo, whole, WIDTH, several, acc)
        for n in range(whole, hi):
            acc = advance(n, True, acc)
        totals.extend(acc)
    sums_out[...] = jnp.broadcast_to((packed_sums(totals) + sums_in[...])[None], sums_out.shape)


def pack_kernel(
    r_hbm, lab_hbm, r_out, lab_out, up_a, down_a, up_b, down_b, next_out, previous_out, lab_in, arrived
):
    h = HALO
    own_x, own_y = lab_in.shape[:2]
    copies = [
        pltpu.make_async_copy(r_hbm, r_out, arrived.at[0]),
        pltpu.make_async_copy(lab_hbm, lab_in, arrived.at[1]),
    ]
    for copy in copies:
        copy.start()
    for copy in copies:
        copy.wait()

    ups, downs = (up_a, up_b), (down_a, down_b)
    node_at, cell_at, edge_at, blocks, _ = y_parts(own_x)
    for x in range(own_x):
        l = lab_in[x].astype(jnp.float32)
        lab_out[x] = l
        part, place = cell_at(x)
        ups[part][place] = l[own_y - h :]
        downs[part][place] = l[:h]
        part, place = edge_at(x)
        ups[part][blocks[part] + place // h, place % h : place % h + 1] = l[own_y - h - 1 : own_y - h]
        if x < h:
            previous_out[3 * h + x] = l
        if x >= own_x - h - 1:
            next_out[3 * h + x - (own_x - h - 1)] = l
        for comp in range(3):
            r = r_out[comp, x]
            part, place = node_at(comp, x)
            ups[part][place] = r[own_y - h :]
            downs[part][place] = r[:h]
            if x < h:
                previous_out[comp * h + x] = r
            if x >= own_x - h:
                next_out[comp * h + x - (own_x - h)] = r


def combine_kernel(sums_ref, t_ref, d_ref, d_first, x_hbm, r_hbm, x_out, r_out, sent):
    total = jnp.sum(sums_ref[...], axis=0, keepdims=True)
    lane = lax.broadcasted_iota(jnp.int32, total.shape, 1)
    entry = [
        jnp.sum(jnp.where(lane == i, total, 0.0), axis=1, keepdims=True) for i in range(SUMS)
    ]
    gram, right = {}, []
    place = 0
    for k in range(ITERS):
        for j in range(k + 1):
            gram[j, k] = gram[k, j] = entry[place]
            place += 1
        right.append(entry[place])
        place += 1
    scale = [gram[k, k] for k in range(ITERS)]
    inv, low = [], {}
    for k in range(ITERS):
        pivot = gram[k, k]
        good = pivot > 1e-7 * scale[k]
        inv.append(jnp.where(good, 1.0 / jnp.where(good, pivot, 1.0), 0.0))
        for i in range(k + 1, ITERS):
            low[i, k] = gram[i, k] * inv[k]
        for i in range(k + 1, ITERS):
            for j in range(k + 1, i + 1):
                gram[i, j] = gram[j, i] = gram[i, j] - low[i, k] * gram[j, k]
            right[i] = right[i] - low[i, k] * right[k]
    y = [None] * ITERS
    for k in reversed(range(ITERS)):
        y[k] = right[k] * inv[k]
        for i in range(k + 1, ITERS):
            y[k] = y[k] - low[i, k] * y[i]
    e = [jnp.ones_like(y[0])] + [jnp.zeros_like(y[0]) for _ in range(ITERS)]
    for k in range(ITERS):
        e[k + 1] = e[k + 1] - STEP[k] * y[k]
        e[k] = e[k] - SHIFT[k] * y[k]
        if k > 1:
            e[k - 1] = e[k - 1] - STEP[k - 1] * y[k]
    y = [jnp.broadcast_to(v, d_first.shape) for v in y]
    e = [jnp.broadcast_to(v, d_first.shape) for v in e]

    def plane(n, diag):
        for comp in range(3):
            t = [t_ref[k, comp, n] for k in range(ITERS + 1)]
            x, r = y[0] * t[0], e[0] * t[0]
            for k in range(1, ITERS):
                x = x + y[k] * t[k]
                r = r + e[k] * t[k]
            r = r + e[ITERS] * t[ITERS]
            x_out[comp, n] = x
            r_out[comp, n] = r * diag

    own_x = d_ref.shape[0]
    group = own_x // HALO
    copies = []
    for i in range(HALO):
        if i == 0:
            plane(0, d_first[...])

        def body(n, _):
            plane(n, d_ref[n])
            return _

        lax.fori_loop(max(1, i * group), (i + 1) * group, body, 0)
        part = slice(i * group, (i + 1) * group)
        for j, (source, target) in enumerate(((x_out, x_hbm), (r_out, r_hbm))):
            copy = pltpu.make_async_copy(source.at[:, part], target.at[:, part], sent.at[i, j])
            copy.start()
            copies.append(copy)
    for copy in copies:
        copy.wait()


def local(right_side, labels):
    own_x, own_y, depth = labels.shape
    h = HALO
    f32 = jnp.float32
    devices = lax.axis_size("gx") * lax.axis_size("gy")
    small = pltpu.CompilerParams(vmem_limit_bytes=16 * 2**20)
    blocks, edge_blocks = y_parts(own_x)[3:]
    right_side, lab, up_a, down_a, up_b, down_b, to_next, to_previous = pl.pallas_call(
        pack_kernel,
        out_shape=(
            jax.ShapeDtypeStruct(right_side.shape, f32),
            jax.ShapeDtypeStruct(labels.shape, f32),
            jax.ShapeDtypeStruct((blocks[0] + edge_blocks[0], h, depth), f32),
            jax.ShapeDtypeStruct((blocks[0], h, depth), f32),
            jax.ShapeDtypeStruct((blocks[1] + edge_blocks[1], h, depth), f32),
            jax.ShapeDtypeStruct((blocks[1], h, depth), f32),
            jax.ShapeDtypeStruct((4 * h + 1, own_y, depth), f32),
            jax.ShapeDtypeStruct((4 * h, own_y, depth), f32),
        ),
        in_specs=[pl.BlockSpec(memory_space=pltpu.HBM)] * 2,
        scratch_shapes=[pltpu.VMEM(labels.shape, jnp.int32), pltpu.SemaphoreType.DMA((2,))],
        compiler_params=small,
        name="pack",
    )(*(pltpu.with_memory_space_constraint(v, pltpu.HBM) for v in (right_side, labels)))

    minus_a, plus_a = shifted(up_a, "gy", 1), shifted(down_a, "gy", -1)
    minus_b, plus_b = shifted(up_b, "gy", 1), shifted(down_b, "gy", -1)
    below = shifted(to_next, "gx", 1)
    above = shifted(to_previous, "gx", -1)

    def stack(minus, plus, count):
        side = jnp.concatenate([plus[:count], minus[:count]], 1)
        return side, minus[count:].reshape(-1, depth)

    def corner(block, rows):
        rows = jnp.pad(rows, ((0, 2 * h - rows.shape[0]), (0, 0)))
        return jnp.concatenate([block, rows[None]], 0)

    side_a, edge_a = stack(minus_a, plus_a, blocks[0])
    below_side = shifted(corner(side_a[: 4 * h + 1], edge_a[: h + 1]), "gx", 1)
    last = corner(side_a[4 * h + 1 :], edge_a[h + 1 : 2 * h + 1])
    above_side = shifted(last, "gx", -1)
    side_b, edge_b = stack(minus_b, plus_b, blocks[1])

    rows = own_y + 2 * h
    tiles = (rows // 8) * (depth // 128)

    across = depth // 128

    def kept(*lead):
        return pltpu.VMEM((*lead, across, rows + 8, 128), f32)

    def scratch(planes):
        return [
            kept(ITERS, 3, planes),
            kept(3, planes),
            pltpu.VMEM((3, planes, rows, depth), f32),
            pltpu.VMEM((planes, len(MODES), tiles + 1, 8, 128), f32),
            kept(planes, len(MODES)),
        ]

    own_kept = jax.ShapeDtypeStruct((3, own_x, across, rows + 8, 128), f32)
    side, t0, t1, inverse, diagonal, first_sums = pl.pallas_call(
        begin_kernel,
        out_shape=(
            jax.ShapeDtypeStruct((4, own_x, 2 * h, depth), f32),
            own_kept,
            own_kept,
            jax.ShapeDtypeStruct((own_x, rows, depth), f32),
            jax.ShapeDtypeStruct((own_x, own_y, depth), f32),
            jax.ShapeDtypeStruct((1, 128), f32),
        ),
        scratch_shapes=[pltpu.VMEM((own_x, depth), f32), *scratch(own_x + WIDTH)[1:]],
        compiler_params=pltpu.CompilerParams(vmem_limit_bytes=24 * 2**20),
        name="begin",
    )(right_side, lab, side_a, side_b, edge_a, edge_b)

    planes = own_x + 2 * h
    basis, d_first, sums = pl.pallas_call(
        basis_kernel,
        out_shape=(
            jax.ShapeDtypeStruct((ITERS + 1, 3, own_x, own_y, depth), f32),
            jax.ShapeDtypeStruct((own_y, depth), f32),
            jax.ShapeDtypeStruct((devices, 1, 128), f32),
        ),
        scratch_shapes=[
            pltpu.VMEM((planes + 2, rows, depth), f32),
            pltpu.VMEM((planes, rows, depth), f32),
            *scratch(planes + 1),
        ],
        compiler_params=pltpu.CompilerParams(vmem_limit_bytes=34 * 2**20),
        name="basis",
    )(
        right_side, lab, side, edge_a, below, above, below_side, above_side,
        t0, t1, inverse, first_sums,
    )

    everyone = lax.all_to_all(sums, ("gx", "gy"), 0, 0)
    out = jax.ShapeDtypeStruct(right_side.shape, f32)
    return pl.pallas_call(
        combine_kernel,
        out_shape=(out, out),
        out_specs=(pl.BlockSpec(memory_space=pltpu.HBM),) * 2,
        scratch_shapes=[
            pltpu.VMEM(right_side.shape, f32),
            pltpu.VMEM(right_side.shape, f32),
            pltpu.SemaphoreType.DMA((h, 2)),
        ],
        compiler_params=small,
        name="combine",
    )(everyone.reshape(devices, 128), basis, diagonal, d_first)


def solution(mesh):
    in_specs = (P(None, "gx", "gy", None), P("gx", "gy", None))
    out_specs = (P(None, "gx", "gy", None), P(None, "gx", "gy", None))
    return jax.shard_map(local, mesh=mesh, in_specs=in_specs, out_specs=out_specs, check_vma=False)
```
